32 devices in a mesh: dp: 4 (over y, x), seq: 8 (over z, core).
Axes of the slice: x: 2, y: 2, z: 4, core: 2. Of those that a mesh axis runs over, the one named last changes fastest.
Arguments:
- hidden_in: bfloat16 [4, 2048, 1536], P('dp', 'seq'), may hold values from -6 to 6
- pre_gain: bfloat16 [1536], P('dp'), may hold values from 0.5 to 1.5
- in_weight: bfloat16 [1536, 6448], P('dp'), may hold values from -0.15625 to 0.15625
- conv_x_weight: float32 [4, 3072], replicated, may hold values from -3 to 3
- conv_x_bias: float32 [3072], replicated, may hold values from -3 to 3
- conv_bc_weight: float32 [4, 256], replicated, may hold values from -3 to 3
- conv_bc_bias: float32 [256], replicated, may hold values from -3 to 3
- dt_bias: float32 [48], replicated, may hold values from -5 to -2
- a_log: float32 [48], replicated, may hold values from -4.5 to 2.8
- skip: float32 [48], replicated, may hold values from 0.5 to 1.5
- norm_gain: bfloat16 [3072], P('dp'), may hold values from 0.5 to 1.5
- out_weight: bfloat16 [3072, 1536], P('dp'), may hold values from -0.109375 to 0.109375
- output_gradient: bfloat16 [4, 2048, 1536], P('dp', 'seq'), may hold values from -6 to 6
Outputs:
- output: float32 [4, 2048, 1536], P('dp', 'seq')
- input_grad: float32 [4, 2048, 1536], P('dp', 'seq')
- pre_gain_grad: float32 [1536], P('dp')
- in_weight_grad: float32 [1536, 6448], P('dp')
- conv_x_weight_grad: float32 [4, 3072], replicated
- conv_x_bias_grad: float32 [3072], replicated
- conv_bc_weight_grad: float32 [4, 256], replicated
- conv_bc_bias_grad: float32 [256], replicated
- dt_bias_grad: float32 [48], replicated
- a_log_grad: float32 [48], replicated
- skip_grad: float32 [48], replicated
- norm_gain_grad: float32 [3072], P('dp')
- out_weight_grad: float32 [3072, 1536], P('dp')
The draws below stay inside these ranges and needn't reach their ends.
All inputs are finite; a program needn't handle non-finite values.
Results may differ from the reference program's by a relative error of at most 0.008.
The reference program's roundings to bfloat16 on the way count: a program that leaves them out, or rounds other values in their place, can miss the bound.
Values may be sent and summed in bfloat16 or wider, within the bound.
A program may use at most 256 MiB of HBM per device.

```python
import jax
import jax.numpy as jnp
from jax import lax

D = 1536
HEADS = 48
STATE = 128
KERNEL = 4
BLOCK = 256
LENGTH = 2048
INNER = 3072
PROJ = 6448
SEQS = 4


def block_levels(stream_key, dims, shards, low, top_value):
    loudness, own = 1.0, jax.random.fold_in(stream_key, 6)
    for position, parts in shards:
        heights = jnp.exp(jax.random.uniform(jax.random.fold_in(own, position), (parts,), jnp.float32, low / len(shards), top_value / len(shards)))
        loudness = loudness * jnp.repeat(heights, dims[position] // parts).reshape([-1 if axis == position else 1 for axis in range(len(dims))])
    return loudness


def bell_draw(own_key, dims, scale, reach, shards=(), kind=jnp.bfloat16):
    level = block_levels(own_key, dims, shards, -0.22, 0.18) if shards else 1.0
    drawn = jax.random.normal(own_key, dims, jnp.float32) * scale * level
    return jnp.minimum(jnp.maximum(drawn, -reach), reach).astype(kind)


def setup_inputs(seed: int = 0) -> dict:
    key_of = jax.random.split(jax.random.key(seed), 14)
    return {
        "hidden_in": bell_draw(key_of[0], (SEQS, LENGTH, D), 1.0, 6.0, ((0, 4), (1, 8))),
        "pre_gain": jnp.clip(0.5 + 1.0 * jax.random.uniform(key_of[1], (D,), jnp.float32) ** block_levels(key_of[1], (D,), ((0, 4),), -0.2, 0.2), 0.5, 1.5).astype(jnp.bfloat16),
        "in_weight": bell_draw(key_of[2], (D, PROJ), D ** -0.5, 0.15625, ((0, 4),)),
        "conv_x_weight": bell_draw(key_of[3], (KERNEL, INNER), KERNEL ** -0.5, 3.0, (), jnp.float32),
        "conv_x_bias": bell_draw(key_of[4], (INNER,), 0.5, 3.0, (), jnp.float32),
        "conv_bc_weight": bell_draw(key_of[5], (KERNEL, 2 * STATE), KERNEL ** -0.5, 3.0, (), jnp.float32),
        "conv_bc_bias": bell_draw(key_of[6], (2 * STATE,), 0.5, 3.0, (), jnp.float32),
        "dt_bias": jnp.clip(jax.random.uniform(key_of[7], (HEADS,), jnp.float32, -5.0, -2.0), -5.0, -2.0),
        "a_log": jnp.clip(jax.random.uniform(key_of[8], (HEADS,), jnp.float32, -4.5, 2.8), -4.5, 2.8),
        "skip": jnp.clip(jax.random.uniform(key_of[9], (HEADS,), jnp.float32, 0.5, 1.5), 0.5, 1.5),
        "norm_gain": jnp.clip(0.5 + 1.0 * jax.random.uniform(key_of[10], (INNER,), jnp.float32) ** block_levels(key_of[10], (INNER,), ((0, 4),), -0.2, 0.2), 0.5, 1.5).astype(jnp.bfloat16),
        "out_weight": bell_draw(key_of[11], (INNER, D), INNER ** -0.5, 0.109375, ((0, 4),)),
        "output_gradient": bell_draw(key_of[12], (SEQS, LENGTH, D), 1.0, 6.0, ((0, 4), (1, 8))),
    }


EPSILON = 1e-05
PRECISE = lax.Precision.HIGHEST

def causal_conv(signal, kernel, offset):
    tap_count = kernel.shape[0]
    length = signal.shape[0]
    padded = jnp.pad(signal, ((tap_count - 1, 0), (0, 0)))
    summed_taps = jnp.zeros_like(signal) + offset[None, :]
    for tap_index in range(tap_count):
        summed_taps = summed_taps + kernel[tap_index][None, :] * padded[tap_index:tap_index + length]
    return summed_taps

def block_scan(values, step_sizes, decay_rates, key_rows, queries):
    length, head_count, head_width = values.shape
    block_count = length // BLOCK
    log_decay = (step_sizes * decay_rates[None, :]).reshape(block_count, BLOCK, head_count)
    lower_mask = lax.broadcasted_iota(jnp.int32, (BLOCK, BLOCK), 0) >= lax.broadcasted_iota(jnp.int32, (BLOCK, BLOCK), 1)
    cumulative = jnp.einsum('ij,cjh->cih', lower_mask.astype(jnp.float32), log_decay, precision=PRECISE)
    value_blocks = values.reshape(block_count, BLOCK, head_count, head_width)
    step_blocks = step_sizes.reshape(block_count, BLOCK, head_count)
    key_blocks = key_rows.reshape(block_count, BLOCK, -1)
    query_blocks = queries.reshape(block_count, BLOCK, -1)
    scores = jnp.einsum('cin,cjn->cij', query_blocks, key_blocks, precision=PRECISE)
    spread = cumulative[:, :, None, :] - cumulative[:, None, :, :]
    decay_table = jnp.exp(jnp.where(lower_mask[None, :, :, None], spread, -1e+30))
    mixing = scores[:, :, :, None] * decay_table * step_blocks[:, None, :, :]
    inside = jnp.einsum('cijh,cjhp->cihp', mixing, value_blocks, precision=PRECISE)
    tail_decay = jnp.exp(cumulative[:, -1:, :] - cumulative) * step_blocks
    fresh_state = jnp.einsum('cjn,cjh,cjhp->chnp', key_blocks, tail_decay, value_blocks, precision=PRECISE)
    block_log = cumulative[:, -1, :]
    block_rows = lax.broadcasted_iota(jnp.int32, (block_count, block_count), 0)
    block_cols = lax.broadcasted_iota(jnp.int32, (block_count, block_count), 1)
    through = jnp.einsum('de,eh->dh', (block_rows >= block_cols).astype(jnp.float32), block_log, precision=PRECISE)
    before = through - block_log
    block_spread = before[:, None, :] - through[None, :, :]
    block_weights = jnp.exp(jnp.where((block_rows > block_cols)[:, :, None], block_spread, -1e+30))
    entering = jnp.einsum('deh,ehnp->dhnp', block_weights, fresh_state, precision=PRECISE)
    outside = jnp.einsum('cin,cih,chnp->cihp', query_blocks, jnp.exp(cumulative), entering, precision=PRECISE)
    return (inside + outside).reshape(length, head_count, head_width)

def mixer(x_raw, dt_raw, bc_raw, conv_weight, conv_bias, bc_weight, bc_bias, dt_shift, a_logs, skip_gain):
    head_count = dt_raw.shape[1]
    length = x_raw.shape[0]
    state_width = bc_raw.shape[1] // 2
    values = jax.nn.silu(causal_conv(x_raw, conv_weight, conv_bias)).reshape(length, head_count, -1)
    key_query = jax.nn.silu(causal_conv(bc_raw, bc_weight, bc_bias))
    step_sizes = jax.nn.softplus(dt_raw + dt_shift[None, :])
    decay_rates = -jnp.exp(a_logs)
    scanned = block_scan(values, step_sizes, decay_rates, key_query[:, :state_width], key_query[:, state_width:])
    scanned = scanned + skip_gain[None, :, None] * values
    return scanned.reshape(length, -1)

def reference(hidden_in, pre_gain, in_weight, conv_x_weight, conv_x_bias, conv_bc_weight, conv_bc_bias, dt_bias, a_log, skip, norm_gain, out_weight, output_gradient):
    inner_width = out_weight.shape[0]
    state_width = conv_bc_bias.shape[0] // 2
    pre_float = pre_gain.astype(jnp.float32)
    norm_float = norm_gain.astype(jnp.float32)
    small_params = (conv_x_weight, conv_x_bias, conv_bc_weight, conv_bc_bias, dt_bias, a_log, skip)

    def one_sequence(totals, pair_item):
        rows_in, rows_grad = pair_item
        rows_float = rows_in.astype(jnp.float32)
        inv_rms = lax.rsqrt(lax.optimization_barrier(jnp.mean(rows_float * rows_float, -1, keepdims=True)) + EPSILON)
        unit_rows = rows_float * inv_rms
        normalized_rows = (unit_rows * pre_float[None, :]).astype(jnp.bfloat16)
        projected = lax.optimization_barrier(jnp.dot(normalized_rows, in_weight, preferred_element_type=jnp.float32).astype(jnp.bfloat16))
        gate_float = projected[:, :inner_width].astype(jnp.float32)
        x_raw = projected[:, inner_width:2 * inner_width].astype(jnp.float32)
        bc_raw = projected[:, 2 * inner_width:2 * inner_width + 2 * state_width].astype(jnp.float32)
        dt_raw = projected[:, 2 * inner_width + 2 * state_width:].astype(jnp.float32)
        mixer_out, pull_back = jax.vjp(mixer, x_raw, dt_raw, bc_raw, *small_params)
        y_float = lax.optimization_barrier(mixer_out.astype(jnp.bfloat16)).astype(jnp.float32)
        gate_sig = jax.nn.sigmoid(gate_float)
        gated_rows = y_float * gate_float * gate_sig
        out_rms = lax.rsqrt(lax.optimization_barrier(jnp.mean(gated_rows * gated_rows, -1, keepdims=True)) + EPSILON)
        unit_gated = gated_rows * out_rms
        mixer_result_rows = (unit_gated * norm_float[None, :]).astype(jnp.bfloat16)
        result_rows = rows_float + jnp.dot(mixer_result_rows, out_weight, preferred_element_type=jnp.float32)
        out_weight_step = jnp.dot(mixer_result_rows.T, rows_grad, preferred_element_type=jnp.float32)
        mixer_rows_gradient = jnp.dot(rows_grad, out_weight.T, preferred_element_type=jnp.float32)
        norm_gain_step = lax.optimization_barrier(jnp.sum(mixer_rows_gradient * unit_gated, 0))
        grad_unit = mixer_rows_gradient * norm_float[None, :]
        grad_gated = out_rms * (grad_unit - unit_gated * lax.optimization_barrier(jnp.mean(grad_unit * unit_gated, -1, keepdims=True)))
        grad_y = lax.optimization_barrier((grad_gated * gate_float * gate_sig).astype(jnp.bfloat16)).astype(jnp.float32)
        grad_gate = grad_gated * y_float * gate_sig * (1.0 + gate_float * (1.0 - gate_sig))
        pulled = pull_back(grad_y)
        projection_gradient = jnp.concatenate([grad_gate, pulled[0], pulled[2], pulled[1]], -1).astype(jnp.bfloat16)
        in_weight_step = jnp.dot(normalized_rows.T, projection_gradient, preferred_element_type=jnp.float32)
        normalized_gradient = jnp.dot(projection_gradient, in_weight.T, preferred_element_type=jnp.float32)
        pre_gain_step = lax.optimization_barrier(jnp.sum(normalized_gradient * unit_rows, 0))
        grad_unit_rows = normalized_gradient * pre_float[None, :]
        input_rows = rows_grad.astype(jnp.float32) + inv_rms * (grad_unit_rows - unit_rows * lax.optimization_barrier(jnp.mean(grad_unit_rows * unit_rows, -1, keepdims=True)))
        small_steps = tuple((total_now + step_now for total_now, step_now in zip(totals[2], pulled[3:])))
        new_totals = (totals[0] + pre_gain_step, totals[1] + in_weight_step, small_steps, totals[3] + norm_gain_step, totals[4] + out_weight_step)
        return (new_totals, (result_rows, input_rows))
    small_zero = tuple((jnp.zeros(param.shape, jnp.float32) for param in small_params))
    start_totals = (jnp.zeros(pre_gain.shape, jnp.float32), jnp.zeros(in_weight.shape, jnp.float32), small_zero, jnp.zeros(norm_gain.shape, jnp.float32), jnp.zeros(out_weight.shape, jnp.float32))
    totals, stacked = lax.scan(one_sequence, start_totals, (hidden_in, output_gradient))
    small_grads = totals[2]
    return (stacked[0], stacked[1], totals[0], totals[1], small_grads[0], small_grads[1], small_grads[2], small_grads[3], small_grads[4], small_grads[5], small_grads[6], totals[3], totals[4])
```

```python
import functools

import jax
import jax.numpy as jnp
from jax import lax
from jax.experimental import pallas as pl
from jax.experimental.pallas import tpu as pltpu
from jax.sharding import Mesh
from jax.sharding import PartitionSpec as P

EPSILON = 1e-05
BLOCK = 256
HALO = 16
F32 = jnp.float32
BF16 = jnp.bfloat16
NN = ((1,), (0,))
NT = ((1,), (1,))
TN = ((0,), (0,))


def mm(a, b, dims=NN):
    return lax.dot_general(
        a.astype(BF16), b.astype(BF16), (dims, ((), ())), preferred_element_type=F32
    )


def split(a):
    high = a.astype(BF16)
    return high, (a - high.astype(F32)).astype(BF16)


def mm3(a, b, dims=NN):
    ah, al = split(a)
    bh, bl = split(b)
    return mm(ah, bh, dims) + (mm(ah, bl, dims) + mm(al, bh, dims))


def mm_exact(a, b, dims=NN):
    b0 = b.astype(BF16)
    r1 = b - b0.astype(F32)
    b1 = r1.astype(BF16)
    b2 = (r1 - b1.astype(F32)).astype(BF16)
    return mm(a, b0, dims) + (mm(a, b1, dims) + mm(a, b2, dims))


def mm_sum(a, b, dims=NN):
    ah, al = split(a)
    return mm(ah, b, dims) + mm(al, b, dims)


def sigmoid(v):
    return 1.0 / (1.0 + jnp.exp(-v))


def lane_mask(width, first):
    lane = lax.broadcasted_iota(jnp.int32, (1, 128), 1)
    return (lane < 64) if first else (lane >= 64)


def expand(v, pair):
    lane = lax.broadcasted_iota(jnp.int32, (1, 128), 1)
    return jnp.where(lane < 64, v[:, 2 * pair : 2 * pair + 1], v[:, 2 * pair + 1 : 2 * pair + 2])


def lower_mask():
    return lax.broadcasted_iota(jnp.int32, (BLOCK, BLOCK), 0) >= lax.broadcasted_iota(
        jnp.int32, (BLOCK, BLOCK), 1
    )


def head_indicator(pair):
    row = lax.broadcasted_iota(jnp.int32, (128, 128), 0)
    col = lax.broadcasted_iota(jnp.int32, (128, 128), 1)
    return (col == 2 * pair + row // 64).astype(BF16)


def conv_block(p_ref, row, col, w_ref, b_ref, wcol):
    raw = p_ref[pl.ds(row, BLOCK + HALO), col : col + 128].astype(F32)
    shifted = [raw[HALO - 3 + k : HALO - 3 + k + BLOCK] for k in range(4)]
    pre = b_ref[0:1, wcol : wcol + 128]
    for k in range(4):
        pre = pre + w_ref[k : k + 1, wcol : wcol + 128] * shifted[k]
    return pre, shifted


def prep_kernel(
    width, px_ref, pt_ref, pd_ref, wx_ref, bx_ref, wb_ref, bb_ref, dtb_ref, alog_ref,
    xs_ref, bc_ref, dt_ref, cum_ref, fin_ref,
):
    blocks = xs_ref.shape[0] // BLOCK
    rate = -jnp.exp(alog_ref[...])
    fin_ref[...] = jnp.zeros_like(fin_ref)

    def step(b, carry):
        row = pl.multiple_of(b * BLOCK, BLOCK)
        for c in range(2):
            pre, _ = conv_block(pt_ref, row, 128 * c, wb_ref, bb_ref, 128 * c)
            bc_ref[pl.ds(row, BLOCK), 128 * c : 128 * c + 128] = pre * sigmoid(pre)
        raw = pd_ref[pl.ds(row + HALO, BLOCK), :].astype(F32)
        raw = raw + dtb_ref[...]
        dt = jnp.maximum(raw, 0.0) + jnp.log1p(jnp.exp(-jnp.abs(raw)))
        cum = mm_exact(lower_mask().astype(F32), dt * rate)
        dt_ref[pl.ds(row, BLOCK), :] = dt
        cum_ref[pl.ds(row, BLOCK), :] = cum
        last = cum[BLOCK - 1 : BLOCK, :]
        weight = dt * jnp.exp(last - cum)
        decay = jnp.exp(last)
        keys_t = bc_ref[pl.ds(row, BLOCK), 0:128].T
        for pair in range(width // 128):
            cols = slice(128 * pair, 128 * pair + 128)
            pre, _ = conv_block(px_ref, row, 128 * pair, wx_ref, bx_ref, 128 * pair)
            xs = pre * sigmoid(pre)
            xs_ref[pl.ds(row, BLOCK), cols] = xs
            fin_ref[:, cols] = fin_ref[:, cols] * expand(decay, pair) + mm3(
                keys_t, xs * expand(weight, pair)
            )
        return carry

    lax.fori_loop(0, blocks, step, 0)


def forward_kernel(
    width, xs_ref, bc_ref, dt_ref, cum_ref, enter_ref, skip_ref, y_ref, yl_ref, states_ref, s_ref
):
    blocks = xs_ref.shape[0] // BLOCK
    s_ref[...] = enter_ref[...].astype(F32)

    def step(b, carry):
        row = pl.multiple_of(b * BLOCK, BLOCK)
        rows = pl.ds(row, BLOCK)
        dt, cum = dt_ref[rows, :], cum_ref[rows, :]
        cum_t = cum.T
        last = cum[BLOCK - 1 : BLOCK, :]
        grow, decay = jnp.exp(cum), jnp.exp(last)
        weight = dt * jnp.exp(last - cum)
        keys, queries = bc_ref[rows, 0:128], bc_ref[rows, 128:256]
        scores = mm3(queries, keys, NT)
        keys_t = keys.T
        mask = lower_mask()
        for pair in range(width // 128):
            cols = slice(128 * pair, 128 * pair + 128)
            xs = xs_ref[rows, cols]
            stepped = xs * expand(dt, pair)
            state = s_ref[:, cols]
            states_ref[b, :, cols] = state
            y = expand(grow, pair) * mm3(queries, state)
            for half in range(2):
                h = 2 * pair + half
                spread = cum[:, h : h + 1] - cum_t[h : h + 1, :]
                table = jnp.exp(jnp.where(mask, spread, -1e30))
                part = jnp.where(lane_mask(128, half == 0), stepped, 0.0)
                y = y + mm3(scores * table, part)
            s_ref[:, cols] = state * expand(decay, pair) + mm3(keys_t, xs * expand(weight, pair))
            yl_ref[rows, cols] = y
            y_ref[rows, cols] = (y + skip_ref[0:1, cols] * xs).astype(BF16)
        return carry

    lax.fori_loop(0, blocks, step, 0)


def leave_kernel(width, bc_ref, cum_ref, gy_ref, out_ref):
    blocks = gy_ref.shape[0] // BLOCK
    out_ref[...] = jnp.zeros_like(out_ref)

    def step(i, carry):
        row = pl.multiple_of((blocks - 1 - i) * BLOCK, BLOCK)
        rows = pl.ds(row, BLOCK)
        cum = cum_ref[rows, :]
        grow, decay = jnp.exp(cum), jnp.exp(cum[BLOCK - 1 : BLOCK, :])
        queries_t = bc_ref[rows, 128:256].T
        for pair in range(width // 128):
            cols = slice(128 * pair, 128 * pair + 128)
            dy = gy_ref[rows, cols].astype(F32)
            out_ref[:, cols] = out_ref[:, cols] * expand(decay, pair) + mm3(
                queries_t, expand(grow, pair) * dy
            )
        return carry

    lax.fori_loop(0, blocks, step, 0)


def backward_kernel(
    width, px_ref, pt_ref, pd_ref, xs_ref, bc_ref, dt_ref, cum_ref, gy_ref, yl_ref, states_ref, ds_in_ref, skip_ref,
    wx_ref, bx_ref, wb_ref, bb_ref, dtb_ref, alog_ref,
    dpre_ref, dpb_ref, gdt_ref, gwx_ref, gwb_ref, head_ref,
    ds_ref, dscore_ref,
):
    blocks = gy_ref.shape[0] // BLOCK
    rate = -jnp.exp(alog_ref[...])
    ds_ref[...] = ds_in_ref[...].astype(F32)
    gwx_ref[...] = jnp.zeros_like(gwx_ref)
    gwb_ref[...] = jnp.zeros_like(gwb_ref)
    head_ref[...] = jnp.zeros_like(head_ref)

    def step(i, carry):
        b = blocks - 1 - i
        row = pl.multiple_of(b * BLOCK, BLOCK)
        rows = pl.ds(row, BLOCK)
        dt, cum = dt_ref[rows, :], cum_ref[rows, :]
        cum_t = cum.T
        last = cum[BLOCK - 1 : BLOCK, :]
        grow, decay, tail = jnp.exp(cum), jnp.exp(last), jnp.exp(last - cum)
        keys, queries = bc_ref[rows, 0:128], bc_ref[rows, 128:256]
        scores = mm3(queries, keys, NT)
        queries_t = queries.T
        mask = lower_mask()
        dscore_ref[...] = jnp.zeros_like(dscore_ref)
        dkeys = jnp.zeros((BLOCK, 128), F32)
        dqueries = jnp.zeros((BLOCK, 128), F32)
        dcum = jnp.zeros((BLOCK, 128), F32)
        ddt = jnp.zeros((BLOCK, 128), F32)
        dlast = jnp.zeros((1, 128), F32)
        for pair in range(width // 128):
            cols = slice(128 * pair, 128 * pair + 128)
            xs = xs_ref[rows, cols]
            dt_e = expand(dt, pair)
            stepped_f = xs * dt_e
            stepped, stepped_low = split(stepped_f)
            dy = gy_ref[rows, cols]
            dy_f = dy.astype(F32)
            state, ds = states_ref[b, :, cols], ds_ref[:, cols]
            dstep = jnp.zeros((BLOCK, 128), F32)
            for half in range(2):
                h = 2 * pair + half
                spread = cum[:, h : h + 1] - cum_t[h : h + 1, :]
                table = jnp.exp(jnp.where(mask, spread, -1e30))
                part = jnp.where(lane_mask(128, half == 0), dy_f, 0.0).astype(BF16)
                dmix = mm(part, stepped, NT) + mm(part, stepped_low, NT)
                dscore_ref[...] += dmix * table
                high, low = split(scores * table)
                dstep = dstep + (mm(high, part, TN) + mm(low, part, TN))
            tail_e = expand(tail, pair)
            carried = mm3(keys, ds) * tail_e
            dstep = dstep + carried
            dkeys = dkeys + mm3(xs * dt_e * tail_e, ds, NT)
            grown = expand(grow, pair) * dy_f
            dqueries = dqueries + mm3(grown, state, NT)
            decay_e = expand(decay, pair)
            ends = jnp.sum(stepped_f * carried, 0, keepdims=True) + decay_e * jnp.sum(
                ds * state, 0, keepdims=True
            )
            ds_ref[:, cols] = ds * decay_e + mm3(queries_t, grown)
            dxs = dstep * dt_e + skip_ref[0:1, cols] * dy_f
            which = head_indicator(pair)
            ddt = ddt + mm_sum(dstep * xs, which)
            dcum = dcum + mm_sum(dy_f * yl_ref[rows, cols] - stepped_f * dstep, which)
            dlast = dlast + mm_sum(jnp.broadcast_to(ends, (8, 128)), which)[0:1]
            pre, shifted = conv_block(px_ref, row, 128 * pair, wx_ref, bx_ref, 128 * pair)
            sig = sigmoid(pre)
            dpre = dxs * sig * (1.0 + pre * (1.0 - sig))
            dpre_ref[rows, cols] = dpre
            for k in range(4):
                gwx_ref[k : k + 1, cols] += jnp.sum(dpre * shifted[k], 0, keepdims=True)
            gwx_ref[4:5, cols] += jnp.sum(dpre, 0, keepdims=True)
            gwx_ref[5:6, cols] += jnp.sum(dy_f * xs, 0, keepdims=True)
        at_end = lax.broadcasted_iota(jnp.int32, (BLOCK, 128), 0) == BLOCK - 1
        dcum = dcum + jnp.where(at_end, dlast, 0.0)
        dlog = mm_exact(mask.astype(F32), dcum, TN)
        raw = pd_ref[pl.ds(row + HALO, BLOCK), :].astype(F32)
        draw = (ddt + dlog * rate) * sigmoid(raw + dtb_ref[...])
        gdt_ref[rows, :] = draw
        head_ref[0:1, :] += jnp.sum(draw, 0, keepdims=True)
        head_ref[1:2, :] += jnp.sum(dlog * dt, 0, keepdims=True) * rate
        dqueries = dqueries + mm3(dscore_ref[...], keys)
        dkeys = dkeys + mm3(dscore_ref[...], queries, TN)
        for c, grad in enumerate((dkeys, dqueries)):
            cols = slice(128 * c, 128 * c + 128)
            pre, shifted = conv_block(pt_ref, row, 128 * c, wb_ref, bb_ref, 128 * c)
            sig = sigmoid(pre)
            dpre = grad * sig * (1.0 + pre * (1.0 - sig))
            dpb_ref[rows, cols] = dpre
            for k in range(4):
                gwb_ref[k : k + 1, cols] += jnp.sum(dpre * shifted[k], 0, keepdims=True)
            gwb_ref[4:5, cols] += jnp.sum(dpre, 0, keepdims=True)
        return carry

    lax.fori_loop(0, blocks, step, 0)


MESH = pl.DeviceIdType.MESH


def bits_of(count):
    return [1 << i for i in range(count.bit_length() - 1)]


def bit_at(index, bit):
    return (index // bit) % 2


def flip(index, bits):
    for bit in bits:
        index = index + bit * (1 - 2 * bit_at(index, bit))
    return index


def subsets(bits):
    found = [frozenset()]
    for bit in bits:
        found = found + [f | {bit} for f in found]
    return found


class Links:
    def __init__(self, send, recv):
        self.send, self.recv, self.count, self.open = send, recv, 0, []

    def make(self, src, dst, target, index=None):
        if index is None:
            index, self.count = self.count, self.count + 1
        return pltpu.make_async_remote_copy(
            src_ref=src, dst_ref=dst, send_sem=self.send.at[index], recv_sem=self.recv.at[index],
            device_id=target, device_id_type=MESH,
        )

    def start(self, src, dst, target):
        copy = self.make(src, dst, target)
        copy.start()
        self.open.append(copy)
        return copy

    def drain(self):
        for copy in self.open:
            copy.wait_send()


def meet(targets):
    barrier = pltpu.get_barrier_semaphore()
    for target in targets:
        pl.semaphore_signal(barrier, inc=1, device_id=target, device_id_type=MESH)
    pl.semaphore_wait(barrier, len(targets))


def neighbours(axis):
    me = lax.axis_index(axis)
    return [{axis: flip(me, (bit,))} for bit in bits_of(lax.axis_size(axis))]


def run_flows(flows):
    flows = list(flows)
    while flows:
        flows = [flow for flow in flows if next(flow, flow) is not flow]


def add_rows(out, a, b):
    rows = out.shape[0]
    step = 16 if rows % 16 == 0 else 8

    @pl.loop(0, rows // step)
    def _(i):
        at = pl.ds(pl.multiple_of(i * step, step), step)
        out[at, :] = (a[at, :].astype(F32) + b[at, :].astype(F32)).astype(out.dtype)


def gather_flow(links, axis, order, own, slot):
    me = lax.axis_index(axis)
    held = [frozenset()]
    for bit in order:
        target = {axis: flip(me, (bit,))}
        copies = [
            links.start(slot(flip(me, f)) if f else own, slot(flip(me, f)), target) for f in held
        ]
        yield None
        for copy in copies:
            copy.wait_recv()
        held = held + [f | {bit} for f in held]


def reduce_flow(links, axis, order, source, inbox, total, final=None):
    me = lax.axis_index(axis)
    base = 0

    def current(f):
        return source(flip(me, f))

    for stage, bit in enumerate(order):
        keep = subsets(order[stage + 1 :])
        target = {axis: flip(me, (bit,))}
        copies = [
            links.start(current(f | {bit}), inbox(base + k), target) for k, f in enumerate(keep)
        ]
        yield None
        places = {}
        for k, f in enumerate(keep):
            copies[k].wait_recv()
            out = total(base + k)
            if final is not None and stage == len(order) - 1:
                out = final
            add_rows(out, current(f), inbox(base + k))
            places[f] = out
        current = places.__getitem__
        base += len(keep)


def spread_flow(links, order, block):
    d, q = lax.axis_index("dp"), lax.axis_index("quad")
    away = {bit: bit_at(d, bit) != bit_at(q, bit) for bit in order}
    for stage, bit in enumerate(order):
        reached = jnp.bool_(True)
        for later in order[stage + 1 :]:
            reached = jnp.logical_and(reached, jnp.logical_not(away[later]))
        holder = jnp.logical_and(reached, jnp.logical_not(away[bit]))
        taker = jnp.logical_and(reached, away[bit])
        index, links.count = links.count, links.count + 1
        target = {"dp": flip(d, (bit,))}

        @pl.when(holder)
        def _():
            links.make(block, block, target, index).start()

        yield None

        @pl.when(holder)
        def _():
            links.make(block, block, target, index).wait_send()

        @pl.when(taker)
        def _():
            links.make(block, block, target, index).wait_recv()


def collect_kernel(
    width, win_ref, wt_ref, wo_in_ref, hid_ref, og_ref, gain_ref,
    wz_ref, wx_ref, wt_out, wo_ref, hid_out, og_out, gain_out, halo_ref, send, recv, local,
):
    d, q, p = lax.axis_index("dp"), lax.axis_index("quad"), lax.axis_index("pair")
    rows = win_ref.shape[0]
    inner = width * lax.axis_size("quad")
    links = Links(send, recv)
    dp_bits, quad_bits = bits_of(lax.axis_size("dp")), bits_of(lax.axis_size("quad"))
    meet(neighbours("dp") + neighbours("quad") + neighbours("pair"))

    def columns(base):
        return pl.ds(pl.multiple_of(base + q * width, 128), width)

    flows = [gather_flow(links, "dp", dp_bits, gain_ref, lambda i: gain_out.at[i])]

    def weights(source, out):
        for h, order in enumerate((dp_bits, dp_bits[::-1])):
            part = pl.ds(h * (rows // 2), rows // 2)
            flows.append(
                gather_flow(links, "dp", order, source(part), lambda i, part=part: out.at[i, part])
            )

    weights(lambda part: win_ref.at[part, columns(inner)], wx_ref)
    weights(lambda part: wt_ref.at[part], wt_out)
    flows.append(gather_flow(links, "quad", quad_bits[::-1], hid_ref, lambda i: hid_out.at[i]))
    weights(lambda part: win_ref.at[part, columns(0)], wz_ref)
    flows.append(gather_flow(links, "quad", quad_bits[::-1], og_ref, lambda i: og_out.at[i]))
    owned = [
        (win_ref.at[:, columns(inner)], wx_ref.at[d]), (wt_ref, wt_out.at[d]),
        (win_ref.at[:, columns(0)], wz_ref.at[d]), (hid_ref, hid_out.at[q]),
        (og_ref, og_out.at[q]), (gain_ref, gain_out.at[d]),
    ]
    copies = [pltpu.make_async_copy(a, b, local.at[i]) for i, (a, b) in enumerate(owned)]

    @pl.when(d == q)
    def _():
        copy = pltpu.make_async_copy(wo_in_ref, wo_ref, local.at[len(owned)])
        copy.start()
        copy.wait()

    half = width // 2
    for h, order in enumerate((dp_bits, dp_bits[::-1])):
        flows.append(spread_flow(links, order, wo_ref.at[pl.ds(h * half, half)]))

    def halo():
        for _ in quad_bits:
            yield None
        tail = hid_out.at[hid_out.shape[0] - 1, pl.ds(hid_out.shape[1] - HALO, HALO)]
        copy = links.start(tail, halo_ref, {"pair": flip(p, (1,))})
        yield None
        copy.wait_recv()

    own_last = copies[3]
    for copy in copies:
        copy.start()
    own_last.wait()
    flows.append(halo())
    run_flows(flows)
    for copy in copies:
        if copy is not own_last:
            copy.wait()
    links.drain()


def combine_kernel(
    in_ref, out_ref, gn_ref, op_ref, small_ref,
    in_all, out_all, gn_own, op_own, small_all,
    in_box, in_sum, in_pair, out_box, out_sum, out_pair, out_tot, gn_box, gn_sum, op_box, op_sum,
    small_box, small_sum, send, recv,
):
    d, q, p = lax.axis_index("dp"), lax.axis_index("quad"), lax.axis_index("pair")
    links = Links(send, recv)
    dp_bits, quad_bits = bits_of(lax.axis_size("dp")), bits_of(lax.axis_size("quad"))
    blocks = lax.axis_size("dp") - 1
    near = neighbours("dp") + neighbours("quad") + neighbours("pair")
    swapped = {"dp": q, "quad": d}

    @pl.when(d == q)
    def _():
        meet(near)

    @pl.when(d != q)
    def _():
        meet([*near, swapped])

    other = {"pair": flip(p, (1,))}
    orders = (dp_bits, dp_bits[::-1])

    def in_flow(h):
        half = in_ref.shape[1] // 2
        part = pl.ds(h * half, half)
        yield from reduce_flow(
            links, "dp", orders[h], lambda i: in_ref.at[i, part],
            lambda k: in_box.at[h, k], lambda k: in_sum.at[h, k],
        )
        mine, box = in_sum.at[h, blocks - 1], in_pair.at[h]
        copy = links.start(mine, box, other)
        yield None
        copy.wait_recv()
        own = in_all.at[q, part]
        add_rows(own, mine, box)
        yield from gather_flow(
            links, "quad", quad_bits[::-1], own, lambda i: in_all.at[i, part]
        )

    def out_flow(h):
        half = out_ref.shape[2] // 2
        part = pl.ds(h * half, half)
        yield from reduce_flow(
            links, "dp", orders[h], lambda i: out_ref.at[i, :, part],
            lambda k: out_box.at[h, k], lambda k: out_sum.at[h, k],
        )
        mine, box, whole = out_sum.at[h, blocks - 1], out_pair.at[h], out_tot.at[h]
        copy = links.start(mine, box, other)
        yield None
        copy.wait_recv()
        add_rows(whole, mine, box)
        index, links.count = links.count, links.count + 1

        @pl.when(d == q)
        def _():
            out_all[q, :, part] = whole[...]

        @pl.when(d != q)
        def _():
            links.make(whole, out_all.at[d, :, part], swapped, index).start()

        yield None

        @pl.when(d != q)
        def _():
            links.make(whole, out_all.at[d, :, part], swapped, index).wait()

        yield from gather_flow(
            links, "quad", quad_bits[::-1], out_all.at[q, :, part], lambda i: out_all.at[i, :, part]
        )

    def small_flow():
        current = small_ref
        steps = [("dp", bit) for bit in dp_bits] + [("pair", 1)]
        for k, (axis, bit) in enumerate(steps):
            target = {axis: flip(lax.axis_index(axis), (bit,))}
            copy = links.start(current, small_box.at[k], target)
            yield None
            copy.wait_recv()
            out = small_sum.at[k] if k < len(steps) - 1 else small_all.at[q]
            out[...] = current[...] + small_box[k]
            current = out
        yield from gather_flow(
            links, "quad", quad_bits[::-1], small_all.at[q], lambda i: small_all.at[i]
        )

    run_flows([
        small_flow(),
        in_flow(0), in_flow(1),
        reduce_flow(
            links, "quad", quad_bits, lambda i: gn_ref.at[i], lambda k: gn_box.at[k],
            lambda k: gn_sum.at[k], gn_own,
        ),
        out_flow(0), out_flow(1),
        reduce_flow(
            links, "quad", quad_bits, lambda i: op_ref.at[i], lambda k: op_box.at[k],
            lambda k: op_sum.at[k], op_own,
        ),
    ])
    links.drain()


def remote_call(kernel, ident, outs, any_inputs, scratch, copies, extra=(), flops=10**6):
    vmem, anywhere = pl.BlockSpec(memory_space=pltpu.VMEM), pl.BlockSpec(memory_space=pl.ANY)

    def run(*args):
        moved = sum(a.size * a.dtype.itemsize for a in (*args, *outs))
        return pl.pallas_call(
            kernel,
            out_shape=tuple(outs),
            in_specs=[anywhere if i in any_inputs else vmem for i in range(len(args))],
            out_specs=tuple([vmem] * len(outs)),
            scratch_shapes=list(scratch)
            + [pltpu.SemaphoreType.DMA((copies,)), pltpu.SemaphoreType.DMA((copies,))]
            + list(extra),
            compiler_params=pltpu.CompilerParams(
                vmem_limit_bytes=62 * 2**20, collective_id=ident, has_side_effects=True
            ),
            cost_estimate=pl.CostEstimate(flops=flops, bytes_accessed=moved, transcendentals=0),
        )(*args)

    return run


def call(kernel, outs, scratch=(), flops=10**9):
    vmem = pl.BlockSpec(memory_space=pltpu.VMEM)

    def run(*args):
        moved = sum(a.size * a.dtype.itemsize for a in (*args, *outs))
        return pl.pallas_call(
            kernel,
            out_shape=tuple(outs),
            in_specs=[vmem] * len(args),
            out_specs=tuple([vmem] * len(outs)),
            scratch_shapes=list(scratch),
            compiler_params=pltpu.CompilerParams(vmem_limit_bytes=60 * 2**20),
            cost_estimate=pl.CostEstimate(flops=flops, bytes_accessed=moved, transcendentals=0),
        )(*args)

    return run


def on_device(
    hidden_in, pre_gain, in_weight, conv_x_weight, conv_x_bias, conv_bc_weight, conv_bc_bias,
    dt_bias, a_log, skip, norm_gain, out_weight, output_gradient,
):
    dp, pairs, quads = lax.axis_size("dp"), lax.axis_size("pair"), lax.axis_size("quad")
    pair_rank, quad = lax.axis_index("pair"), lax.axis_index("quad")
    _, local, model = hidden_in.shape
    inner = conv_x_bias.shape[0]
    state2 = conv_bc_bias.shape[0]
    heads = dt_bias.shape[0]
    width, own_heads, bc_cols = inner // quads, heads // quads, state2 // quads
    tokens = local * quads
    everyone = ("dp", "pair", "quad")

    def own(v, n, axis, base=0):
        return lax.dynamic_slice_in_dim(v, base + quad * n, n, axis)

    def sds(shape, dtype=F32):
        return jax.ShapeDtypeStruct(shape, dtype)

    pre_size = pre_gain.shape[0]
    gain_block = jnp.broadcast_to(jnp.concatenate([pre_gain, norm_gain]).astype(F32), (8, pre_size + norm_gain.shape[0]))
    w_tail = in_weight[:, 2 * inner :]
    tail_width = w_tail.shape[1] + -w_tail.shape[1] % 128
    w_tail = jnp.pad(w_tail, ((0, 0), (0, tail_width - w_tail.shape[1])))
    rows_dp = in_weight.shape[0]
    bits = len(bits_of(dp))
    copies = (dp - 1) * 7 + 2 * (quads - 1) + 2 * bits + 1
    wz, w_x, w_t, w_out, hidden_all, grad_all, gains, halo_rows = remote_call(
        functools.partial(collect_kernel, width), 0,
        [
            sds((dp, rows_dp, width), BF16), sds((dp, rows_dp, width), BF16),
            sds((dp, rows_dp, tail_width), BF16), sds((width, model), BF16),
            sds((quads, local, model), BF16), sds((quads, local, model), BF16),
            sds((dp, *gain_block.shape)), sds((HALO, model), BF16),
        ],
        range(6), [], copies, extra=[pltpu.SemaphoreType.DMA((7,))],
    )(in_weight, w_tail, out_weight, hidden_in[0], output_gradient[0], gain_block)
    pre_full = gains[:, 0, :pre_size].reshape(-1)
    norm_own = own(gains[:, 0, pre_size:].reshape(-1), width, 0)[None]
    wz, w_x = wz.reshape(model, width), w_x.reshape(model, width)
    w_t = w_t.reshape(model, tail_width)
    grad_all = grad_all.reshape(tokens, model)

    def unit(v):
        v = v.astype(F32)
        return v * lax.rsqrt(jnp.mean(v * v, -1, keepdims=True) + EPSILON)

    rows = hidden_in[0].astype(F32)
    inv_rms = lax.rsqrt(jnp.mean(rows * rows, -1, keepdims=True) + EPSILON)
    unit_rows = rows * inv_rms
    unit_all = unit(hidden_all.reshape(tokens, model))
    halo_unit = jnp.where(pair_rank > 0, unit(halo_rows), 0.0)
    normed_all = (unit_all * pre_full[None]).astype(BF16)
    normed_halo = jnp.concatenate([(halo_unit * pre_full[None]).astype(BF16), normed_all], 0)
    grad_rows = output_gradient[0]

    def project(v, w):
        return lax.optimization_barrier(jnp.dot(v, w, preferred_element_type=F32).astype(BF16))

    px, pt = project(normed_halo, w_x), project(normed_halo, w_t)
    gate = project(normed_all, wz).astype(F32)
    pd = jnp.pad(own(pt, own_heads, 1, state2), ((0, 0), (0, 128 - own_heads)))

    def pad_heads(v):
        return jnp.pad(own(v, own_heads, 0), (0, 128 - own_heads))[None]

    wx, bx = own(conv_x_weight, width, 1), own(conv_x_bias, width, 0)[None]
    wb, bb = conv_bc_weight, conv_bc_bias[None]
    dtb, alog = pad_heads(dt_bias), pad_heads(a_log)
    skip_own = jnp.repeat(own(skip, own_heads, 0), width // own_heads)[None]

    big, col = (tokens, width), (tokens, 128)
    xs, bc, dt, cum, final = call(
        functools.partial(prep_kernel, width),
        [sds(big), sds((tokens, state2)), sds(col), sds(col), sds((128, width))],
    )(px, pt, pd, wx, bx, wb, bb, dtb, alog)
    enter = lax.ppermute(final, "pair", [(i, i + 1) for i in range(pairs - 1)])
    y, y_long, states = call(
        functools.partial(forward_kernel, width),
        [sds(big, BF16), sds(big), sds((tokens // BLOCK, 128, width))],
        [pltpu.VMEM((128, width), F32)],
    )(xs, bc, dt, cum, enter, skip_own)

    y_float = y.astype(F32)
    sig = jax.nn.sigmoid(gate)
    gated = y_float * gate * sig
    grad_mixed = jnp.einsum("tf,cf->tc", grad_all, w_out, preferred_element_type=F32)
    grad_unit = grad_mixed * norm_own
    stats = lax.psum(
        jnp.stack([jnp.sum(gated * gated, -1), jnp.sum(grad_unit * gated, -1)]), "quad"
    )
    out_rms = lax.rsqrt(stats[0] / inner + EPSILON)[:, None]
    mean_dot = out_rms * stats[1][:, None] / inner
    unit_gated = gated * out_rms
    mixed = (unit_gated * norm_own).astype(BF16)
    norm_part = jnp.sum(grad_mixed * unit_gated, 0)
    grad_gated = out_rms * (grad_unit - unit_gated * mean_dot)
    grad_y = (grad_gated * gate * sig).astype(BF16)
    grad_gate = (grad_gated * y_float * sig * (1.0 + gate * (1.0 - sig))).astype(BF16)

    out_part = jnp.dot(mixed, w_out, preferred_element_type=F32).astype(BF16)

    leaving = call(functools.partial(leave_kernel, width), [sds((128, width))])(bc, cum, grad_y)[0]
    back = [(i + 1, i) for i in range(pairs - 1)]
    ds_in = lax.ppermute(leaving, "pair", back)
    dpre, dpb, gdt, gwx, gwb, heads_grad = call(
        functools.partial(backward_kernel, width),
        [sds(big), sds((tokens, state2)), sds(col), sds((8, width)), sds((8, state2)), sds((8, 128))],
        [pltpu.VMEM((128, width), F32), pltpu.VMEM((BLOCK, BLOCK), F32)],
    )(
        px, pt, pd, xs, bc, dt, cum, grad_y, y_long, states, ds_in, skip_own,
        wx, bx, wb, bb, dtb, alog,
    )
    after = lax.ppermute(jnp.concatenate([dpre[:8], dpb[:8]], 1), "pair", back)

    def unconv(v, tail, kernel):
        padded = jnp.concatenate([v, tail], 0)
        return sum(kernel[k][None] * padded[3 - k : 3 - k + tokens] for k in range(4))

    grad_x = unconv(dpre, after[:, :width], wx).astype(BF16)
    grad_bc = unconv(dpb, after[:, width:], wb)
    bc_local = lax.psum_scatter(grad_bc, "quad", scatter_dimension=0, tiled=True).astype(BF16)
    bc_all = lax.all_gather(bc_local, "quad", axis=0, tiled=True)
    tail_cols = jnp.concatenate(
        [own(bc_all, bc_cols, 1), gdt[:, :own_heads].astype(BF16)], 1
    )
    tail_pad = -(bc_cols + own_heads) % 128
    tail_cols = jnp.pad(tail_cols, ((0, 0), (0, tail_pad)))
    grad_proj = jnp.concatenate([grad_gate, grad_x, tail_cols], 1)
    w_tail_own = jnp.concatenate(
        [
            own(w_t, bc_cols, 1),
            own(w_t, own_heads, 1, state2),
        ],
        1,
    )
    w_tail_own = jnp.pad(w_tail_own, ((0, 0), (0, tail_pad)))
    nt = (((1,), (1,)), ((), ()))
    normed_part = (
        lax.dot_general(grad_gate, wz, nt, preferred_element_type=F32)
        + lax.dot_general(grad_x, w_x, nt, preferred_element_type=F32)
        + lax.dot_general(tail_cols, w_tail_own, nt, preferred_element_type=F32)
    )
    pre_part = jnp.sum(normed_part * unit_all, 0)
    in_part = jnp.einsum("tc,tp->cp", normed_all, grad_proj, preferred_element_type=F32)
    out_part_w = jnp.einsum("tc,tf->cf", mixed, grad_all, preferred_element_type=F32)
    norm_part = norm_part.reshape(-1, 128)
    small_in = jnp.concatenate(
        [
            gwx[:6].reshape(-1, 128), gwb[:5].reshape(-1, 128), heads_grad[:2],
            pre_part.reshape(-1, 128), norm_part,
        ],
        0,
    )
    small_rows = small_in.shape[0]
    small_in = jnp.pad(small_in, ((0, -small_rows % 8), (0, 0)))
    own_in, own_out = rows_dp, width // dp
    gw = grad_proj.shape[1]
    vm = pltpu.VMEM
    copies = 2 * (dp - 1 + 1 + quads - 1) + 2 * (dp - 1 + 2 + quads - 1) + 2 * (quads - 1) + bits + 1 + quads - 1
    in_all, out_all, gn_own, op_own, small_all = remote_call(
        combine_kernel, 1,
        [
            sds((quads, own_in, gw), BF16), sds((quads, own_out, model), BF16),
            sds((local, model)), sds((local, model)), sds((quads, *small_in.shape)),
        ],
        (),
        [
            vm((2, dp - 1, own_in // 2, gw), BF16), vm((2, dp - 1, own_in // 2, gw), BF16),
            vm((2, own_in // 2, gw), BF16),
            vm((2, dp - 1, own_out, model // 2), BF16), vm((2, dp - 1, own_out, model // 2), BF16),
            vm((2, own_out, model // 2), BF16), vm((2, own_out, model // 2), BF16),
            vm((quads - 1, local, model), BF16), vm((quads - 1, local, model), BF16),
            vm((quads - 1, local, model), BF16), vm((quads - 1, local, model), BF16),
            vm((bits + 1, *small_in.shape), F32), vm((bits + 1, *small_in.shape), F32),
        ],
        copies,
    )(
        in_part.astype(BF16).reshape(dp, own_in, gw), out_part_w.astype(BF16).reshape(dp, own_out, model),
        normed_part.astype(BF16).reshape(quads, local, model), out_part.reshape(quads, local, model),
        small_in,
    )
    output = rows + op_own
    normed_grad = gn_own
    unit_grad = normed_grad * pre_full[None]
    input_grad = grad_rows.astype(F32) + inv_rms * (
        unit_grad - unit_rows * jnp.mean(unit_grad * unit_rows, -1, keepdims=True)
    )
    cuts = (0, width, 2 * width, 2 * width + bc_cols, 2 * width + bc_cols + own_heads)
    in_weight_grad = jnp.concatenate(
        [in_all[q, :, lo:hi] for lo, hi in zip(cuts[:-1], cuts[1:]) for q in range(quads)], 1
    ).astype(F32)
    out_weight_grad = out_all.reshape(width, model).astype(F32)
    n_x, n_b = width // 128, state2 // 128
    at = 6 * n_x
    by_channel = small_all[:, :at].reshape(quads, 6, width)
    conv_x_grad = jnp.moveaxis(by_channel[:, :4], 0, 1).reshape(4, inner)
    conv_x_bias_grad = by_channel[:, 4].reshape(inner)
    skip_grad = by_channel[:, 5].reshape(heads, -1).sum(-1)
    summed = small_all.sum(0)
    bc_grad = summed[at : at + 5 * n_b].reshape(5, state2)
    at += 5 * n_b
    head_grad = jnp.moveaxis(small_all[:, at : at + 2, :own_heads], 0, 1).reshape(2, heads)
    at += 2
    pre_sum = summed[at : at + model // 128].reshape(-1)
    at += model // 128
    norm_sum = small_all[:, at : at + n_x].reshape(-1)
    rank = lax.axis_index("dp")
    return (
        output[None], input_grad[None],
        lax.dynamic_slice_in_dim(pre_sum, rank * (model // dp), model // dp, 0), in_weight_grad,
        conv_x_grad, conv_x_bias_grad, bc_grad[:4], bc_grad[4], head_grad[0], head_grad[1], skip_grad,
        lax.dynamic_slice_in_dim(norm_sum, rank * (inner // dp), inner // dp, 0), out_weight_grad,
    )


def solution(mesh):
    dp, seq = mesh.shape["dp"], mesh.shape["seq"]
    fine = Mesh(mesh.devices.reshape(dp, 2, seq // 2), ("dp", "pair", "quad"))
    tokens, whole, rows = P("dp", ("pair", "quad"), None), P(), P("dp", None)
    return jax.shard_map(
        on_device,
        mesh=fine,
        in_specs=(
            tokens, P("dp"), rows, whole, whole, whole, whole, whole, whole, whole, P("dp"), rows, tokens,
        ),
        out_specs=(
            tokens, tokens, P("dp"), rows, whole, whole, whole, whole, whole, whole, whole, P("dp"), rows,
        ),
        check_vma=False,
    )
```

```python
import functools
import types

import jax
import jax.numpy as jnp
from jax import lax
from jax.experimental import pallas as pl
from jax.experimental.pallas import tpu as pltpu
from jax.sharding import Mesh
from jax.sharding import PartitionSpec as P

EPSILON = 1e-05
BLOCK = 256
HALO = 16
F32 = jnp.float32
BF16 = jnp.bfloat16
NN = ((1,), (0,))
NT = ((1,), (1,))
TN = ((0,), (0,))


def mm(a, b, dims=NN):
    return lax.dot_general(
        a.astype(BF16), b.astype(BF16), (dims, ((), ())), preferred_element_type=F32
    )


def split(a):
    high = a.astype(BF16)
    return high, (a - high.astype(F32)).astype(BF16)


def mm3(a, b, dims=NN):
    ah, al = split(a)
    bh, bl = split(b)
    return mm(ah, bh, dims) + (mm(ah, bl, dims) + mm(al, bh, dims))


def mm_exact(a, b, dims=NN):
    b0 = b.astype(BF16)
    r1 = b - b0.astype(F32)
    b1 = r1.astype(BF16)
    b2 = (r1 - b1.astype(F32)).astype(BF16)
    return mm(a, b0, dims) + (mm(a, b1, dims) + mm(a, b2, dims))


def mm_sum(a, b, dims=NN):
    ah, al = split(a)
    return mm(ah, b, dims) + mm(al, b, dims)


def sigmoid(v):
    return 1.0 / (1.0 + jnp.exp(-v))


def lane_mask(width, first):
    lane = lax.broadcasted_iota(jnp.int32, (1, 128), 1)
    return (lane < 64) if first else (lane >= 64)


def expand(v, pair):
    lane = lax.broadcasted_iota(jnp.int32, (1, 128), 1)
    return jnp.where(lane < 64, v[:, 2 * pair : 2 * pair + 1], v[:, 2 * pair + 1 : 2 * pair + 2])


def lower_mask():
    return lax.broadcasted_iota(jnp.int32, (BLOCK, BLOCK), 0) >= lax.broadcasted_iota(
        jnp.int32, (BLOCK, BLOCK), 1
    )


def head_indicator(pair):
    row = lax.broadcasted_iota(jnp.int32, (128, 128), 0)
    col = lax.broadcasted_iota(jnp.int32, (128, 128), 1)
    return (col == 2 * pair + row // 64).astype(BF16)


def conv_block(p_ref, row, col, w_ref, b_ref, wcol):
    raw = p_ref[pl.ds(row, BLOCK + HALO), col : col + 128].astype(F32)
    shifted = [raw[HALO - 3 + k : HALO - 3 + k + BLOCK] for k in range(4)]
    pre = b_ref[0:1, wcol : wcol + 128]
    for k in range(4):
        pre = pre + w_ref[k : k + 1, wcol : wcol + 128] * shifted[k]
    return pre, shifted


def run_hooks(hooks, at):
    for index, hook in hooks.items():
        pl.when(at == index)(hook)


def prep_pass(width, px_ref, pt_ref, pd_ref, wx_ref, bx_ref, wb_ref, bb_ref, dtb_ref, alog_ref,
              xs_ref, bc_ref, dt_ref, cum_ref, fin_ref, hooks):
    blocks = xs_ref.shape[0] // BLOCK
    rate = -jnp.exp(alog_ref[...])
    fin_ref[...] = jnp.zeros_like(fin_ref)

    def step(b, carry):
        row = pl.multiple_of(b * BLOCK, BLOCK)
        for c in range(2):
            pre, _ = conv_block(pt_ref, row, 128 * c, wb_ref, bb_ref, 128 * c)
            bc_ref[pl.ds(row, BLOCK), 128 * c : 128 * c + 128] = pre * sigmoid(pre)
        raw = pd_ref[pl.ds(row + HALO, BLOCK), :].astype(F32)
        raw = raw + dtb_ref[...]
        dt = jnp.maximum(raw, 0.0) + jnp.log1p(jnp.exp(-jnp.abs(raw)))
        cum = mm_exact(lower_mask().astype(F32), dt * rate)
        dt_ref[pl.ds(row, BLOCK), :] = dt
        cum_ref[pl.ds(row, BLOCK), :] = cum
        last = cum[BLOCK - 1 : BLOCK, :]
        weight = dt * jnp.exp(last - cum)
        decay = jnp.exp(last)
        keys_t = bc_ref[pl.ds(row, BLOCK), 0:128].T
        for pair in range(width // 128):
            cols = slice(128 * pair, 128 * pair + 128)
            pre, _ = conv_block(px_ref, row, 128 * pair, wx_ref, bx_ref, 128 * pair)
            xs = pre * sigmoid(pre)
            xs_ref[pl.ds(row, BLOCK), cols] = xs
            fin_ref[:, cols] = fin_ref[:, cols] * expand(decay, pair) + mm3(
                keys_t, xs * expand(weight, pair)
            )
        run_hooks(hooks, b)
        return carry

    lax.fori_loop(0, blocks, step, 0)


def inside_pass(width, xs_ref, bc_ref, dt_ref, cum_ref, yl_ref, hooks):
    def step(b, carry):
        rows = pl.ds(pl.multiple_of(b * BLOCK, BLOCK), BLOCK)
        dt, cum = dt_ref[rows, :], cum_ref[rows, :]
        cum_t = cum.T
        scores = mm3(bc_ref[rows, 128:256], bc_ref[rows, 0:128], NT)
        mask = lower_mask()
        for pair in range(width // 128):
            cols = slice(128 * pair, 128 * pair + 128)
            stepped = xs_ref[rows, cols] * expand(dt, pair)
            y = jnp.zeros((BLOCK, 128), F32)
            for half in range(2):
                h = 2 * pair + half
                spread = cum[:, h : h + 1] - cum_t[h : h + 1, :]
                table = jnp.exp(jnp.where(mask, spread, -1e30))
                part = jnp.where(lane_mask(128, half == 0), stepped, 0.0)
                y = y + mm3(scores * table, part)
            yl_ref[rows, cols] = y
        run_hooks(hooks, b)
        return carry

    lax.fori_loop(0, xs_ref.shape[0] // BLOCK, step, 0)


def outside_pass(
    width, xs_ref, bc_ref, dt_ref, cum_ref, skip_ref, y_ref, yl_ref, states_ref, s_ref, hooks
):
    def step(b, carry):
        rows = pl.ds(pl.multiple_of(b * BLOCK, BLOCK), BLOCK)
        dt, cum = dt_ref[rows, :], cum_ref[rows, :]
        last = cum[BLOCK - 1 : BLOCK, :]
        grow, decay = jnp.exp(cum), jnp.exp(last)
        weight = dt * jnp.exp(last - cum)
        queries = bc_ref[rows, 128:256]
        keys_t = bc_ref[rows, 0:128].T
        for pair in range(width // 128):
            cols = slice(128 * pair, 128 * pair + 128)
            xs = xs_ref[rows, cols]
            state = s_ref[:, cols]
            states_ref[b, :, cols] = state
            y = yl_ref[rows, cols] + expand(grow, pair) * mm3(queries, state)
            s_ref[:, cols] = state * expand(decay, pair) + mm3(keys_t, xs * expand(weight, pair))
            yl_ref[rows, cols] = y
            y_ref[rows, cols] = (y + skip_ref[0:1, cols] * xs).astype(BF16)
        run_hooks(hooks, b)
        return carry

    lax.fori_loop(0, xs_ref.shape[0] // BLOCK, step, 0)


MESH = pl.DeviceIdType.MESH


def bits_of(count):
    return [1 << i for i in range(count.bit_length() - 1)]


def bit_at(index, bit):
    return (index // bit) % 2


def flip(index, bits):
    for bit in bits:
        index = index + bit * (1 - 2 * bit_at(index, bit))
    return index


def subsets(bits):
    found = [frozenset()]
    for bit in bits:
        found = found + [f | {bit} for f in found]
    return found


class Links:
    def __init__(self, send, recv):
        self.send, self.recv, self.count, self.open = send, recv, 0, []

    def make(self, src, dst, target):
        index, self.count = self.count, self.count + 1
        return pltpu.make_async_remote_copy(
            src_ref=src, dst_ref=dst, send_sem=self.send.at[index], recv_sem=self.recv.at[index],
            device_id=target, device_id_type=MESH,
        )

    def stage(self, copies, after=None):
        def begin():
            for copy in copies:
                copy.start()
                self.open.append(lambda copy=copy: copy.wait_send())

        def end():
            for copy in copies:
                copy.wait_recv()
            if after is not None:
                after()

        return begin, end

    def stage_if(self, copy, sends, takes):
        def left():
            pl.when(sends)(copy.wait_send)

        def begin():
            pl.when(sends)(copy.start)
            self.open.append(left)

        def end():
            pl.when(takes)(copy.wait_recv)

        return begin, end

    def drain(self):
        for left in self.open:
            left()
        self.open = []


def meet(targets):
    barrier = pltpu.get_barrier_semaphore()
    for target in targets:
        pl.semaphore_signal(barrier, inc=1, device_id=target, device_id_type=MESH)
    pl.semaphore_wait(barrier, len(targets))


def neighbours(axis):
    me = lax.axis_index(axis)
    return [{axis: flip(me, (bit,))} for bit in bits_of(lax.axis_size(axis))]


class Flow:
    def __init__(self, links, stages):
        self.links, self.stages, self.at, self.sent = links, stages, -1, []

    def go(self):
        if 0 <= self.at < len(self.stages):
            self.stages[self.at][1]()
        self.at += 1
        if self.at < len(self.stages):
            before = len(self.links.open)
            self.stages[self.at][0]()
            self.sent += self.links.open[before:]

    def drain(self):
        for left in self.sent:
            left()
        done = {id(left) for left in self.sent}
        self.links.open = [left for left in self.links.open if id(left) not in done]
        self.sent = []

    def finish(self):
        while self.at < len(self.stages):
            self.go()


def step(*flows):
    for flow in flows:
        flow.go()


def finish(*flows):
    while any(flow.at < len(flow.stages) for flow in flows):
        for flow in flows:
            if flow.at < len(flow.stages):
                flow.go()


def add_rows(out, a, b):
    rows = out.shape[0]
    step = 16 if rows % 16 == 0 else 8

    @pl.loop(0, rows // step)
    def _(i):
        at = pl.ds(pl.multiple_of(i * step, step), step)
        out[at, :] = (a[at, :].astype(F32) + b[at, :].astype(F32)).astype(out.dtype)


def gather_stages(links, axis, order, own, slot):
    me = lax.axis_index(axis)
    held, stages = [frozenset()], []
    for bit in order:
        target = {axis: flip(me, (bit,))}
        stages.append(
            links.stage([
                links.make(slot(flip(me, f)) if f else own, slot(flip(me, f)), target) for f in held
            ])
        )
        held = held + [f | {bit} for f in held]
    return stages


def reduce_stages(links, axis, order, source, inbox, final=None):
    me = lax.axis_index(axis)
    base, stages = 0, []
    blocks = {f: source(flip(me, f)) for f in subsets(order)}
    for stage, bit in enumerate(order):
        keep = subsets(order[stage + 1 :])
        target = {axis: flip(me, (bit,))}
        boxes = [inbox(base + k) for k in range(len(keep))]
        outs = [final] if final is not None and stage == len(order) - 1 else boxes
        copies = [links.make(blocks[f | {bit}], box, target) for f, box in zip(keep, boxes)]

        def after(mine=[blocks[f] for f in keep], boxes=boxes, outs=outs):
            for a, b, out in zip(mine, boxes, outs):
                add_rows(out, a, b)

        stages.append(links.stage(copies, after))
        blocks = dict(zip(keep, outs))
        base += len(keep)
    return stages


def spread_stages(links, order, block):
    d, q = lax.axis_index("dp"), lax.axis_index("quad")
    away = {bit: bit_at(d, bit) != bit_at(q, bit) for bit in order}
    stages = []
    for stage, bit in enumerate(order):
        reached = jnp.bool_(True)
        for later in order[stage + 1 :]:
            reached = jnp.logical_and(reached, jnp.logical_not(away[later]))
        holder = jnp.logical_and(reached, jnp.logical_not(away[bit]))
        taker = jnp.logical_and(reached, away[bit])
        copy = links.make(block, block, {"dp": flip(d, (bit,))})
        stages.append(links.stage_if(copy, holder, taker))
    return stages


def leave_pass(width, bc_ref, cum_ref, gy_ref, out_ref):
    blocks = gy_ref.shape[0] // BLOCK
    out_ref[...] = jnp.zeros_like(out_ref)

    def step(i, carry):
        rows = pl.ds(pl.multiple_of((blocks - 1 - i) * BLOCK, BLOCK), BLOCK)
        cum = cum_ref[rows, :]
        grow, decay = jnp.exp(cum), jnp.exp(cum[BLOCK - 1 : BLOCK, :])
        queries_t = bc_ref[rows, 128:256].T
        for pair in range(width // 128):
            cols = slice(128 * pair, 128 * pair + 128)
            dy = gy_ref[rows, cols].astype(F32)
            out_ref[:, cols] = out_ref[:, cols] * expand(decay, pair) + mm3(
                queries_t, expand(grow, pair) * dy
            )
        return carry

    lax.fori_loop(0, blocks, step, 0)


def back_inside_pass(width, r, hooks):
    def step(b, carry):
        rows = pl.ds(pl.multiple_of(b * BLOCK, BLOCK), BLOCK)
        dt, cum = r.dt[rows, :], r.cum[rows, :]
        cum_t = cum.T
        keys, queries = r.bc[rows, 0:128], r.bc[rows, 128:256]
        scores = mm3(queries, keys, NT)
        mask = lower_mask()
        r.dscore[...] = jnp.zeros_like(r.dscore)
        for pair in range(width // 128):
            cols = slice(128 * pair, 128 * pair + 128)
            stepped, stepped_low = split(r.xs[rows, cols] * expand(dt, pair))
            dy = r.y[rows, cols].astype(F32)
            dstep = jnp.zeros((BLOCK, 128), F32)
            for half in range(2):
                h = 2 * pair + half
                spread = cum[:, h : h + 1] - cum_t[h : h + 1, :]
                table = jnp.exp(jnp.where(mask, spread, -1e30))
                part = jnp.where(lane_mask(128, half == 0), dy, 0.0).astype(BF16)
                dmix = mm(part, stepped, NT) + mm(part, stepped_low, NT)
                r.dscore[...] += dmix * table
                high, low = split(scores * table)
                dstep = dstep + (mm(high, part, TN) + mm(low, part, TN))
            r.gm[rows, cols] = dstep
        r.dbc[rows, 0:128] = mm3(r.dscore[...], queries, TN)
        r.dbc[rows, 128:256] = mm3(r.dscore[...], keys)
        run_hooks(hooks, b)
        return carry

    lax.fori_loop(0, r.y.shape[0] // BLOCK, step, 0)


def back_outside_pass(width, r, hooks):
    blocks = r.y.shape[0] // BLOCK
    rate = -jnp.exp(r.alog[...])
    r.heads[...] = jnp.zeros_like(r.heads)

    def step(i, carry):
        b = blocks - 1 - i
        row = pl.multiple_of(b * BLOCK, BLOCK)
        rows = pl.ds(row, BLOCK)
        dt, cum = r.dt[rows, :], r.cum[rows, :]
        last = cum[BLOCK - 1 : BLOCK, :]
        grow, decay, tail = jnp.exp(cum), jnp.exp(last), jnp.exp(last - cum)
        keys, queries = r.bc[rows, 0:128], r.bc[rows, 128:256]
        queries_t = queries.T
        dkeys, dqueries = r.dbc[rows, 0:128], r.dbc[rows, 128:256]
        dcum = jnp.zeros((BLOCK, 128), F32)
        ddt = jnp.zeros((BLOCK, 128), F32)
        dlast = jnp.zeros((8, 128), F32)
        dskip = jnp.zeros((8, 128), F32)
        for pair in range(width // 128):
            cols = slice(128 * pair, 128 * pair + 128)
            xs = r.xs[rows, cols]
            dt_e = expand(dt, pair)
            stepped = xs * dt_e
            dy = r.y[rows, cols].astype(F32)
            state, ds = r.states[b, :, cols], r.ds[:, cols]
            tail_e = expand(tail, pair)
            carried = mm3(keys, ds) * tail_e
            dstep = r.gm[rows, cols] + carried
            dkeys = dkeys + mm3(stepped * tail_e, ds, NT)
            grown = expand(grow, pair) * dy
            dqueries = dqueries + mm3(grown, state, NT)
            decay_e = expand(decay, pair)
            ends = jnp.sum(stepped * carried, 0, keepdims=True) + decay_e * jnp.sum(
                ds * state, 0, keepdims=True
            )
            r.ds[:, cols] = ds * decay_e + mm3(queries_t, grown)
            dxs = dstep * dt_e + r.skip[0:1, cols] * dy
            which = head_indicator(pair)
            ddt = ddt + mm_sum(dstep * xs, which)
            dcum = dcum + mm_sum(dy * r.yl[rows, cols] - stepped * dstep, which)
            dlast = dlast + mm_sum(jnp.broadcast_to(ends, (8, 128)), which)
            skips = jnp.sum(dy * xs, 0, keepdims=True)
            dskip = dskip + mm_sum(jnp.broadcast_to(skips, (8, 128)), which)
            pre, shifted = conv_block(r.px, row, 128 * pair, r.wxc, r.bxc, 128 * pair)
            sig = sigmoid(pre)
            dpre = dxs * sig * (1.0 + pre * (1.0 - sig))
            r.xs[rows, cols] = dpre
            for k in range(4):
                r.sx[k : k + 1, cols] += jnp.sum(dpre * shifted[k], 0, keepdims=True)
            r.sx[4:5, cols] += jnp.sum(dpre, 0, keepdims=True)
        at_end = lax.broadcasted_iota(jnp.int32, (BLOCK, 128), 0) == BLOCK - 1
        dcum = dcum + jnp.where(at_end, dlast[0:1], 0.0)
        dlog = mm_exact(lower_mask().astype(F32), dcum, TN)
        raw = r.pd[pl.ds(row + HALO, BLOCK), :].astype(F32)
        draw = (ddt + dlog * rate) * sigmoid(raw + r.dtb[...])
        r.gdt[rows, :] = draw.astype(BF16)
        r.heads[0:1, :] += jnp.sum(draw, 0, keepdims=True)
        r.heads[1:2, :] += jnp.sum(dlog * dt, 0, keepdims=True) * rate
        r.heads[2:3, :] += dskip[0:1]
        for c, grad in enumerate((dkeys, dqueries)):
            cols = slice(128 * c, 128 * c + 128)
            pre, shifted = conv_block(r.pt, row, 128 * c, r.wbc, r.bbc, 128 * c)
            sig = sigmoid(pre)
            dpre = grad * sig * (1.0 + pre * (1.0 - sig))
            r.dbc[rows, cols] = dpre
            for k in range(4):
                r.sb[k : k + 1, cols] += jnp.sum(dpre * shifted[k], 0, keepdims=True)
            r.sb[4:5, cols] += jnp.sum(dpre, 0, keepdims=True)
        run_hooks(hooks, i)
        return carry

    lax.fori_loop(0, blocks, step, 0)


INPUTS = (
    "win", "wo_in", "hid_in", "og_in", "gain_in", "wxc", "bxc", "wbc", "bbc", "dtb", "alog", "skip",
)
OUTPUTS = (
    "in_out", "out_out", "op_own", "gn_own", "cxw", "cxb", "norm", "cbw", "cbb", "head", "pre", "pre_gain",
)
SCRATCH = (
    "wz", "wx", "wt", "wo", "xn", "og", "hid", "px", "pt", "pd", "xs", "bc", "dt", "cum", "y", "yl", "states", "z", "gm", "mixed", "dbc", "gdt", "bcs", "bcbox", "bcall", "tail", "wtail", "grad", "gradt", "zbox", "zpair", "xpair", "tbox", "tpair", "obox", "opair", "opbox", "ttot", "tstage", "gain", "halo", "fin", "enter", "ds", "stat", "statbox", "dscore", "heads", "sx", "sb", "sp", "sxbox", "sbbox", "spbox", "sxall", "sball", "spall", "hx", "hb", "dsin", "send", "recv", "local",
)


def block_kernel(width, own_heads, heads, *refs):
    r = types.SimpleNamespace(**dict(zip((*INPUTS, *OUTPUTS, *SCRATCH), refs, strict=True)))
    d, q, p = lax.axis_index("dp"), lax.axis_index("quad"), lax.axis_index("pair")
    dps, quads = lax.axis_size("dp"), lax.axis_size("quad")
    tokens, piece, model = r.y.shape[0], r.hid.shape[1], r.hid.shape[2]
    inner, share, state2 = width * quads, model // dps, r.bc.shape[1]
    bc_cols = state2 // quads
    links = Links(r.send, r.recv)
    dp_bits, up = bits_of(dps), bits_of(quads)
    orders, down = (dp_bits, dp_bits[::-1]), up[::-1]
    other, swapped = {"pair": flip(p, (1,))}, {"dp": q, "quad": d}
    near = neighbours("dp") + neighbours("quad") + neighbours("pair")
    sides = ((0, width // 2), (width // 2, width // 2))
    tail_rows = r.win.shape[0] - 2 * inner
    cut = tail_rows // 32 * 16 + 16
    tail_sides = ((0, cut), (cut, tail_rows - cut))
    lane_row = lax.broadcasted_iota(jnp.int32, (128, 128), 0)
    lane_col = lax.broadcasted_iota(jnp.int32, (128, 128), 1)
    first_half, second_half = p == 0, p > 0

    @pl.when(d == q)
    def _():
        meet(near)

    @pl.when(d != q)
    def _():
        meet([*near, swapped])

    def win_rows(base, at, size):
        return r.win.at[pl.ds(pl.multiple_of(base + q * width + at, 16), size)]

    def tail_source(at, size):
        return r.win.at[pl.ds(2 * inner + at, size)]

    def weights(source, out, parts):
        return [
            Flow(links, gather_stages(
                links, "dp", order, source(at, size),
                lambda i, at=at, size=size: out.at[i, pl.ds(at, size)],
            ))
            for order, (at, size) in zip(orders, parts)
        ]

    gain_flow = Flow(links, gather_stages(links, "dp", dp_bits, r.gain_in, lambda i: r.gain.at[i]))
    hid_flow = Flow(links, gather_stages(links, "quad", down, r.hid_in, lambda i: r.hid.at[i]))
    og_flow = Flow(links, gather_stages(links, "quad", down, r.og_in, lambda i: r.og.at[i]))
    wt_flows = weights(tail_source, r.wt, tail_sides)
    wx_flows = weights(lambda at, size: win_rows(inner, at, size), r.wx, sides)
    wz_flows = weights(lambda at, size: win_rows(0, at, size), r.wz, sides)
    parts = 4
    wo_flows = [
        Flow(links, spread_stages(links, dp_bits[::-1], r.wo.at[pl.ds(k * (width // parts), width // parts)]))
        for k in range(parts)
    ]
    tail = r.hid.at[quads - 1, pl.ds(piece - HALO, HALO)]
    halo_flow = Flow(links, [links.stage_if(links.make(tail, r.halo, other), first_half, second_half)])
    state_flow = Flow(links, [links.stage_if(links.make(r.fin, r.enter, other), first_half, second_half)])
    ds_flow = Flow(links, [links.stage_if(links.make(r.fin, r.dsin, other), second_half, first_half)])
    edge_flows = [
        Flow(links, [links.stage_if(links.make(a.at[pl.ds(0, 8)], b, other), second_half, first_half)])
        for a, b in ((r.xs, r.hx), (r.dbc, r.hb))
    ]
    stat_flow = Flow(links, [
        links.stage(
            [links.make(r.stat.at[k], r.statbox.at[k], {"quad": flip(q, (bit,))})],
            lambda k=k: r.stat.at[k + 1].__setitem__(..., r.stat[k] + r.statbox[k]),
        )
        for k, bit in enumerate(up)
    ])
    kept = []

    def keeper(own, place, index):
        return pltpu.make_async_copy(own, place, r.local.at[index])

    def in_flow(h, at, size, part_ref, box, pair_box, slot, index):
        rows = pl.ds(at, size)
        stages = reduce_stages(
            links, "dp", orders[h], lambda i: part_ref.at[i, rows], lambda k: box.at[k, rows]
        )
        mine, own = box.at[dps - 2, rows], pair_box.at[rows]
        keep = keeper(own, slot(q), index)

        def after():
            add_rows(own, mine, own)
            keep.start()
            kept.append(keep)

        stages.append(links.stage([links.make(mine, own, other)], after))
        return Flow(links, stages + gather_stages(links, "quad", down, own, slot))

    def columns_slot(base, at, size):
        return lambda i: r.in_out.at[pl.ds(pl.multiple_of(base + i * width + at, 16), size)]

    def out_flow(h):
        half = model // 2
        part, size = pl.ds(h * half, half), width // dps
        stages = reduce_stages(
            links, "dp", orders[h],
            lambda i: r.wo.at[pl.ds(pl.multiple_of(i * size, 16), size), part],
            lambda k: r.obox.at[h, k],
        )
        mine, whole = r.obox.at[h, dps - 2], r.opair.at[h]
        place = r.out_out.at[d, :, part]
        stages.append(
            links.stage([links.make(mine, whole, other)], lambda: add_rows(whole, mine, whole))
        )
        near_copy = pltpu.make_async_copy(whole, place, r.local.at[14 + h])
        far_copy = links.make(whole, place, swapped)

        def begin():
            pl.when(d == q)(near_copy.start)
            pl.when(d != q)(far_copy.start)

        def end():
            pl.when(d == q)(near_copy.wait)
            pl.when(d != q)(far_copy.wait)

        stages.append((begin, end))
        return Flow(links,
            stages
            + gather_stages(
                links, "quad", down, r.out_out.at[q, :, part], lambda i: r.out_out.at[i, :, part]
            )
        )

    def row_sum_flow(source, box, final):
        return Flow(links, reduce_stages(
            links, "quad", up, lambda i: source.at[i], lambda k: box.at[k], final
        ))

    def small_flow(mine, box, every):
        current, stages = mine, []
        steps = [("dp", bit) for bit in dp_bits] + [("pair", 1)]
        for k, (axis, bit) in enumerate(steps):
            target = {axis: flip(lax.axis_index(axis), (bit,))}
            out = box.at[k] if k < len(steps) - 1 else every.at[q]

            def after(out=out, current=current, k=k):
                out[...] = current[...] + box[k]

            stages.append(links.stage([links.make(current, box.at[k], target)], after))
            current = out
        return Flow(links,
            stages + gather_stages(links, "quad", down, every.at[q], lambda i: every.at[i])
        )

    z_flows = [
        in_flow(h, at, size, r.grad, r.zbox, r.zpair, columns_slot(0, at, size), 7 + h)
        for h, (at, size) in enumerate(sides)
    ]
    x_flows = [
        in_flow(h, at, size, r.grad, r.zbox, r.xpair, columns_slot(inner, at, size), 9 + h)
        for h, (at, size) in enumerate(sides)
    ]
    t_flow = in_flow(0, 0, 128, r.gradt, r.tbox, r.tpair, lambda i: r.ttot.at[i], 11)
    out_flows = [out_flow(0), out_flow(1)]
    op_flow = row_sum_flow(r.hid, r.opbox, r.op_own)
    gn_flow = row_sum_flow(r.og, r.opbox, r.gn_own)
    bc_flow = Flow(links,
        reduce_stages(links, "quad", up, lambda i: r.bcs.at[i], lambda k: r.bcbox.at[k], r.bcall.at[q])
        + gather_stages(links, "quad", down, r.bcall.at[q], lambda i: r.bcall.at[i])
    )
    sx_flow, sb_flow, sp_flow = (
        small_flow(r.sx, r.sxbox, r.sxall), small_flow(r.sb, r.sbbox, r.sball),
        small_flow(r.sp, r.spbox, r.spall),
    )

    step(gain_flow, hid_flow, *wt_flows, *wx_flows)
    owned = [
        (r.hid_in, r.hid.at[q]), (r.gain_in, r.gain.at[d]),
        (tail_source(0, tail_rows), r.wt.at[d, pl.ds(0, tail_rows)]),
        (win_rows(inner, 0, width), r.wx.at[d]), (win_rows(0, 0, width), r.wz.at[d]),
        (r.og_in, r.og.at[q]),
    ]
    copies = [pltpu.make_async_copy(a, b, r.local.at[i]) for i, (a, b) in enumerate(owned)]
    for copy in copies:
        copy.start()

    @pl.when(d == q)
    def _():
        copy = pltpu.make_async_copy(r.wo_in, r.wo, r.local.at[len(owned)])
        copy.start()
        copy.wait()

    for i in range(dps):
        r.wt[i, tail_rows:, :] = jnp.zeros((r.wt.shape[1] - tail_rows, share), BF16)
    r.sx[...] = jnp.zeros_like(r.sx)
    r.sb[...] = jnp.zeros_like(r.sb)
    for copy in copies:
        copy.wait()
    finish(gain_flow)
    step(hid_flow, *wt_flows, *wx_flows)
    step(*wz_flows, og_flow)
    step(*wo_flows)
    hid_flow.finish()
    step(halo_flow)
    halo_flow.finish()

    gains = r.gain[0]
    for i in range(1, dps):
        gains = gains + r.gain[i]
    pre = gains[:, :model]
    r.pre_gain[...] = pre

    def normed(v):
        v = v.astype(F32)
        unit = v * lax.rsqrt(jnp.mean(v * v, -1, keepdims=True) + EPSILON)
        return (unit * pre).astype(BF16)

    def put_normed(at, rows, v):
        for i in range(dps):
            r.xn[i, pl.ds(at, rows), :] = v[:, i * share : (i + 1) * share]

    put_normed(0, HALO, jnp.where(p > 0, normed(r.halo[...]), jnp.zeros((HALO, model), BF16)))
    few = 32

    @pl.loop(0, tokens // few)
    def _(i):
        at = i * few
        rows = pl.ds(pl.multiple_of(at % piece, few), few)
        put_normed(pl.multiple_of(at + HALO, 16), few, normed(r.hid[at // piece, rows, :]))

    finish(*wt_flows, *wx_flows)

    def project(out_ref, out_at, at, rows, w_ref):
        total = jnp.zeros((rows, w_ref.shape[1]), F32)
        for i in range(dps):
            total = total + mm(r.xn[i, pl.ds(at, rows), :], w_ref[i], NT)
        out_ref[pl.ds(out_at, rows), :] = total.astype(BF16)

    for out_ref, w_ref in ((r.pt, r.wt), (r.px, r.wx)):
        project(out_ref, 0, 0, HALO, w_ref)

        @pl.loop(0, tokens // BLOCK)
        def _(i, out_ref=out_ref, w_ref=w_ref):
            at = pl.multiple_of(i * BLOCK + HALO, 16)
            project(out_ref, at, at, BLOCK, w_ref)

    pick = jnp.logical_and(lane_row == lane_col + q * own_heads, lane_col < own_heads).astype(BF16)
    r.pd[...] = mm(r.pt[:, state2 : state2 + 128], pick).astype(BF16)
    prep_pass(
        width, r.px, r.pt, r.pd, r.wxc, r.bxc, r.wbc, r.bbc, r.dtb, r.alog,
        r.xs, r.bc, r.dt, r.cum, r.fin, {0: lambda: step(*wz_flows, og_flow), 3: wo_flows[0].go},
    )
    step(state_flow)
    inside_pass(
        width, r.xs, r.bc, r.dt, r.cum, r.yl, {1: wo_flows[1].go, 3: wo_flows[2].go},
    )
    state_flow.finish()
    r.ds[...] = jnp.where(p > 0, r.enter[...], 0.0)
    outside_pass(
        width, r.xs, r.bc, r.dt, r.cum, r.skip, r.y, r.yl, r.states, r.ds, {1: wo_flows[3].go},
    )
    finish(*wz_flows)

    @pl.loop(0, tokens // BLOCK)
    def _(i):
        at = pl.multiple_of(i * BLOCK, BLOCK)
        project(r.z, at, pl.multiple_of(at + HALO, 16), BLOCK, r.wz)

    finish(og_flow, *wo_flows)

    @pl.loop(0, quads)
    def _(i):
        r.gm[pl.ds(pl.multiple_of(i * piece, piece), piece), :] = mm(r.og[i], r.wo[...], NT)

    norm_all = gains[:, model:]
    norm_own = norm_all[:, :width]
    for i in range(1, quads):
        norm_own = jnp.where(q == i, norm_all[:, i * width : (i + 1) * width], norm_own)
    chunk = 128

    @pl.loop(0, tokens // chunk)
    def _(i):
        rows = pl.ds(pl.multiple_of(i * chunk, chunk), chunk)
        gate = r.z[rows, :].astype(F32)
        gated = r.y[rows, :].astype(F32) * gate * sigmoid(gate)
        first = jnp.sum(gated * gated, -1, keepdims=True)
        second = jnp.sum(r.gm[rows, :] * norm_own * gated, -1, keepdims=True)
        lane = lax.broadcasted_iota(jnp.int32, (chunk, 128), 1)
        both = jnp.where(lane == 0, first, jnp.where(lane == 1, second, 0.0))
        r.stat[0, :, rows] = both.T[0:8, :]

    finish(stat_flow)

    @pl.loop(0, tokens // chunk)
    def _(i):
        rows = pl.ds(pl.multiple_of(i * chunk, chunk), chunk)
        stats = r.stat[len(up), :, rows]
        stats = jnp.concatenate([stats] * (128 // 8), 0).T
        out_rms = lax.rsqrt(stats[:, 0:1] / inner + EPSILON)
        mean_dot = out_rms * stats[:, 1:2] / inner
        gate = r.z[rows, :].astype(F32)
        y = r.y[rows, :].astype(F32)
        sig = sigmoid(gate)
        unit_gated = y * gate * sig * out_rms
        grad_mixed = r.gm[rows, :]
        r.mixed[rows, :] = (unit_gated * norm_own).astype(BF16)
        r.sx[5:6, :] += jnp.sum(grad_mixed * unit_gated, 0, keepdims=True)
        grad_gated = out_rms * (grad_mixed * norm_own - unit_gated * mean_dot)
        r.y[rows, :] = (grad_gated * gate * sig).astype(BF16)
        r.z[rows, :] = (grad_gated * y * sig * (1.0 + gate * (1.0 - sig))).astype(BF16)

    def weight_grad(grad_ref, out_ref):
        for i in range(dps):
            out_ref[i] = mm(grad_ref[...], r.xn[i, pl.ds(HALO, tokens), :], TN).astype(BF16)

    links.drain()

    @pl.loop(0, quads)
    def _(i):
        rows = pl.ds(pl.multiple_of(i * piece, piece), piece)
        r.hid[i] = mm(r.mixed[rows, :], r.wo[...]).astype(BF16)

    step(op_flow)
    weight_grad(r.z, r.grad)
    op_flow.go()
    step(*z_flows)
    leave_pass(width, r.bc, r.cum, r.y, r.fin)
    step(ds_flow)
    size = BLOCK if width % BLOCK == 0 else 128

    @pl.loop(0, width // size)
    def _(i):
        cols = pl.ds(pl.multiple_of(i * size, size), size)
        total = jnp.zeros((size, model), F32)
        for k in range(quads):
            total = total + mm(r.mixed[k * piece : (k + 1) * piece, cols], r.og[k], TN)
        r.wo[cols, :] = total.astype(BF16)

    step(*z_flows, *out_flows)
    back_inside_pass(width, r, {1: lambda: step(*z_flows)})
    ds_flow.finish()
    r.ds[...] = jnp.where(p > 0, 0.0, r.dsin[...])
    back_outside_pass(
        width, r, {1: lambda: step(*out_flows), 3: lambda: step(*out_flows)},
    )
    step(*edge_flows)
    r.sb[5:6, 0:128], r.sb[6:7, 0:128], r.sb[7:8, 0:128] = r.heads[0:1], r.heads[1:2], r.heads[2:3]
    op_flow.finish()
    op_flow.drain()
    for flow in z_flows:
        flow.drain()
    step(*z_flows)
    step(sx_flow, sb_flow)
    finish(*edge_flows)
    r.xs[pl.ds(tokens, 8), :] = jnp.where(p > 0, 0.0, r.hx[...])
    r.dbc[pl.ds(tokens, 8), :] = jnp.where(p > 0, 0.0, r.hb[...])

    def unconv(source, row, cols, w_ref):
        wide = source[pl.ds(row, chunk + 8), cols]
        total = jnp.zeros((chunk, 128), F32)
        for k in range(4):
            total = total + w_ref[k : k + 1, cols] * wide[3 - k : 3 - k + chunk]
        return total

    @pl.loop(0, tokens // chunk)
    def _(i):
        row = pl.multiple_of(i * chunk, chunk)
        inside = pl.ds(pl.multiple_of(row % piece, chunk), chunk)
        for c in range(2):
            cols = slice(128 * c, 128 * c + 128)
            r.bcs[row // piece, inside, cols] = unconv(r.dbc, row, cols, r.wbc)
        for pair in range(width // 128):
            cols = slice(128 * pair, 128 * pair + 128)
            r.mixed[pl.ds(row, chunk), cols] = unconv(r.xs, row, cols, r.wxc).astype(BF16)

    step(bc_flow)
    weight_grad(r.mixed, r.grad)
    for _ in dp_bits:
        step(sx_flow)
    step(*x_flows, bc_flow)
    row = lax.broadcasted_iota(jnp.int32, (state2, 128), 0)
    col = lax.broadcasted_iota(jnp.int32, (state2, 128), 1)
    from_bc = jnp.logical_and(row == col + q * bc_cols, col < bc_cols).astype(BF16)
    from_dt = jnp.logical_and(lane_col == lane_row + bc_cols, lane_row < own_heads).astype(BF16)

    wide_rows = r.wt.shape[1]
    row = lax.broadcasted_iota(jnp.int32, (128, wide_rows), 0)
    col = lax.broadcasted_iota(jnp.int32, (128, wide_rows), 1)

    def dt_rows(i):
        return jnp.logical_and(
            jnp.logical_and(row >= bc_cols, row < bc_cols + own_heads),
            col == state2 + i * own_heads + row - bc_cols,
        )

    def bc_rows(i):
        return jnp.logical_and(row < bc_cols, col == row + i * bc_cols)

    take = dt_rows(q).astype(BF16)
    for i in range(dps):
        r.wtail[i] = mm(take, r.wt[i]).astype(BF16)
    r.tail[...] = mm(r.gdt[...], from_dt).astype(BF16)
    r.sp[...] = jnp.zeros_like(r.sp)

    def grad_rows(k, carry):
        at = pl.multiple_of(k * chunk, chunk)
        rows = pl.ds(at, chunk)
        inside = pl.ds(pl.multiple_of(at % piece, chunk), chunk)
        gz, gx, gt = r.z[rows, :], r.mixed[rows, :], r.tail[rows, :]
        for i in range(dps):
            grad = mm(gz, r.wz[i]) + mm(gx, r.wx[i]) + mm(gt, r.wtail[i])
            cols = slice(i * share, (i + 1) * share)
            unit = r.xn[i, pl.ds(pl.multiple_of(at + HALO, 16), chunk), :].astype(F32)
            r.sp[:, cols] += jnp.sum(grad * unit, 0, keepdims=True)
            r.og[at // piece, inside, cols] = grad.astype(BF16)
        return carry

    lax.fori_loop(0, tokens // chunk, grad_rows, 0)
    step(gn_flow, bc_flow, *x_flows)
    step(gn_flow)
    finish(bc_flow)
    step(*x_flows)

    @pl.loop(0, quads)
    def _(i):
        rows = pl.ds(pl.multiple_of(i * piece, piece), piece)
        r.tail[rows, :] = (mm(r.bcall[i], from_bc) + mm(r.gdt[rows, :], from_dt)).astype(BF16)

    weight_grad(r.tail, r.gradt)
    step(t_flow, sb_flow, sx_flow, *out_flows)
    own_bc = r.bcall[q]
    for i in range(dps):
        cols = slice(i * share, (i + 1) * share)
        grad = mm(own_bc, r.wt[i, 0:state2, :])
        at = pl.ds(pl.multiple_of(q * piece + HALO, 16), piece)
        r.sp[:, cols] += jnp.sum(grad * r.xn[i, at, :].astype(F32), 0, keepdims=True)
        r.yl[i * piece : (i + 1) * piece, 0:share] = grad
    r.sp[...] = r.sp[...] / pre
    step(sp_flow)
    finish(t_flow, sp_flow, sx_flow, sb_flow, *z_flows, *out_flows, *x_flows, gn_flow)
    for i in range(dps):
        cols = slice(i * share, (i + 1) * share)
        r.gn_own[:, cols] += r.yl[i * piece : (i + 1) * piece, 0:share]

    for copy in kept:
        copy.wait()
    for i in range(quads):
        place = jnp.logical_or(bc_rows(i), dt_rows(i)).astype(BF16)
        piece_t = mm(place, r.ttot[i], TN)
        r.tstage[...] = piece_t.astype(BF16) if i == 0 else (r.tstage[...].astype(F32) + piece_t).astype(BF16)
    last = keeper(r.tstage.at[pl.ds(0, tail_rows)], r.in_out.at[pl.ds(2 * inner, tail_rows)], 12)
    last.start()
    for i in range(quads):
        cols = slice(i * width, (i + 1) * width)
        r.cxw[:, cols] = r.sxall[i, 0:4, :]
        r.cxb[:, cols] = r.sxall[i, 4:5, :]
        r.norm[:, cols] = r.sxall[i, 5:6, :]
    total = r.sball[0]
    every = r.spall[0]
    lane = lax.broadcasted_iota(jnp.int32, (8, 128), 1)
    packed = jnp.where(lane < own_heads, r.sball[0, :, 0:128], 0.0)
    for i in range(1, quads):
        total = total + r.sball[i]
        every = every + r.spall[i]
        moved = jnp.where(lane < own_heads, r.sball[i, :, 0:128], 0.0)
        packed = packed + pltpu.roll(moved, i * own_heads, 1)
    r.cbw[...] = total[0:4]
    r.cbb[...] = total[4:5]
    r.head[...] = packed
    r.pre[...] = every
    last.wait()
    links.drain()


def remote_call(kernel, ident, outs, any_inputs, any_outputs, scratch, flops=2 * 10**10):
    vmem, anywhere = pl.BlockSpec(memory_space=pltpu.VMEM), pl.BlockSpec(memory_space=pltpu.HBM)

    def run(*args):
        moved = sum(a.size * a.dtype.itemsize for a in (*args, *outs))
        return pl.pallas_call(
            kernel,
            out_shape=tuple(outs),
            in_specs=[anywhere if i in any_inputs else vmem for i in range(len(args))],
            out_specs=tuple([anywhere if i in any_outputs else vmem for i in range(len(outs))]),
            scratch_shapes=list(scratch),
            compiler_params=pltpu.CompilerParams(
                vmem_limit_bytes=67043328, collective_id=ident, has_side_effects=True
            ),
            cost_estimate=pl.CostEstimate(flops=flops, bytes_accessed=moved, transcendentals=0),
        )(*args)

    return run


def on_device(
    hidden_in, pre_gain, in_weight, conv_x_weight, conv_x_bias, conv_bc_weight, conv_bc_bias,
    dt_bias, a_log, skip, norm_gain, out_weight, output_gradient,
):
    dp, quads, rank = lax.axis_size("dp"), lax.axis_size("quad"), lax.axis_index("dp")
    quad = lax.axis_index("quad")
    _, local, model = hidden_in.shape
    inner, state2, heads = conv_x_bias.shape[0], conv_bc_bias.shape[0], dt_bias.shape[0]
    width, own_heads = inner // quads, heads // quads
    tokens, share, columns = local * quads, model // dp, in_weight.shape[1]

    def own(v, n, axis):
        return lax.dynamic_slice_in_dim(v, quad * n, n, axis)

    def spaced(v):
        return lax.dynamic_update_slice_in_dim(
            jnp.zeros((v.shape[0] * dp,), F32), v.astype(F32), rank * v.shape[0], 0
        )

    def pad_heads(v):
        return jnp.pad(own(v, own_heads, 0), (0, 128 - own_heads))[None]

    gain_row = jnp.concatenate([spaced(pre_gain), spaced(norm_gain)])[None]
    skip_own = jnp.repeat(own(skip, own_heads, 0), width // own_heads)[None]
    tail_rows = columns - 2 * inner
    tail_wide = tail_rows + -tail_rows % 128

    def sds(shape, dtype=F32):
        return jax.ShapeDtypeStruct(shape, dtype)

    def vm(*shape):
        return pltpu.VMEM(shape, F32)

    def vb(*shape):
        return pltpu.VMEM(shape, BF16)

    rows, own_out, steps = HALO + tokens, width // dp, len(bits_of(dp)) + 1
    levels = len(bits_of(quads))
    scratch = dict(
        wz=vb(dp, width, share), wx=vb(dp, width, share), wt=vb(dp, tail_wide, share),
        wo=vb(width, model), xn=vb(dp, rows, share), og=vb(quads, local, model),
        hid=vb(quads, local, model), px=vb(rows, width), pt=vb(rows, tail_wide), pd=vb(rows, 128),
        xs=vm(tokens + 8, width), bc=vm(tokens, state2), dt=vm(tokens, 128), cum=vm(tokens, 128),
        y=vb(tokens, width), yl=vm(tokens, width), states=vm(tokens // BLOCK, 128, width),
        z=vb(tokens, width), gm=vm(tokens, width), mixed=vb(tokens, width),
        dbc=vm(tokens + 8, state2), gdt=vb(tokens, 128), bcs=vm(quads, local, state2),
        bcbox=vm(quads - 1, local, state2), bcall=vb(quads, local, state2), tail=vb(tokens, 128),
        wtail=vb(dp, 128, share), grad=vb(dp, width, share), gradt=vb(dp, 128, share),
        zbox=vb(dp - 1, width, share), zpair=vb(width, share),
        xpair=vb(width, share),
        tbox=vb(dp - 1, 128, share), tpair=vb(128, share),
        obox=vb(2, dp - 1, own_out, model // 2), opair=vb(2, own_out, model // 2),
        opbox=vb(quads - 1, local, model),
        ttot=vb(quads, 128, share), tstage=vb(tail_wide, share),
        gain=vm(dp, *gain_row.shape), halo=vb(HALO, model), fin=vm(128, width), enter=vm(128, width),
        ds=vm(128, width), stat=vm(levels + 1, 8, tokens), statbox=vm(levels, 8, tokens),
        dscore=vm(BLOCK, BLOCK), heads=vm(8, 128), sx=vm(8, width), sb=vm(8, state2), sp=vm(1, model),
        sxbox=vm(steps, 8, width), sbbox=vm(steps, 8, state2), spbox=vm(steps, 1, model),
        sxall=vm(quads, 8, width), sball=vm(quads, 8, state2), spall=vm(quads, 1, model),
        hx=vm(8, width), hb=vm(8, state2), dsin=vm(128, width),
        send=pltpu.SemaphoreType.DMA((192,)), recv=pltpu.SemaphoreType.DMA((192,)),
        local=pltpu.SemaphoreType.DMA((16,)),
    )
    (
        in_out, out_out, op_own, gn_own, conv_x_grad, conv_x_bias_grad, norm_grad, conv_bc_grad,
        conv_bc_bias_grad, head_grad, pre_grad, pre_full,
    ) = remote_call(
        functools.partial(block_kernel, width, own_heads, heads), 0,
        [
            sds((columns, share), BF16), sds((quads, own_out, model), BF16), sds((local, model)),
            sds((local, model)), sds((4, inner)), sds((1, inner)), sds((1, inner)), sds((4, state2)),
            sds((1, state2)), sds((8, 128)), sds((1, model)), sds((1, model)),
        ],
        range(5), range(2), [scratch[name] for name in SCRATCH],
    )(
        in_weight.T, out_weight, hidden_in[0], output_gradient[0], gain_row,
        own(conv_x_weight, width, 1), own(conv_x_bias, width, 0)[None], conv_bc_weight,
        conv_bc_bias[None], pad_heads(dt_bias), pad_heads(a_log), skip_own,
    )
    wide = hidden_in[0].astype(F32)
    inv_rms = lax.rsqrt(jnp.mean(wide * wide, -1, keepdims=True) + EPSILON)
    unit_rows = wide * inv_rms
    unit_grad = gn_own * pre_full
    input_grad = output_gradient[0].astype(F32) + inv_rms * (
        unit_grad - unit_rows * jnp.mean(unit_grad * unit_rows, -1, keepdims=True)
    )
    return (
        (wide + op_own)[None], input_grad[None],
        lax.dynamic_slice_in_dim(pre_grad[0], rank * share, share, 0), in_out.T.astype(F32),
        conv_x_grad, conv_x_bias_grad[0], conv_bc_grad, conv_bc_bias_grad[0],
        head_grad[5, :heads], head_grad[6, :heads], head_grad[7, :heads],
        lax.dynamic_slice_in_dim(norm_grad[0], rank * (inner // dp), inner // dp, 0),
        out_out.reshape(width, model).astype(F32),
    )


def solution(mesh):
    dp, seq = mesh.shape["dp"], mesh.shape["seq"]
    fine = Mesh(mesh.devices.reshape(dp, 2, seq // 2), ("dp", "pair", "quad"))
    tokens, whole, rows = P("dp", ("pair", "quad"), None), P(), P("dp", None)
    return jax.shard_map(
        on_device,
        mesh=fine,
        in_specs=(
            tokens, P("dp"), rows, whole, whole, whole, whole, whole, whole, whole, P("dp"), rows, tokens,
        ),
        out_specs=(
            tokens, tokens, P("dp"), rows, whole, whole, whole, whole, whole, whole, whole, P("dp"), rows,
        ),
        check_vma=False,
    )
```

```python
import functools
import types

import jax
import jax.numpy as jnp
from jax import lax
from jax.experimental import pallas as pl
from jax.experimental.pallas import tpu as pltpu
from jax.sharding import Mesh
from jax.sharding import PartitionSpec as P

EPSILON = 1e-05
BLOCK = 256
HALO = 16
F32 = jnp.float32
BF16 = jnp.bfloat16
NN = ((1,), (0,))
NT = ((1,), (1,))
TN = ((0,), (0,))


def mm(a, b, dims=NN):
    return lax.dot_general(
        a.astype(BF16), b.astype(BF16), (dims, ((), ())), preferred_element_type=F32
    )


def split(a):
    high = a.astype(BF16)
    return high, (a - high.astype(F32)).astype(BF16)


def mm3(a, b, dims=NN):
    ah, al = split(a)
    bh, bl = split(b)
    return mm(ah, bh, dims) + (mm(ah, bl, dims) + mm(al, bh, dims))


def mm_exact(a, b, dims=NN):
    b0 = b.astype(BF16)
    r1 = b - b0.astype(F32)
    b1 = r1.astype(BF16)
    b2 = (r1 - b1.astype(F32)).astype(BF16)
    return mm(a, b0, dims) + (mm(a, b1, dims) + mm(a, b2, dims))


def mm_sum(a, b, dims=NN):
    ah, al = split(a)
    return mm(ah, b, dims) + mm(al, b, dims)


def sigmoid(v):
    return 1.0 / (1.0 + jnp.exp(-v))


def lane_mask(width, first):
    lane = lax.broadcasted_iota(jnp.int32, (1, 128), 1)
    return (lane < 64) if first else (lane >= 64)


def expand(v, pair):
    lane = lax.broadcasted_iota(jnp.int32, (1, 128), 1)
    return jnp.where(lane < 64, v[:, 2 * pair : 2 * pair + 1], v[:, 2 * pair + 1 : 2 * pair + 2])


def lower_mask():
    return lax.broadcasted_iota(jnp.int32, (BLOCK, BLOCK), 0) >= lax.broadcasted_iota(
        jnp.int32, (BLOCK, BLOCK), 1
    )


def head_indicator(pair):
    row = lax.broadcasted_iota(jnp.int32, (128, 128), 0)
    col = lax.broadcasted_iota(jnp.int32, (128, 128), 1)
    return (col == 2 * pair + row // 64).astype(BF16)


def conv_block(p_ref, row, col, w_ref, b_ref, wcol):
    raw = p_ref[pl.ds(row, BLOCK + HALO), col : col + 128].astype(F32)
    shifted = [raw[HALO - 3 + k : HALO - 3 + k + BLOCK] for k in range(4)]
    pre = b_ref[0:1, wcol : wcol + 128]
    for k in range(4):
        pre = pre + w_ref[k : k + 1, wcol : wcol + 128] * shifted[k]
    return pre, shifted


def run_hooks(hooks, at):
    for index, hook in hooks.items():
        pl.when(at == index)(hook)


def prep_pass(width, px_ref, pt_ref, pd_ref, wx_ref, bx_ref, wb_ref, bb_ref, dtb_ref, alog_ref,
              xs_ref, bc_ref, dt_ref, cum_ref, fin_ref, hooks):
    blocks = xs_ref.shape[0] // BLOCK
    rate = -jnp.exp(alog_ref[...])
    fin_ref[...] = jnp.zeros_like(fin_ref)

    def step(b, carry):
        row = pl.multiple_of(b * BLOCK, BLOCK)
        for c in range(2):
            pre, _ = conv_block(pt_ref, row, 128 * c, wb_ref, bb_ref, 128 * c)
            bc_ref[pl.ds(row, BLOCK), 128 * c : 128 * c + 128] = pre * sigmoid(pre)
        raw = pd_ref[pl.ds(row + HALO, BLOCK), :].astype(F32)
        raw = raw + dtb_ref[...]
        dt = jnp.maximum(raw, 0.0) + jnp.log1p(jnp.exp(-jnp.abs(raw)))
        cum = mm_exact(lower_mask().astype(F32), dt * rate)
        dt_ref[pl.ds(row, BLOCK), :] = dt
        cum_ref[pl.ds(row, BLOCK), :] = cum
        last = cum[BLOCK - 1 : BLOCK, :]
        weight = dt * jnp.exp(last - cum)
        decay = jnp.exp(last)
        keys_t = bc_ref[pl.ds(row, BLOCK), 0:128].T
        for pair in range(width // 128):
            cols = slice(128 * pair, 128 * pair + 128)
            pre, _ = conv_block(px_ref, row, 128 * pair, wx_ref, bx_ref, 128 * pair)
            xs = pre * sigmoid(pre)
            xs_ref[pl.ds(row, BLOCK), cols] = xs
            fin_ref[:, cols] = fin_ref[:, cols] * expand(decay, pair) + mm3(
                keys_t, xs * expand(weight, pair)
            )
        run_hooks(hooks, b)
        return carry

    lax.fori_loop(0, blocks, step, 0)


def inside_pass(width, xs_ref, bc_ref, dt_ref, cum_ref, yl_ref, hooks):
    def step(b, carry):
        rows = pl.ds(pl.multiple_of(b * BLOCK, BLOCK), BLOCK)
        dt, cum = dt_ref[rows, :], cum_ref[rows, :]
        cum_t = cum.T
        scores = mm3(bc_ref[rows, 128:256], bc_ref[rows, 0:128], NT)
        mask = lower_mask()
        for pair in range(width // 128):
            cols = slice(128 * pair, 128 * pair + 128)
            stepped = xs_ref[rows, cols] * expand(dt, pair)
            y = jnp.zeros((BLOCK, 128), F32)
            for half in range(2):
                h = 2 * pair + half
                spread = cum[:, h : h + 1] - cum_t[h : h + 1, :]
                table = jnp.exp(jnp.where(mask, spread, -1e30))
                part = jnp.where(lane_mask(128, half == 0), stepped, 0.0)
                y = y + mm3(scores * table, part)
            yl_ref[rows, cols] = y
        run_hooks(hooks, b)
        return carry

    lax.fori_loop(0, xs_ref.shape[0] // BLOCK, step, 0)


def outside_pass(
    width, xs_ref, bc_ref, dt_ref, cum_ref, skip_ref, y_ref, yl_ref, states_ref, s_ref, hooks
):
    def step(b, carry):
        rows = pl.ds(pl.multiple_of(b * BLOCK, BLOCK), BLOCK)
        dt, cum = dt_ref[rows, :], cum_ref[rows, :]
        last = cum[BLOCK - 1 : BLOCK, :]
        grow, decay = jnp.exp(cum), jnp.exp(last)
        weight = dt * jnp.exp(last - cum)
        queries = bc_ref[rows, 128:256]
        keys_t = bc_ref[rows, 0:128].T
        for pair in range(width // 128):
            cols = slice(128 * pair, 128 * pair + 128)
            xs = xs_ref[rows, cols]
            state = s_ref[:, cols]
            states_ref[b, :, cols] = state
            y = yl_ref[rows, cols] + expand(grow, pair) * mm3(queries, state)
            s_ref[:, cols] = state * expand(decay, pair) + mm3(keys_t, xs * expand(weight, pair))
            yl_ref[rows, cols] = y
            y_ref[rows, cols] = (y + skip_ref[0:1, cols] * xs).astype(BF16)
        run_hooks(hooks, b)
        return carry

    lax.fori_loop(0, xs_ref.shape[0] // BLOCK, step, 0)


MESH = pl.DeviceIdType.MESH


def bits_of(count):
    return [1 << i for i in range(count.bit_length() - 1)]


def bit_at(index, bit):
    return (index // bit) % 2


def flip(index, bits):
    for bit in bits:
        index = index + bit * (1 - 2 * bit_at(index, bit))
    return index


def subsets(bits):
    found = [frozenset()]
    for bit in bits:
        found = found + [f | {bit} for f in found]
    return found


class Links:
    def __init__(self, send, recv):
        self.send, self.recv, self.count, self.open = send, recv, 0, []

    def make(self, src, dst, target):
        index, self.count = self.count, self.count + 1
        return pltpu.make_async_remote_copy(
            src_ref=src, dst_ref=dst, send_sem=self.send.at[index], recv_sem=self.recv.at[index],
            device_id=target, device_id_type=MESH,
        )

    def stage(self, copies, after=None):
        def begin():
            for copy in copies:
                copy.start()
                self.open.append(lambda copy=copy: copy.wait_send())

        def end():
            for copy in copies:
                copy.wait_recv()
            if after is not None:
                after()

        return begin, end

    def stage_if(self, copy, sends, takes):
        def left():
            pl.when(sends)(copy.wait_send)

        def begin():
            pl.when(sends)(copy.start)
            self.open.append(left)

        def end():
            pl.when(takes)(copy.wait_recv)

        return begin, end

    def drain(self):
        for left in self.open:
            left()
        self.open = []


def meet(targets):
    barrier = pltpu.get_barrier_semaphore()
    for target in targets:
        pl.semaphore_signal(barrier, inc=1, device_id=target, device_id_type=MESH)
    pl.semaphore_wait(barrier, len(targets))


def neighbours(axis):
    me = lax.axis_index(axis)
    return [{axis: flip(me, (bit,))} for bit in bits_of(lax.axis_size(axis))]


class Flow:
    def __init__(self, links, stages):
        self.links, self.stages, self.at, self.sent = links, stages, -1, []

    def go(self):
        if 0 <= self.at < len(self.stages):
            self.stages[self.at][1]()
        self.at += 1
        if self.at < len(self.stages):
            before = len(self.links.open)
            self.stages[self.at][0]()
            self.sent += self.links.open[before:]

    def drain(self):
        for left in self.sent:
            left()
        done = {id(left) for left in self.sent}
        self.links.open = [left for left in self.links.open if id(left) not in done]
        self.sent = []

    def finish(self):
        while self.at < len(self.stages):
            self.go()


def step(*flows):
    for flow in flows:
        flow.go()


def finish(*flows):
    while any(flow.at < len(flow.stages) for flow in flows):
        for flow in flows:
            if flow.at < len(flow.stages):
                flow.go()


def add_rows(out, a, b):
    rows = out.shape[0]
    step = 16 if rows % 16 == 0 else 8
    while out.shape[1] * step * 2 <= 24576 and rows % (2 * step) == 0:
        step *= 2

    @pl.loop(0, rows // step)
    def _(i):
        at = pl.ds(pl.multiple_of(i * step, step), step)
        out[at, :] = (a[at, :].astype(F32) + b[at, :].astype(F32)).astype(out.dtype)


def gather_stages(links, axis, order, own, slot):
    me = lax.axis_index(axis)
    held, stages = [frozenset()], []
    for bit in order:
        target = {axis: flip(me, (bit,))}
        stages.append(
            links.stage([
                links.make(slot(flip(me, f)) if f else own, slot(flip(me, f)), target) for f in held
            ])
        )
        held = held + [f | {bit} for f in held]
    return stages


def reduce_stages(links, axis, order, source, inbox, final=None):
    me = lax.axis_index(axis)
    base, stages = 0, []
    blocks = {f: source(flip(me, f)) for f in subsets(order)}
    for stage, bit in enumerate(order):
        keep = subsets(order[stage + 1 :])
        target = {axis: flip(me, (bit,))}
        boxes = [inbox(base + k) for k in range(len(keep))]
        outs = [final] if final is not None and stage == len(order) - 1 else boxes
        copies = [links.make(blocks[f | {bit}], box, target) for f, box in zip(keep, boxes)]

        def after(mine=[blocks[f] for f in keep], boxes=boxes, outs=outs):
            for a, b, out in zip(mine, boxes, outs):
                add_rows(out, a, b)

        stages.append(links.stage(copies, after))
        blocks = dict(zip(keep, outs))
        base += len(keep)
    return stages


def spread_stages(links, order, block):
    d, q = lax.axis_index("dp"), lax.axis_index("quad")
    away = {bit: bit_at(d, bit) != bit_at(q, bit) for bit in order}
    stages = []
    for stage, bit in enumerate(order):
        reached = jnp.bool_(True)
        for later in order[stage + 1 :]:
            reached = jnp.logical_and(reached, jnp.logical_not(away[later]))
        holder = jnp.logical_and(reached, jnp.logical_not(away[bit]))
        taker = jnp.logical_and(reached, away[bit])
        copy = links.make(block, block, {"dp": flip(d, (bit,))})
        stages.append(links.stage_if(copy, holder, taker))
    return stages


def leave_pass(width, bc_ref, cum_ref, gy_ref, out_ref):
    blocks = gy_ref.shape[0] // BLOCK
    out_ref[...] = jnp.zeros_like(out_ref)

    def step(i, carry):
        rows = pl.ds(pl.multiple_of((blocks - 1 - i) * BLOCK, BLOCK), BLOCK)
        cum = cum_ref[rows, :]
        grow, decay = jnp.exp(cum), jnp.exp(cum[BLOCK - 1 : BLOCK, :])
        queries_t = bc_ref[rows, 128:256].T
        for pair in range(width // 128):
            cols = slice(128 * pair, 128 * pair + 128)
            dy = gy_ref[rows, cols].astype(F32)
            out_ref[:, cols] = out_ref[:, cols] * expand(decay, pair) + mm3(
                queries_t, expand(grow, pair) * dy
            )
        return carry

    lax.fori_loop(0, blocks, step, 0)


def back_inside_pass(width, r, hooks):
    def step(b, carry):
        rows = pl.ds(pl.multiple_of(b * BLOCK, BLOCK), BLOCK)
        dt, cum = r.dt[rows, :], r.cum[rows, :]
        cum_t = cum.T
        keys, queries = r.bc[rows, 0:128], r.bc[rows, 128:256]
        scores = mm3(queries, keys, NT)
        mask = lower_mask()
        r.dscore[...] = jnp.zeros_like(r.dscore)
        for pair in range(width // 128):
            cols = slice(128 * pair, 128 * pair + 128)
            stepped, stepped_low = split(r.xs[rows, cols] * expand(dt, pair))
            dy = r.y[rows, cols].astype(F32)
            dstep = jnp.zeros((BLOCK, 128), F32)
            for half in range(2):
                h = 2 * pair + half
                spread = cum[:, h : h + 1] - cum_t[h : h + 1, :]
                table = jnp.exp(jnp.where(mask, spread, -1e30))
                part = jnp.where(lane_mask(128, half == 0), dy, 0.0).astype(BF16)
                dmix = mm(part, stepped, NT) + mm(part, stepped_low, NT)
                r.dscore[...] += dmix * table
                high, low = split(scores * table)
                dstep = dstep + (mm(high, part, TN) + mm(low, part, TN))
            r.gm[rows, cols] = dstep
        r.dbc[rows, 0:128] = mm3(r.dscore[...], queries, TN)
        r.dbc[rows, 128:256] = mm3(r.dscore[...], keys)
        run_hooks(hooks, b)
        return carry

    lax.fori_loop(0, r.y.shape[0] // BLOCK, step, 0)


def back_outside_pass(width, r, hooks):
    blocks = r.y.shape[0] // BLOCK
    rate = -jnp.exp(r.alog[...])
    r.heads[...] = jnp.zeros_like(r.heads)

    def step(i, carry):
        b = blocks - 1 - i
        row = pl.multiple_of(b * BLOCK, BLOCK)
        rows = pl.ds(row, BLOCK)
        dt, cum = r.dt[rows, :], r.cum[rows, :]
        last = cum[BLOCK - 1 : BLOCK, :]
        grow, decay, tail = jnp.exp(cum), jnp.exp(last), jnp.exp(last - cum)
        keys, queries = r.bc[rows, 0:128], r.bc[rows, 128:256]
        queries_t = queries.T
        dkeys, dqueries = r.dbc[rows, 0:128], r.dbc[rows, 128:256]
        dcum = jnp.zeros((BLOCK, 128), F32)
        ddt = jnp.zeros((BLOCK, 128), F32)
        dlast = jnp.zeros((8, 128), F32)
        dskip = jnp.zeros((8, 128), F32)
        for pair in range(width // 128):
            cols = slice(128 * pair, 128 * pair + 128)
            xs = r.xs[rows, cols]
            dt_e = expand(dt, pair)
            stepped = xs * dt_e
            dy = r.y[rows, cols].astype(F32)
            state, ds = r.states[b, :, cols], r.ds[:, cols]
            tail_e = expand(tail, pair)
            carried = mm3(keys, ds) * tail_e
            dstep = r.gm[rows, cols] + carried
            dkeys = dkeys + mm3(stepped * tail_e, ds, NT)
            grown = expand(grow, pair) * dy
            dqueries = dqueries + mm3(grown, state, NT)
            decay_e = expand(decay, pair)
            ends = jnp.sum(stepped * carried, 0, keepdims=True) + decay_e * jnp.sum(
                ds * state, 0, keepdims=True
            )
            r.ds[:, cols] = ds * decay_e + mm3(queries_t, grown)
            dxs = dstep * dt_e + r.skip[0:1, cols] * dy
            which = head_indicator(pair)
            ddt = ddt + mm_sum(dstep * xs, which)
            dcum = dcum + mm_sum(dy * r.yl[rows, cols] - stepped * dstep, which)
            dlast = dlast + mm_sum(jnp.broadcast_to(ends, (8, 128)), which)
            skips = jnp.sum(dy * xs, 0, keepdims=True)
            dskip = dskip + mm_sum(jnp.broadcast_to(skips, (8, 128)), which)
            pre, shifted = conv_block(r.px, row, 128 * pair, r.wxc, r.bxc, 128 * pair)
            sig = sigmoid(pre)
            dpre = dxs * sig * (1.0 + pre * (1.0 - sig))
            r.xs[rows, cols] = dpre
            for k in range(4):
                r.sx[k : k + 1, cols] += jnp.sum(dpre * shifted[k], 0, keepdims=True)
            r.sx[4:5, cols] += jnp.sum(dpre, 0, keepdims=True)
        at_end = lax.broadcasted_iota(jnp.int32, (BLOCK, 128), 0) == BLOCK - 1
        dcum = dcum + jnp.where(at_end, dlast[0:1], 0.0)
        dlog = mm_exact(lower_mask().astype(F32), dcum, TN)
        raw = r.pd[pl.ds(row + HALO, BLOCK), :].astype(F32)
        draw = (ddt + dlog * rate) * sigmoid(raw + r.dtb[...])
        r.gdt[rows, :] = draw.astype(BF16)
        r.heads[0:1, :] += jnp.sum(draw, 0, keepdims=True)
        r.heads[1:2, :] += jnp.sum(dlog * dt, 0, keepdims=True) * rate
        r.heads[2:3, :] += dskip[0:1]
        for c, grad in enumerate((dkeys, dqueries)):
            cols = slice(128 * c, 128 * c + 128)
            pre, shifted = conv_block(r.pt, row, 128 * c, r.wbc, r.bbc, 128 * c)
            sig = sigmoid(pre)
            dpre = grad * sig * (1.0 + pre * (1.0 - sig))
            r.dbc[rows, cols] = dpre
            for k in range(4):
                r.sb[k : k + 1, cols] += jnp.sum(dpre * shifted[k], 0, keepdims=True)
            r.sb[4:5, cols] += jnp.sum(dpre, 0, keepdims=True)
        run_hooks(hooks, i)
        return carry

    lax.fori_loop(0, blocks, step, 0)


INPUTS = (
    "win", "wo_in", "hid_in", "og_in", "gain_in", "wx_all", "bx_all", "wbc", "bbc", "per_head",
)
OUTPUTS = (
    "in_out", "out_out", "op_own", "gn_own", "cxw", "cxb", "norm", "cbw", "cbb", "head", "pre",
)
SCRATCH = (
    "wz", "wx", "wt", "wo", "xn", "og", "hid", "px", "pt", "pd", "xs", "bc", "dt", "cum", "y", "yl", "states", "z", "gm", "mixed", "dbc", "gdt", "bcs", "bcbox", "bcall", "tail", "wtail", "grad", "gradt", "zbox", "zpair", "xpair", "tbox", "tpair", "obox", "opair", "opbox", "ttot", "tstage", "gain", "halo", "fin", "enter", "ds", "stat", "statbox", "dscore", "heads", "sx", "sb", "sp", "sxbox", "sbbox", "spbox", "sxall", "sball", "spall", "hx", "hb", "dsin", "hown", "oown", "wxc", "bxc", "dtb", "alog", "skip", "send", "recv", "local",
)


def block_kernel(width, own_heads, heads, *refs):
    r = types.SimpleNamespace(**dict(zip((*INPUTS, *OUTPUTS, *SCRATCH), refs, strict=True)))
    d, q, p = lax.axis_index("dp"), lax.axis_index("quad"), lax.axis_index("pair")
    dps, quads = lax.axis_size("dp"), lax.axis_size("quad")
    tokens, piece, model = r.y.shape[0], r.hid.shape[1], r.hid.shape[2]
    inner, share, state2 = width * quads, model // dps, r.bc.shape[1]
    bc_cols = state2 // quads
    links = Links(r.send, r.recv)
    dp_bits, up = bits_of(dps), bits_of(quads)
    orders, down = (dp_bits, dp_bits[::-1]), up[::-1]
    other, swapped = {"pair": flip(p, (1,))}, {"dp": q, "quad": d}
    near = neighbours("dp") + neighbours("quad") + neighbours("pair")
    sides = ((0, width // 2), (width // 2, width // 2))
    tail_rows = r.win.shape[0] - 2 * inner
    cut = tail_rows // 32 * 16 + 16
    tail_sides = ((0, cut), (cut, tail_rows - cut))
    lane_row = lax.broadcasted_iota(jnp.int32, (128, 128), 0)
    lane_col = lax.broadcasted_iota(jnp.int32, (128, 128), 1)
    first_half, second_half = p == 0, p > 0

    @pl.when(d == q)
    def _():
        meet(near)

    @pl.when(d != q)
    def _():
        meet([*near, swapped])

    def win_rows(base, at, size):
        return r.win.at[pl.ds(pl.multiple_of(base + q * width + at, 16), size)]

    def tail_source(at, size):
        return r.win.at[pl.ds(2 * inner + at, size)]

    def weights(source, out, parts):
        return [
            Flow(links, gather_stages(
                links, "dp", order, source(at, size),
                lambda i, at=at, size=size: out.at[i, pl.ds(at, size)],
            ))
            for order, (at, size) in zip(orders, parts)
        ]

    gain_flow = Flow(links, gather_stages(links, "dp", dp_bits, r.gain_in, lambda i: r.gain.at[i]))
    hid_flow = Flow(links, gather_stages(links, "quad", down, r.hid_in, lambda i: r.hid.at[i]))
    og_flow = Flow(links, gather_stages(links, "quad", down, r.og_in, lambda i: r.og.at[i]))
    wt_flows = weights(tail_source, r.wt, tail_sides)
    wx_flows = weights(lambda at, size: win_rows(inner, at, size), r.wx, sides)
    wz_flows = weights(lambda at, size: win_rows(0, at, size), r.wz, sides)
    parts = 4
    wo_flows = [
        Flow(links, spread_stages(links, dp_bits[::-1], r.wo.at[pl.ds(k * (width // parts), width // parts)]))
        for k in range(parts)
    ]
    tail = r.hid.at[quads - 1, pl.ds(piece - HALO, HALO)]
    halo_flow = Flow(links, [links.stage_if(links.make(tail, r.halo, other), first_half, second_half)])
    state_flow = Flow(links, [links.stage_if(links.make(r.fin, r.enter, other), first_half, second_half)])
    ds_flow = Flow(links, [links.stage_if(links.make(r.fin, r.dsin, other), second_half, first_half)])
    edge_flows = [
        Flow(links, [links.stage_if(links.make(a.at[pl.ds(0, 8)], b, other), second_half, first_half)])
        for a, b in ((r.xs, r.hx), (r.dbc, r.hb))
    ]
    stat_flow = Flow(links, [
        links.stage(
            [links.make(r.stat.at[k], r.statbox.at[k], {"quad": flip(q, (bit,))})],
            lambda k=k: r.stat.at[k + 1].__setitem__(..., r.stat[k] + r.statbox[k]),
        )
        for k, bit in enumerate(up)
    ])
    kept = []

    def keeper(own, place, index):
        return pltpu.make_async_copy(own, place, r.local.at[index])

    def in_flow(h, at, size, part_ref, box, pair_box, slot, index):
        rows = pl.ds(at, size)
        stages = reduce_stages(
            links, "dp", orders[h], lambda i: part_ref.at[i, rows], lambda k: box.at[k, rows]
        )
        mine, own = box.at[dps - 2, rows], pair_box.at[rows]
        keep = keeper(own, slot(q), index)

        def after():
            add_rows(own, mine, own)
            keep.start()
            kept.append(keep)

        stages.append(links.stage([links.make(mine, own, other)], after))
        return Flow(links, stages + gather_stages(links, "quad", down, own, slot))

    def columns_slot(base, at, size):
        return lambda i: r.in_out.at[pl.ds(pl.multiple_of(base + i * width + at, 16), size)]

    def out_flow(h):
        half = model // 2
        part, size = pl.ds(h * half, half), width // dps
        stages = reduce_stages(
            links, "dp", orders[h],
            lambda i: r.wo.at[pl.ds(pl.multiple_of(i * size, 16), size), part],
            lambda k: r.obox.at[h, k],
        )
        mine, whole = r.obox.at[h, dps - 2], r.opair.at[h]
        place = r.out_out.at[d, :, part]
        stages.append(
            links.stage([links.make(mine, whole, other)], lambda: add_rows(whole, mine, whole))
        )
        near_copy = pltpu.make_async_copy(whole, place, r.local.at[14 + h])
        far_copy = links.make(whole, place, swapped)

        def begin():
            pl.when(d == q)(near_copy.start)
            pl.when(d != q)(far_copy.start)

        def end():
            pl.when(d == q)(near_copy.wait)
            pl.when(d != q)(far_copy.wait)

        stages.append((begin, end))
        return Flow(links,
            stages
            + gather_stages(
                links, "quad", down, r.out_out.at[q, :, part], lambda i: r.out_out.at[i, :, part]
            )
        )

    def row_sum_flow(source, box, final):
        return Flow(links, reduce_stages(
            links, "quad", up, lambda i: source.at[i], lambda k: box.at[k], final
        ))

    def small_flow(mine, box, every):
        current, stages = mine, []
        steps = [("dp", bit) for bit in dp_bits] + [("pair", 1)]
        for k, (axis, bit) in enumerate(steps):
            target = {axis: flip(lax.axis_index(axis), (bit,))}
            out = box.at[k] if k < len(steps) - 1 else every.at[q]

            def after(out=out, current=current, k=k):
                out[...] = current[...] + box[k]

            stages.append(links.stage([links.make(current, box.at[k], target)], after))
            current = out
        return Flow(links,
            stages + gather_stages(links, "quad", down, every.at[q], lambda i: every.at[i])
        )

    z_flows = [
        in_flow(h, at, size, r.grad, r.zbox, r.zpair, columns_slot(0, at, size), 7 + h)
        for h, (at, size) in enumerate(sides)
    ]
    x_flows = [
        in_flow(h, at, size, r.grad, r.zbox, r.xpair, columns_slot(inner, at, size), 9 + h)
        for h, (at, size) in enumerate(sides)
    ]
    t_flow = in_flow(0, 0, 128, r.gradt, r.tbox, r.tpair, lambda i: r.ttot.at[i], 11)
    out_flows = [out_flow(0), out_flow(1)]
    op_flow = row_sum_flow(r.hid, r.opbox, r.op_own)
    gn_flow = row_sum_flow(r.og, r.opbox, r.gn_own)
    bc_flow = Flow(links,
        reduce_stages(links, "quad", up, lambda i: r.bcs.at[i], lambda k: r.bcbox.at[k], r.bcall.at[q])
        + gather_stages(links, "quad", down, r.bcall.at[q], lambda i: r.bcall.at[i])
    )
    sx_flow, sb_flow, sp_flow = (
        small_flow(r.sx, r.sxbox, r.sxall), small_flow(r.sb, r.sbbox, r.sball),
        small_flow(r.sp, r.spbox, r.spall),
    )

    step(gain_flow, hid_flow, *wt_flows, *wx_flows)
    owned = [
        (r.hid_in, r.hid.at[q]), (r.gain_in, r.gain.at[d]),
        (tail_source(0, tail_rows), r.wt.at[d, pl.ds(0, tail_rows)]),
        (win_rows(inner, 0, width), r.wx.at[d]), (win_rows(0, 0, width), r.wz.at[d]),
        (r.og_in, r.og.at[q]),
    ]
    copies = [pltpu.make_async_copy(a, b, r.local.at[i]) for i, (a, b) in enumerate(owned)]
    for copy in copies:
        copy.start()

    @pl.when(d == q)
    def _():
        copy = pltpu.make_async_copy(r.wo_in, r.wo, r.local.at[len(owned)])
        copy.start()
        copy.wait()

    for i in range(dps):
        r.wt[i, tail_rows:, :] = jnp.zeros((r.wt.shape[1] - tail_rows, share), BF16)
    r.sx[...] = jnp.zeros_like(r.sx)
    r.sb[...] = jnp.zeros_like(r.sb)
    own_cols = pl.ds(pl.multiple_of(q * width, 128), width)
    r.wxc[...] = r.wx_all[:, own_cols]
    r.bxc[...] = r.bx_all[:, own_cols]
    turned = r.per_head[...]
    for i in range(1, quads):
        turned = jnp.where(q == i, pltpu.roll(r.per_head[...], 128 - i * own_heads, 1), turned)
    r.dtb[...] = turned[0:1]
    r.alog[...] = turned[1:2]
    head_row = lax.broadcasted_iota(jnp.int32, (128, width), 0)
    head_col = lax.broadcasted_iota(jnp.int32, (128, width), 1)
    widen = (head_row == head_col // (width // own_heads)).astype(BF16)
    s0 = turned.astype(BF16)
    rest = turned - s0.astype(F32)
    s1 = rest.astype(BF16)
    s2 = (rest - s1.astype(F32)).astype(BF16)
    r.skip[...] = (mm(s0, widen) + mm(s1, widen) + mm(s2, widen))[2:3]
    for copy in copies:
        copy.wait()
    finish(gain_flow)
    step(hid_flow, *wt_flows, *wx_flows)
    step(*wz_flows, og_flow)
    step(*wo_flows)
    hid_flow.finish()
    step(halo_flow)
    halo_flow.finish()

    gains = r.gain[0]
    for i in range(1, dps):
        gains = gains + r.gain[i]
    pre = gains[:, :model]

    def normed(v):
        v = v.astype(F32)
        unit = v * lax.rsqrt(jnp.mean(v * v, -1, keepdims=True) + EPSILON)
        return (unit * pre).astype(BF16)

    def put_normed(at, rows, v):
        for i in range(dps):
            r.xn[i, pl.ds(at, rows), :] = v[:, i * share : (i + 1) * share]

    put_normed(0, HALO, jnp.where(p > 0, normed(r.halo[...]), jnp.zeros((HALO, model), BF16)))
    few = 32

    @pl.loop(0, tokens // few)
    def _(i):
        at = i * few
        rows = pl.ds(pl.multiple_of(at % piece, few), few)
        put_normed(pl.multiple_of(at + HALO, 16), few, normed(r.hid[at // piece, rows, :]))

    finish(*wt_flows, *wx_flows)

    def project(out_ref, out_at, at, rows, w_ref):
        total = jnp.zeros((rows, w_ref.shape[1]), F32)
        for i in range(dps):
            total = total + mm(r.xn[i, pl.ds(at, rows), :], w_ref[i], NT)
        out_ref[pl.ds(out_at, rows), :] = total.astype(BF16)

    for out_ref, w_ref in ((r.pt, r.wt), (r.px, r.wx)):
        project(out_ref, 0, 0, HALO, w_ref)

        @pl.loop(0, tokens // BLOCK)
        def _(i, out_ref=out_ref, w_ref=w_ref):
            at = pl.multiple_of(i * BLOCK + HALO, 16)
            project(out_ref, at, at, BLOCK, w_ref)

    pick = jnp.logical_and(lane_row == lane_col + q * own_heads, lane_col < own_heads).astype(BF16)
    r.pd[...] = mm(r.pt[:, state2 : state2 + 128], pick).astype(BF16)
    prep_pass(
        width, r.px, r.pt, r.pd, r.wxc, r.bxc, r.wbc, r.bbc, r.dtb, r.alog,
        r.xs, r.bc, r.dt, r.cum, r.fin, {0: lambda: step(*wz_flows, og_flow), 3: wo_flows[0].go},
    )
    step(state_flow)
    inside_pass(
        width, r.xs, r.bc, r.dt, r.cum, r.yl, {1: wo_flows[1].go, 3: wo_flows[2].go},
    )
    finish(*wz_flows)

    @pl.loop(0, tokens // BLOCK)
    def _(i):
        at = pl.multiple_of(i * BLOCK, BLOCK)
        project(r.z, at, pl.multiple_of(at + HALO, 16), BLOCK, r.wz)

    state_flow.finish()
    r.ds[...] = jnp.where(p > 0, r.enter[...], 0.0)
    outside_pass(
        width, r.xs, r.bc, r.dt, r.cum, r.skip, r.y, r.yl, r.states, r.ds, {1: wo_flows[3].go},
    )
    finish(og_flow, *wo_flows)

    @pl.loop(0, quads)
    def _(i):
        r.gm[pl.ds(pl.multiple_of(i * piece, piece), piece), :] = mm(r.og[i], r.wo[...], NT)

    norm_all = gains[:, model:]
    norm_own = norm_all[:, :width]
    for i in range(1, quads):
        norm_own = jnp.where(q == i, norm_all[:, i * width : (i + 1) * width], norm_own)
    chunk = 128

    @pl.loop(0, tokens // chunk)
    def _(i):
        rows = pl.ds(pl.multiple_of(i * chunk, chunk), chunk)
        gate = r.z[rows, :].astype(F32)
        gated = r.y[rows, :].astype(F32) * gate * sigmoid(gate)
        first = jnp.sum(gated * gated, -1, keepdims=True)
        second = jnp.sum(r.gm[rows, :] * norm_own * gated, -1, keepdims=True)
        lane = lax.broadcasted_iota(jnp.int32, (chunk, 128), 1)
        both = jnp.where(lane == 0, first, jnp.where(lane == 1, second, 0.0))
        r.stat[0, :, rows] = both.T[0:8, :]

    finish(stat_flow)

    @pl.loop(0, tokens // chunk)
    def _(i):
        rows = pl.ds(pl.multiple_of(i * chunk, chunk), chunk)
        stats = r.stat[len(up), :, rows]
        stats = jnp.concatenate([stats] * (128 // 8), 0).T
        out_rms = lax.rsqrt(stats[:, 0:1] / inner + EPSILON)
        mean_dot = out_rms * stats[:, 1:2] / inner
        gate = r.z[rows, :].astype(F32)
        y = r.y[rows, :].astype(F32)
        sig = sigmoid(gate)
        unit_gated = y * gate * sig * out_rms
        grad_mixed = r.gm[rows, :]
        r.mixed[rows, :] = (unit_gated * norm_own).astype(BF16)
        r.sx[5:6, :] += jnp.sum(grad_mixed * unit_gated, 0, keepdims=True)
        grad_gated = out_rms * (grad_mixed * norm_own - unit_gated * mean_dot)
        r.y[rows, :] = (grad_gated * gate * sig).astype(BF16)
        r.z[rows, :] = (grad_gated * y * sig * (1.0 + gate * (1.0 - sig))).astype(BF16)

    def weight_grad(grad_ref, out_ref):
        for i in range(dps):
            out_ref[i] = mm(grad_ref[...], r.xn[i, pl.ds(HALO, tokens), :], TN).astype(BF16)

    links.drain()

    @pl.loop(0, quads)
    def _(i):
        rows = pl.ds(pl.multiple_of(i * piece, piece), piece)
        r.hid[i] = mm(r.mixed[rows, :], r.wo[...]).astype(BF16)

    own_copies = [
        pltpu.make_async_copy(a, b, r.local.at[i])
        for i, (a, b) in enumerate(((r.hid_in, r.hown), (r.og_in, r.oown)))
    ]
    for copy in own_copies:
        copy.start()
    step(op_flow)
    weight_grad(r.z, r.grad)
    op_flow.go()
    step(*z_flows)
    leave_pass(width, r.bc, r.cum, r.y, r.fin)
    step(ds_flow)
    size = BLOCK if width % BLOCK == 0 else 128

    @pl.loop(0, width // size)
    def _(i):
        cols = pl.ds(pl.multiple_of(i * size, size), size)
        total = jnp.zeros((size, model), F32)
        for k in range(quads):
            total = total + mm(r.mixed[k * piece : (k + 1) * piece, cols], r.og[k], TN)
        r.wo[cols, :] = total.astype(BF16)

    step(*z_flows, *out_flows)
    blocks = tokens // BLOCK
    back_inside_pass(width, r, {1: lambda: step(*z_flows)})
    ds_flow.finish()
    r.ds[...] = jnp.where(p > 0, 0.0, r.dsin[...])
    back_outside_pass(
        width, r, {1: lambda: step(*out_flows), blocks - 1: lambda: step(*edge_flows, *out_flows)},
    )
    r.sb[5:6, 0:128], r.sb[6:7, 0:128], r.sb[7:8, 0:128] = r.heads[0:1], r.heads[1:2], r.heads[2:3]
    finish(*edge_flows)
    r.xs[pl.ds(tokens, 8), :] = jnp.where(p > 0, 0.0, r.hx[...])
    r.dbc[pl.ds(tokens, 8), :] = jnp.where(p > 0, 0.0, r.hb[...])

    def unconv(source, row, cols, w_ref):
        wide = source[pl.ds(row, chunk + 8), cols]
        total = jnp.zeros((chunk, 128), F32)
        for k in range(4):
            total = total + w_ref[k : k + 1, cols] * wide[3 - k : 3 - k + chunk]
        return total

    @pl.loop(0, tokens // chunk)
    def _(i):
        row = pl.multiple_of(i * chunk, chunk)
        inside = pl.ds(pl.multiple_of(row % piece, chunk), chunk)
        for c in range(2):
            cols = slice(128 * c, 128 * c + 128)
            r.bcs[row // piece, inside, cols] = unconv(r.dbc, row, cols, r.wbc)
        for pair in range(width // 128):
            cols = slice(128 * pair, 128 * pair + 128)
            r.mixed[pl.ds(row, chunk), cols] = unconv(r.xs, row, cols, r.wxc).astype(BF16)

    op_flow.finish()
    op_flow.drain()
    for flow in z_flows:
        flow.drain()
    step(*z_flows)
    step(sx_flow, sb_flow)
    step(bc_flow)
    weight_grad(r.mixed, r.grad)
    for _ in dp_bits:
        step(sx_flow)
    step(*x_flows, bc_flow)
    row = lax.broadcasted_iota(jnp.int32, (state2, 128), 0)
    col = lax.broadcasted_iota(jnp.int32, (state2, 128), 1)
    from_bc = jnp.logical_and(row == col + q * bc_cols, col < bc_cols).astype(BF16)
    from_dt = jnp.logical_and(lane_col == lane_row + bc_cols, lane_row < own_heads).astype(BF16)

    wide_rows = r.wt.shape[1]
    row = lax.broadcasted_iota(jnp.int32, (128, wide_rows), 0)
    col = lax.broadcasted_iota(jnp.int32, (128, wide_rows), 1)

    def dt_rows(i):
        return jnp.logical_and(
            jnp.logical_and(row >= bc_cols, row < bc_cols + own_heads),
            col == state2 + i * own_heads + row - bc_cols,
        )

    def bc_rows(i):
        return jnp.logical_and(row < bc_cols, col == row + i * bc_cols)

    take = dt_rows(q).astype(BF16)
    for i in range(dps):
        r.wtail[i] = mm(take, r.wt[i]).astype(BF16)
    r.tail[...] = mm(r.gdt[...], from_dt).astype(BF16)
    r.sp[...] = jnp.zeros_like(r.sp)

    def grad_rows(k, carry):
        at = pl.multiple_of(k * chunk, chunk)
        rows = pl.ds(at, chunk)
        inside = pl.ds(pl.multiple_of(at % piece, chunk), chunk)
        gz, gx, gt = r.z[rows, :], r.mixed[rows, :], r.tail[rows, :]
        for i in range(dps):
            grad = mm(gz, r.wz[i]) + mm(gx, r.wx[i]) + mm(gt, r.wtail[i])
            cols = slice(i * share, (i + 1) * share)
            unit = r.xn[i, pl.ds(pl.multiple_of(at + HALO, 16), chunk), :].astype(F32)
            r.sp[:, cols] += jnp.sum(grad * unit, 0, keepdims=True)
            r.og[at // piece, inside, cols] = grad.astype(BF16)
        return carry

    lax.fori_loop(0, tokens // chunk, grad_rows, 0)
    step(gn_flow, *x_flows)
    step(bc_flow, gn_flow)
    step(*x_flows)
    step(*out_flows)
    finish(bc_flow)

    @pl.loop(0, quads)
    def _(i):
        rows = pl.ds(pl.multiple_of(i * piece, piece), piece)
        r.tail[rows, :] = (mm(r.bcall[i], from_bc) + mm(r.gdt[rows, :], from_dt)).astype(BF16)

    weight_grad(r.tail, r.gradt)
    step(t_flow, sb_flow, sx_flow)
    own_bc = r.bcall[q]
    for i in range(dps):
        cols = slice(i * share, (i + 1) * share)
        grad = mm(own_bc, r.wt[i, 0:state2, :])
        at = pl.ds(pl.multiple_of(q * piece + HALO, 16), piece)
        r.sp[:, cols] += jnp.sum(grad * r.xn[i, at, :].astype(F32), 0, keepdims=True)
        r.yl[i * piece : (i + 1) * piece, 0:share] = grad
    r.sp[...] = r.sp[...] / pre
    step(sp_flow, t_flow, *out_flows)
    step(sp_flow, t_flow)
    step(*z_flows)
    step(sp_flow, sx_flow, sb_flow, *out_flows)
    finish(*x_flows, t_flow, sp_flow, *out_flows, *z_flows, sx_flow, sb_flow, gn_flow)
    for copy in own_copies:
        copy.wait()
    for i in range(dps):
        cols = slice(i * share, (i + 1) * share)
        r.gn_own[:, cols] += r.yl[i * piece : (i + 1) * piece, 0:share]

    @pl.loop(0, piece // few)
    def _(i):
        rows = pl.ds(pl.multiple_of(i * few, few), few)
        wide = r.hown[rows, :].astype(F32)
        r.op_own[rows, :] = wide + r.op_own[rows, :]
        inv_rms = lax.rsqrt(jnp.mean(wide * wide, -1, keepdims=True) + EPSILON)
        unit = wide * inv_rms
        grad = r.gn_own[rows, :] * pre
        r.gn_own[rows, :] = r.oown[rows, :].astype(F32) + inv_rms * (
            grad - unit * jnp.mean(grad * unit, -1, keepdims=True)
        )

    for copy in kept:
        copy.wait()
    for i in range(quads):
        place = jnp.logical_or(bc_rows(i), dt_rows(i)).astype(BF16)
        piece_t = mm(place, r.ttot[i], TN)
        r.tstage[...] = piece_t.astype(BF16) if i == 0 else (r.tstage[...].astype(F32) + piece_t).astype(BF16)
    last = keeper(r.tstage.at[pl.ds(0, tail_rows)], r.in_out.at[pl.ds(2 * inner, tail_rows)], 12)
    last.start()
    for i in range(quads):
        cols = slice(i * width, (i + 1) * width)
        r.cxw[:, cols] = r.sxall[i, 0:4, :]
        r.cxb[:, cols] = r.sxall[i, 4:5, :]
        r.norm[:, cols] = r.sxall[i, 5:6, :]
    total = r.sball[0]
    every = r.spall[0]
    lane = lax.broadcasted_iota(jnp.int32, (8, 128), 1)
    packed = jnp.where(lane < own_heads, r.sball[0, :, 0:128], 0.0)
    for i in range(1, quads):
        total = total + r.sball[i]
        every = every + r.spall[i]
        moved = jnp.where(lane < own_heads, r.sball[i, :, 0:128], 0.0)
        packed = packed + pltpu.roll(moved, i * own_heads, 1)
    r.cbw[...] = total[0:4]
    r.cbb[...] = total[4:5]
    r.head[...] = packed
    r.pre[...] = every
    last.wait()
    links.drain()


def remote_call(kernel, ident, outs, any_inputs, any_outputs, scratch, flops=2 * 10**10):
    vmem, anywhere = pl.BlockSpec(memory_space=pltpu.VMEM), pl.BlockSpec(memory_space=pltpu.HBM)

    def run(*args):
        moved = sum(a.size * a.dtype.itemsize for a in (*args, *outs))
        return pl.pallas_call(
            kernel,
            out_shape=tuple(outs),
            in_specs=[anywhere if i in any_inputs else vmem for i in range(len(args))],
            out_specs=tuple([anywhere if i in any_outputs else vmem for i in range(len(outs))]),
            scratch_shapes=list(scratch),
            compiler_params=pltpu.CompilerParams(
                vmem_limit_bytes=67043328, collective_id=ident, has_side_effects=True
            ),
            cost_estimate=pl.CostEstimate(flops=flops, bytes_accessed=moved, transcendentals=0),
        )(*args)

    return run


def on_device(
    hidden_in, pre_gain, in_weight, conv_x_weight, conv_x_bias, conv_bc_weight, conv_bc_bias,
    dt_bias, a_log, skip, norm_gain, out_weight, output_gradient,
):
    dp, quads, rank = lax.axis_size("dp"), lax.axis_size("quad"), lax.axis_index("dp")
    _, local, model = hidden_in.shape
    inner, state2, heads = conv_x_bias.shape[0], conv_bc_bias.shape[0], dt_bias.shape[0]
    width, own_heads = inner // quads, heads // quads
    tokens, share, columns = local * quads, model // dp, in_weight.shape[1]

    def spaced(v):
        return lax.dynamic_update_slice_in_dim(
            jnp.zeros((v.shape[0] * dp,), F32), v.astype(F32), rank * v.shape[0], 0
        )

    gain_row = jnp.concatenate([spaced(pre_gain), spaced(norm_gain)])[None]
    per_head = jnp.pad(jnp.stack([dt_bias, a_log, skip]), ((0, 5), (0, 128 - heads)))
    tail_rows = columns - 2 * inner
    tail_wide = tail_rows + -tail_rows % 128

    def sds(shape, dtype=F32):
        return jax.ShapeDtypeStruct(shape, dtype)

    def vm(*shape):
        return pltpu.VMEM(shape, F32)

    def vb(*shape):
        return pltpu.VMEM(shape, BF16)

    rows, own_out, steps = HALO + tokens, width // dp, len(bits_of(dp)) + 1
    levels = len(bits_of(quads))
    scratch = dict(
        wz=vb(dp, width, share), wx=vb(dp, width, share), wt=vb(dp, tail_wide, share),
        wo=vb(width, model), xn=vb(dp, rows, share), og=vb(quads, local, model),
        hid=vb(quads, local, model), px=vb(rows, width), pt=vb(rows, tail_wide), pd=vb(rows, 128),
        xs=vm(tokens + 8, width), bc=vm(tokens, state2), dt=vm(tokens, 128), cum=vm(tokens, 128),
        y=vb(tokens, width), yl=vm(tokens, width), states=vm(tokens // BLOCK, 128, width),
        z=vb(tokens, width), gm=vm(tokens, width), mixed=vb(tokens, width),
        dbc=vm(tokens + 8, state2), gdt=vb(tokens, 128), bcs=vm(quads, local, state2),
        bcbox=vm(quads - 1, local, state2), bcall=vb(quads, local, state2), tail=vb(tokens, 128),
        wtail=vb(dp, 128, share), grad=vb(dp, width, share), gradt=vb(dp, 128, share),
        zbox=vb(dp - 1, width, share), zpair=vb(width, share),
        xpair=vb(width, share),
        tbox=vb(dp - 1, 128, share), tpair=vb(128, share),
        obox=vb(2, dp - 1, own_out, model // 2), opair=vb(2, own_out, model // 2),
        opbox=vb(quads - 1, local, model),
        ttot=vb(quads, 128, share), tstage=vb(tail_wide, share),
        gain=vm(dp, *gain_row.shape), halo=vb(HALO, model), fin=vm(128, width), enter=vm(128, width),
        ds=vm(128, width), stat=vm(levels + 1, 8, tokens), statbox=vm(levels, 8, tokens),
        dscore=vm(BLOCK, BLOCK), heads=vm(8, 128), sx=vm(8, width), sb=vm(8, state2), sp=vm(1, model),
        sxbox=vm(steps, 8, width), sbbox=vm(steps, 8, state2), spbox=vm(steps, 1, model),
        sxall=vm(quads, 8, width), sball=vm(quads, 8, state2), spall=vm(quads, 1, model),
        hx=vm(8, width), hb=vm(8, state2), dsin=vm(128, width), hown=vb(local, model), oown=vb(local, model),
        wxc=vm(4, width), bxc=vm(1, width), dtb=vm(1, 128), alog=vm(1, 128), skip=vm(1, width),
        send=pltpu.SemaphoreType.DMA((192,)), recv=pltpu.SemaphoreType.DMA((192,)),
        local=pltpu.SemaphoreType.DMA((16,)),
    )
    (
        in_out, out_out, op_own, gn_own, conv_x_grad, conv_x_bias_grad, norm_grad, conv_bc_grad,
        conv_bc_bias_grad, head_grad, pre_grad,
    ) = remote_call(
        functools.partial(block_kernel, width, own_heads, heads), 0,
        [
            sds((columns, share), BF16), sds((quads, own_out, model), BF16), sds((local, model)),
            sds((local, model)), sds((4, inner)), sds((1, inner)), sds((1, inner)), sds((4, state2)),
            sds((1, state2)), sds((8, 128)), sds((1, model)),
        ],
        range(5), range(2), [scratch[name] for name in SCRATCH],
    )(
        in_weight.T, out_weight, hidden_in[0], output_gradient[0], gain_row, conv_x_weight,
        conv_x_bias[None], conv_bc_weight, conv_bc_bias[None], per_head,
    )
    return (
        op_own[None], gn_own[None],
        lax.dynamic_slice_in_dim(pre_grad[0], rank * share, share, 0), in_out.T.astype(F32),
        conv_x_grad, conv_x_bias_grad[0], conv_bc_grad, conv_bc_bias_grad[0],
        head_grad[5, :heads], head_grad[6, :heads], head_grad[7, :heads],
        lax.dynamic_slice_in_dim(norm_grad[0], rank * (inner // dp), inner // dp, 0),
        out_out.reshape(width, model).astype(F32),
    )


def solution(mesh):
    dp, seq = mesh.shape["dp"], mesh.shape["seq"]
    fine = Mesh(mesh.devices.reshape(dp, 2, seq // 2), ("dp", "pair", "quad"))
    tokens, whole, rows = P("dp", ("pair", "quad"), None), P(), P("dp", None)
    return jax.shard_map(
        on_device,
        mesh=fine,
        in_specs=(
            tokens, P("dp"), rows, whole, whole, whole, whole, whole, whole, whole, P("dp"), rows, tokens,
        ),
        out_specs=(
            tokens, tokens, P("dp"), rows, whole, whole, whole, whole, whole, whole, whole, P("dp"), rows,
        ),
        check_vma=False,
    )
```

```python
import functools
import types

import jax
import jax.numpy as jnp
from jax import lax
from jax.experimental import pallas as pl
from jax.experimental.pallas import tpu as pltpu
from jax.sharding import Mesh
from jax.sharding import PartitionSpec as P

EPSILON = 1e-05
BLOCK = 256
HALO = 16
F32 = jnp.float32
BF16 = jnp.bfloat16
NN = ((1,), (0,))
NT = ((1,), (1,))
TN = ((0,), (0,))


def mm(a, b, dims=NN):
    return lax.dot_general(
        a.astype(BF16), b.astype(BF16), (dims, ((), ())), preferred_element_type=F32
    )


def split(a):
    high = a.astype(BF16)
    return high, (a - high.astype(F32)).astype(BF16)


def mm3(a, b, dims=NN):
    ah, al = split(a)
    bh, bl = split(b)
    return mm(ah, bh, dims) + (mm(ah, bl, dims) + mm(al, bh, dims))


def mm_exact(a, b, dims=NN):
    b0 = b.astype(BF16)
    r1 = b - b0.astype(F32)
    b1 = r1.astype(BF16)
    b2 = (r1 - b1.astype(F32)).astype(BF16)
    return mm(a, b0, dims) + (mm(a, b1, dims) + mm(a, b2, dims))


def mm_sum(a, b, dims=NN):
    ah, al = split(a)
    return mm(ah, b, dims) + mm(al, b, dims)


def sigmoid(v):
    return 1.0 / (1.0 + jnp.exp(-v))


def lane_mask(width, first):
    lane = lax.broadcasted_iota(jnp.int32, (1, 128), 1)
    return (lane < 64) if first else (lane >= 64)


def expand(v, pair):
    lane = lax.broadcasted_iota(jnp.int32, (1, 128), 1)
    return jnp.where(lane < 64, v[:, 2 * pair : 2 * pair + 1], v[:, 2 * pair + 1 : 2 * pair + 2])


def lower_mask():
    return lax.broadcasted_iota(jnp.int32, (BLOCK, BLOCK), 0) >= lax.broadcasted_iota(
        jnp.int32, (BLOCK, BLOCK), 1
    )


def head_indicator(pair):
    row = lax.broadcasted_iota(jnp.int32, (128, 128), 0)
    col = lax.broadcasted_iota(jnp.int32, (128, 128), 1)
    return (col == 2 * pair + row // 64).astype(BF16)


def conv_block(p_ref, row, col, w_ref, b_ref, wcol):
    raw = p_ref[pl.ds(row, BLOCK + HALO), col : col + 128].astype(F32)
    shifted = [raw[HALO - 3 + k : HALO - 3 + k + BLOCK] for k in range(4)]
    pre = b_ref[0:1, wcol : wcol + 128]
    for k in range(4):
        pre = pre + w_ref[k : k + 1, wcol : wcol + 128] * shifted[k]
    return pre, shifted


def run_hooks(hooks, at):
    for index, hook in hooks.items():
        pl.when(at == index)(hook)


def prep_pass(width, px_ref, pt_ref, pd_ref, wx_ref, bx_ref, wb_ref, bb_ref, dtb_ref, alog_ref,
              xs_ref, bc_ref, dt_ref, cum_ref, fin_ref, hooks):
    blocks = xs_ref.shape[0] // BLOCK
    rate = -jnp.exp(alog_ref[...])
    fin_ref[...] = jnp.zeros_like(fin_ref)

    def step(b, carry):
        row = pl.multiple_of(b * BLOCK, BLOCK)
        for c in range(2):
            pre, _ = conv_block(pt_ref, row, 128 * c, wb_ref, bb_ref, 128 * c)
            bc_ref[pl.ds(row, BLOCK), 128 * c : 128 * c + 128] = pre * sigmoid(pre)
        raw = pd_ref[pl.ds(row + HALO, BLOCK), :].astype(F32)
        raw = raw + dtb_ref[...]
        dt = jnp.maximum(raw, 0.0) + jnp.log1p(jnp.exp(-jnp.abs(raw)))
        cum = mm_exact(lower_mask().astype(F32), dt * rate)
        dt_ref[pl.ds(row, BLOCK), :] = dt
        cum_ref[pl.ds(row, BLOCK), :] = cum
        last = cum[BLOCK - 1 : BLOCK, :]
        weight = dt * jnp.exp(last - cum)
        decay = jnp.exp(last)
        keys_t = bc_ref[pl.ds(row, BLOCK), 0:128].T
        for pair in range(width // 128):
            cols = slice(128 * pair, 128 * pair + 128)
            pre, _ = conv_block(px_ref, row, 128 * pair, wx_ref, bx_ref, 128 * pair)
            xs = pre * sigmoid(pre)
            xs_ref[pl.ds(row, BLOCK), cols] = xs
            fin_ref[:, cols] = fin_ref[:, cols] * expand(decay, pair) + mm3(
                keys_t, xs * expand(weight, pair)
            )
        run_hooks(hooks, b)
        return carry

    lax.fori_loop(0, blocks, step, 0)


def inside_pass(width, xs_ref, bc_ref, dt_ref, cum_ref, yl_ref, hooks):
    def step(b, carry):
        rows = pl.ds(pl.multiple_of(b * BLOCK, BLOCK), BLOCK)
        dt, cum = dt_ref[rows, :], cum_ref[rows, :]
        cum_t = cum.T
        scores = mm3(bc_ref[rows, 128:256], bc_ref[rows, 0:128], NT)
        mask = lower_mask()
        for pair in range(width // 128):
            cols = slice(128 * pair, 128 * pair + 128)
            stepped = xs_ref[rows, cols] * expand(dt, pair)
            y = jnp.zeros((BLOCK, 128), F32)
            for half in range(2):
                h = 2 * pair + half
                spread = cum[:, h : h + 1] - cum_t[h : h + 1, :]
                table = jnp.exp(jnp.where(mask, spread, -1e30))
                part = jnp.where(lane_mask(128, half == 0), stepped, 0.0)
                y = y + mm3(scores * table, part)
            yl_ref[rows, cols] = y
        run_hooks(hooks, b)
        return carry

    lax.fori_loop(0, xs_ref.shape[0] // BLOCK, step, 0)


def outside_pass(
    width, xs_ref, bc_ref, dt_ref, cum_ref, skip_ref, y_ref, yl_ref, states_ref, s_ref, hooks
):
    def step(b, carry):
        rows = pl.ds(pl.multiple_of(b * BLOCK, BLOCK), BLOCK)
        dt, cum = dt_ref[rows, :], cum_ref[rows, :]
        last = cum[BLOCK - 1 : BLOCK, :]
        grow, decay = jnp.exp(cum), jnp.exp(last)
        weight = dt * jnp.exp(last - cum)
        queries = bc_ref[rows, 128:256]
        keys_t = bc_ref[rows, 0:128].T
        for pair in range(width // 128):
            cols = slice(128 * pair, 128 * pair + 128)
            xs = xs_ref[rows, cols]
            state = s_ref[:, cols]
            states_ref[b, :, cols] = state
            y = yl_ref[rows, cols] + expand(grow, pair) * mm3(queries, state)
            s_ref[:, cols] = state * expand(decay, pair) + mm3(keys_t, xs * expand(weight, pair))
            yl_ref[rows, cols] = y
            y_ref[rows, cols] = (y + skip_ref[0:1, cols] * xs).astype(BF16)
        run_hooks(hooks, b)
        return carry

    lax.fori_loop(0, xs_ref.shape[0] // BLOCK, step, 0)


MESH = pl.DeviceIdType.MESH


def bits_of(count):
    return [1 << i for i in range(count.bit_length() - 1)]


def bit_at(index, bit):
    return (index // bit) % 2


def flip(index, bits):
    for bit in bits:
        index = index + bit * (1 - 2 * bit_at(index, bit))
    return index


def subsets(bits):
    found = [frozenset()]
    for bit in bits:
        found = found + [f | {bit} for f in found]
    return found


class Links:
    def __init__(self, send, recv):
        self.send, self.recv, self.count, self.open = send, recv, 0, []

    def make(self, src, dst, target):
        index, self.count = self.count, self.count + 1
        return pltpu.make_async_remote_copy(
            src_ref=src, dst_ref=dst, send_sem=self.send.at[index], recv_sem=self.recv.at[index],
            device_id=target, device_id_type=MESH,
        )

    def stage(self, copies, after=None):
        def begin():
            for copy in copies:
                copy.start()
                self.open.append(lambda copy=copy: copy.wait_send())

        def end():
            for copy in copies:
                copy.wait_recv()
            if after is not None:
                after()

        return begin, end

    def stage_if(self, copy, sends, takes):
        def left():
            pl.when(sends)(copy.wait_send)

        def begin():
            pl.when(sends)(copy.start)
            self.open.append(left)

        def end():
            pl.when(takes)(copy.wait_recv)

        return begin, end

    def drain(self):
        for left in self.open:
            left()
        self.open = []


def meet(targets):
    barrier = pltpu.get_barrier_semaphore()
    for target in targets:
        pl.semaphore_signal(barrier, inc=1, device_id=target, device_id_type=MESH)
    pl.semaphore_wait(barrier, len(targets))


def neighbours(axis):
    me = lax.axis_index(axis)
    return [{axis: flip(me, (bit,))} for bit in bits_of(lax.axis_size(axis))]


class Flow:
    def __init__(self, links, stages):
        self.links, self.stages, self.at, self.sent = links, stages, -1, []

    def go(self):
        if 0 <= self.at < len(self.stages):
            self.stages[self.at][1]()
        self.at += 1
        if self.at < len(self.stages):
            before = len(self.links.open)
            self.stages[self.at][0]()
            self.sent += self.links.open[before:]

    def drain(self):
        for left in self.sent:
            left()
        done = {id(left) for left in self.sent}
        self.links.open = [left for left in self.links.open if id(left) not in done]
        self.sent = []

    def finish(self):
        while self.at < len(self.stages):
            self.go()


def step(*flows):
    for flow in flows:
        flow.go()


def finish(*flows):
    while any(flow.at < len(flow.stages) for flow in flows):
        for flow in flows:
            if flow.at < len(flow.stages):
                flow.go()


def add_rows(out, a, b):
    rows = out.shape[0]
    step = 16 if rows % 16 == 0 else 8
    while out.shape[1] * step * 2 <= 24576 and rows % (2 * step) == 0:
        step *= 2

    @pl.loop(0, rows // step)
    def _(i):
        at = pl.ds(pl.multiple_of(i * step, step), step)
        out[at, :] = (a[at, :].astype(F32) + b[at, :].astype(F32)).astype(out.dtype)


def gather_stages(links, axis, order, own, slot):
    me = lax.axis_index(axis)
    held, stages = [frozenset()], []
    for bit in order:
        target = {axis: flip(me, (bit,))}
        stages.append(
            links.stage([
                links.make(slot(flip(me, f)) if f else own, slot(flip(me, f)), target) for f in held
            ])
        )
        held = held + [f | {bit} for f in held]
    return stages


def reduce_stages(links, axis, order, source, inbox, final=None):
    me = lax.axis_index(axis)
    base, stages = 0, []
    blocks = {f: source(flip(me, f)) for f in subsets(order)}
    for stage, bit in enumerate(order):
        keep = subsets(order[stage + 1 :])
        target = {axis: flip(me, (bit,))}
        boxes = [inbox(base + k) for k in range(len(keep))]
        outs = [final] if final is not None and stage == len(order) - 1 else boxes
        copies = [links.make(blocks[f | {bit}], box, target) for f, box in zip(keep, boxes)]

        def after(mine=[blocks[f] for f in keep], boxes=boxes, outs=outs):
            for a, b, out in zip(mine, boxes, outs):
                add_rows(out, a, b)

        stages.append(links.stage(copies, after))
        blocks = dict(zip(keep, outs))
        base += len(keep)
    return stages


def spread_stages(links, order, block):
    d, q = lax.axis_index("dp"), lax.axis_index("quad")
    away = {bit: bit_at(d, bit) != bit_at(q, bit) for bit in order}
    stages = []
    for stage, bit in enumerate(order):
        reached = jnp.bool_(True)
        for later in order[stage + 1 :]:
            reached = jnp.logical_and(reached, jnp.logical_not(away[later]))
        holder = jnp.logical_and(reached, jnp.logical_not(away[bit]))
        taker = jnp.logical_and(reached, away[bit])
        copy = links.make(block, block, {"dp": flip(d, (bit,))})
        stages.append(links.stage_if(copy, holder, taker))
    return stages


def leave_pass(width, bc_ref, cum_ref, gy_ref, out_ref):
    blocks = gy_ref.shape[0] // BLOCK
    out_ref[...] = jnp.zeros_like(out_ref)

    def step(i, carry):
        rows = pl.ds(pl.multiple_of((blocks - 1 - i) * BLOCK, BLOCK), BLOCK)
        cum = cum_ref[rows, :]
        grow, decay = jnp.exp(cum), jnp.exp(cum[BLOCK - 1 : BLOCK, :])
        queries_t = bc_ref[rows, 128:256].T
        for pair in range(width // 128):
            cols = slice(128 * pair, 128 * pair + 128)
            dy = gy_ref[rows, cols].astype(F32)
            out_ref[:, cols] = out_ref[:, cols] * expand(decay, pair) + mm3(
                queries_t, expand(grow, pair) * dy
            )
        return carry

    lax.fori_loop(0, blocks, step, 0)


def back_inside_pass(width, r, hooks):
    def step(b, carry):
        rows = pl.ds(pl.multiple_of(b * BLOCK, BLOCK), BLOCK)
        dt, cum = r.dt[rows, :], r.cum[rows, :]
        cum_t = cum.T
        keys, queries = r.bc[rows, 0:128], r.bc[rows, 128:256]
        scores = mm3(queries, keys, NT)
        mask = lower_mask()
        r.dscore[...] = jnp.zeros_like(r.dscore)
        for pair in range(width // 128):
            cols = slice(128 * pair, 128 * pair + 128)
            stepped, stepped_low = split(r.xs[rows, cols] * expand(dt, pair))
            dy = r.y[rows, cols].astype(F32)
            dstep = jnp.zeros((BLOCK, 128), F32)
            for half in range(2):
                h = 2 * pair + half
                spread = cum[:, h : h + 1] - cum_t[h : h + 1, :]
                table = jnp.exp(jnp.where(mask, spread, -1e30))
                part = jnp.where(lane_mask(128, half == 0), dy, 0.0).astype(BF16)
                dmix = mm(part, stepped, NT) + mm(part, stepped_low, NT)
                r.dscore[...] += dmix * table
                high, low = split(scores * table)
                dstep = dstep + (mm(high, part, TN) + mm(low, part, TN))
            r.gm[rows, cols] = dstep
        r.dbc[rows, 0:128] = mm3(r.dscore[...], queries, TN)
        r.dbc[rows, 128:256] = mm3(r.dscore[...], keys)
        run_hooks(hooks, b)
        return carry

    lax.fori_loop(0, r.y.shape[0] // BLOCK, step, 0)


def back_outside_pass(width, r, hooks):
    blocks = r.y.shape[0] // BLOCK
    rate = -jnp.exp(r.alog[...])
    r.heads[...] = jnp.zeros_like(r.heads)

    def step(i, carry):
        b = blocks - 1 - i
        row = pl.multiple_of(b * BLOCK, BLOCK)
        rows = pl.ds(row, BLOCK)
        dt, cum = r.dt[rows, :], r.cum[rows, :]
        last = cum[BLOCK - 1 : BLOCK, :]
        grow, decay, tail = jnp.exp(cum), jnp.exp(last), jnp.exp(last - cum)
        keys, queries = r.bc[rows, 0:128], r.bc[rows, 128:256]
        queries_t = queries.T
        dkeys, dqueries = r.dbc[rows, 0:128], r.dbc[rows, 128:256]
        dcum = jnp.zeros((BLOCK, 128), F32)
        ddt = jnp.zeros((BLOCK, 128), F32)
        dlast = jnp.zeros((8, 128), F32)
        dskip = jnp.zeros((8, 128), F32)
        for pair in range(width // 128):
            cols = slice(128 * pair, 128 * pair + 128)
            xs = r.xs[rows, cols]
            dt_e = expand(dt, pair)
            stepped = xs * dt_e
            dy = r.y[rows, cols].astype(F32)
            state, ds = r.states[b, :, cols], r.ds[:, cols]
            tail_e = expand(tail, pair)
            carried = mm3(keys, ds) * tail_e
            dstep = r.gm[rows, cols] + carried
            dkeys = dkeys + mm3(stepped * tail_e, ds, NT)
            grown = expand(grow, pair) * dy
            dqueries = dqueries + mm3(grown, state, NT)
            decay_e = expand(decay, pair)
            ends = jnp.sum(stepped * carried, 0, keepdims=True) + decay_e * jnp.sum(
                ds * state, 0, keepdims=True
            )
            r.ds[:, cols] = ds * decay_e + mm3(queries_t, grown)
            dxs = dstep * dt_e + r.skip[0:1, cols] * dy
            which = head_indicator(pair)
            ddt = ddt + mm_sum(dstep * xs, which)
            dcum = dcum + mm_sum(dy * r.yl[rows, cols] - stepped * dstep, which)
            dlast = dlast + mm_sum(jnp.broadcast_to(ends, (8, 128)), which)
            skips = jnp.sum(dy * xs, 0, keepdims=True)
            dskip = dskip + mm_sum(jnp.broadcast_to(skips, (8, 128)), which)
            pre, shifted = conv_block(r.px, row, 128 * pair, r.wxc, r.bxc, 128 * pair)
            sig = sigmoid(pre)
            dpre = dxs * sig * (1.0 + pre * (1.0 - sig))
            r.xs[rows, cols] = dpre
            for k in range(4):
                r.sx[k : k + 1, cols] += jnp.sum(dpre * shifted[k], 0, keepdims=True)
            r.sx[4:5, cols] += jnp.sum(dpre, 0, keepdims=True)
        at_end = lax.broadcasted_iota(jnp.int32, (BLOCK, 128), 0) == BLOCK - 1
        dcum = dcum + jnp.where(at_end, dlast[0:1], 0.0)
        dlog = mm_exact(lower_mask().astype(F32), dcum, TN)
        raw = r.pd[pl.ds(row + HALO, BLOCK), :].astype(F32)
        draw = (ddt + dlog * rate) * sigmoid(raw + r.dtb[...])
        r.gdt[rows, :] = draw.astype(BF16)
        r.heads[0:1, :] += jnp.sum(draw, 0, keepdims=True)
        r.heads[1:2, :] += jnp.sum(dlog * dt, 0, keepdims=True) * rate
        r.heads[2:3, :] += dskip[0:1]
        for c, grad in enumerate((dkeys, dqueries)):
            cols = slice(128 * c, 128 * c + 128)
            pre, shifted = conv_block(r.pt, row, 128 * c, r.wbc, r.bbc, 128 * c)
            sig = sigmoid(pre)
            dpre = grad * sig * (1.0 + pre * (1.0 - sig))
            r.dbc[rows, cols] = dpre
            for k in range(4):
                r.sb[k : k + 1, cols] += jnp.sum(dpre * shifted[k], 0, keepdims=True)
            r.sb[4:5, cols] += jnp.sum(dpre, 0, keepdims=True)
        run_hooks(hooks, i)
        return carry

    lax.fori_loop(0, blocks, step, 0)


INPUTS = (
    "win", "wo_in", "hid_in", "og_in", "gain_in", "wx_all", "bx_all", "wbc", "bbc", "per_head",
)
OUTPUTS = (
    "in_out", "out_out", "op_own", "gn_own", "cxw", "cxb", "norm", "cbw", "cbb", "head", "pre",
)
SCRATCH = (
    "wz", "wx", "wt", "wo", "xn", "og", "hid", "px", "pt", "pd", "xs", "bc", "dt", "cum", "y", "yl", "states", "z", "gm", "mixed", "dbc", "gdt", "bcs", "bcbox", "bcall", "tail", "wtail", "grad", "gradt", "zbox", "zpair", "xpair", "tbox", "tpair", "obox", "opair", "opbox", "ttot", "tstage", "gain", "halo", "fin", "enter", "ds", "stat", "statbox", "dscore", "heads", "sx", "sb", "sp", "sxbox", "sbbox", "spbox", "sxall", "sball", "spall", "hx", "hb", "dsin", "hown", "oown", "wxc", "bxc", "dtb", "alog", "skip", "send", "recv", "local",
)


def block_kernel(width, own_heads, heads, *refs):
    r = types.SimpleNamespace(**dict(zip((*INPUTS, *OUTPUTS, *SCRATCH), refs, strict=True)))
    d, q, p = lax.axis_index("dp"), lax.axis_index("quad"), lax.axis_index("pair")
    dps, quads = lax.axis_size("dp"), lax.axis_size("quad")
    tokens, piece, model = r.y.shape[0], r.hid.shape[1], r.hid.shape[2]
    inner, share, state2 = width * quads, model // dps, r.bc.shape[1]
    bc_cols = state2 // quads
    links = Links(r.send, r.recv)
    dp_bits, up = bits_of(dps), bits_of(quads)
    orders, down = (dp_bits, dp_bits[::-1]), up[::-1]
    other, swapped = {"pair": flip(p, (1,))}, {"dp": q, "quad": d}
    near = neighbours("dp") + neighbours("quad") + neighbours("pair")
    sides = ((0, width // 2), (width // 2, width // 2))
    tail_rows = r.win.shape[0] - 2 * inner
    cut = tail_rows // 32 * 16 + 16
    tail_sides = ((0, cut), (cut, tail_rows - cut))
    lane_row = lax.broadcasted_iota(jnp.int32, (128, 128), 0)
    lane_col = lax.broadcasted_iota(jnp.int32, (128, 128), 1)
    first_half, second_half = p == 0, p > 0

    @pl.when(d == q)
    def _():
        meet(near)

    @pl.when(d != q)
    def _():
        meet([*near, swapped])

    def win_rows(base, at, size):
        return r.win.at[pl.ds(pl.multiple_of(base + q * width + at, 16), size)]

    def tail_source(at, size):
        return r.win.at[pl.ds(2 * inner + at, size)]

    def weights(source, out, parts):
        return [
            Flow(links, gather_stages(
                links, "dp", order, source(at, size),
                lambda i, at=at, size=size: out.at[i, pl.ds(at, size)],
            ))
            for order, (at, size) in zip(orders, parts)
        ]

    gain_flow = Flow(links, gather_stages(links, "dp", dp_bits, r.gain_in, lambda i: r.gain.at[i]))
    hid_flow = Flow(links, gather_stages(links, "quad", down, r.hid_in, lambda i: r.hid.at[i]))
    og_flow = Flow(links, gather_stages(links, "quad", down, r.og_in, lambda i: r.og.at[i]))
    wt_flows = weights(tail_source, r.wt, tail_sides)
    wx_flows = weights(lambda at, size: win_rows(inner, at, size), r.wx, sides)
    wz_flows = weights(lambda at, size: win_rows(0, at, size), r.wz, sides)
    parts = 4
    wo_flows = [
        Flow(links, spread_stages(links, dp_bits[::-1], r.wo.at[pl.ds(k * (width // parts), width // parts)]))
        for k in range(parts)
    ]
    tail = r.hid.at[quads - 1, pl.ds(piece - HALO, HALO)]
    halo_flow = Flow(links, [links.stage_if(links.make(tail, r.halo, other), first_half, second_half)])
    state_flow = Flow(links, [links.stage_if(links.make(r.fin, r.enter, other), first_half, second_half)])
    ds_flow = Flow(links, [links.stage_if(links.make(r.fin, r.dsin, other), second_half, first_half)])
    edge_flows = [
        Flow(links, [links.stage_if(links.make(a.at[pl.ds(0, 8)], b, other), second_half, first_half)])
        for a, b in ((r.xs, r.hx), (r.dbc, r.hb))
    ]
    stat_flow = Flow(links, [
        links.stage(
            [links.make(r.stat.at[k], r.statbox.at[k], {"quad": flip(q, (bit,))})],
            lambda k=k: r.stat.at[k + 1].__setitem__(..., r.stat[k] + r.statbox[k]),
        )
        for k, bit in enumerate(up)
    ])
    kept = []

    def keeper(own, place, index):
        return pltpu.make_async_copy(own, place, r.local.at[index])

    def in_flow(h, at, size, part_ref, box, pair_box, slot, index):
        rows = pl.ds(at, size)
        stages = reduce_stages(
            links, "dp", orders[h], lambda i: part_ref.at[i, rows], lambda k: box.at[k, rows]
        )
        mine, own = box.at[dps - 2, rows], pair_box.at[rows]
        keep = keeper(own, slot(q), index)

        def after():
            add_rows(own, mine, own)
            keep.start()
            kept.append(keep)

        stages.append(links.stage([links.make(mine, own, other)], after))
        return Flow(links, stages + gather_stages(links, "quad", down, own, slot))

    def columns_slot(base, at, size):
        return lambda i: r.in_out.at[pl.ds(pl.multiple_of(base + i * width + at, 16), size)]

    def out_flow(h):
        half = model // 2
        part, size = pl.ds(h * half, half), width // dps
        stages = reduce_stages(
            links, "dp", orders[h],
            lambda i: r.wo.at[pl.ds(pl.multiple_of(i * size, 16), size), part],
            lambda k: r.obox.at[h, k],
        )
        mine, whole = r.obox.at[h, dps - 2], r.opair.at[h]
        place = r.out_out.at[d, :, part]
        stages.append(
            links.stage([links.make(mine, whole, other)], lambda: add_rows(whole, mine, whole))
        )
        near_copy = pltpu.make_async_copy(whole, place, r.local.at[14 + h])
        far_copy = links.make(whole, place, swapped)

        def begin():
            pl.when(d == q)(near_copy.start)
            pl.when(d != q)(far_copy.start)

        def end():
            pl.when(d == q)(near_copy.wait)
            pl.when(d != q)(far_copy.wait)

        stages.append((begin, end))
        return Flow(links,
            stages
            + gather_stages(
                links, "quad", down, r.out_out.at[q, :, part], lambda i: r.out_out.at[i, :, part]
            )
        )

    def row_sum_flow(source, box, final):
        return Flow(links, reduce_stages(
            links, "quad", up, lambda i: source.at[i], lambda k: box.at[k], final
        ))

    def small_flow(mine, box, every):
        current, stages = mine, []
        steps = [("dp", bit) for bit in dp_bits] + [("pair", 1)]
        for k, (axis, bit) in enumerate(steps):
            target = {axis: flip(lax.axis_index(axis), (bit,))}
            out = box.at[k] if k < len(steps) - 1 else every.at[q]

            def after(out=out, current=current, k=k):
                out[...] = current[...] + box[k]

            stages.append(links.stage([links.make(current, box.at[k], target)], after))
            current = out
        return Flow(links,
            stages + gather_stages(links, "quad", down, every.at[q], lambda i: every.at[i])
        )

    z_flows = [
        in_flow(h, at, size, r.grad, r.zbox, r.zpair, columns_slot(0, at, size), 7 + h)
        for h, (at, size) in enumerate(sides)
    ]
    x_flows = [
        in_flow(h, at, size, r.grad, r.zbox, r.xpair, columns_slot(inner, at, size), 9 + h)
        for h, (at, size) in enumerate(sides)
    ]
    t_flow = in_flow(0, 0, 128, r.gradt, r.tbox, r.tpair, lambda i: r.ttot.at[i], 11)
    out_flows = [out_flow(0), out_flow(1)]
    op_flow = row_sum_flow(r.hid, r.opbox, r.op_own)
    gn_flow = row_sum_flow(r.og, r.opbox, r.gn_own)
    bc_flow = Flow(links,
        reduce_stages(links, "quad", up, lambda i: r.bcs.at[i], lambda k: r.bcbox.at[k], r.bcall.at[q])
        + gather_stages(links, "quad", down, r.bcall.at[q], lambda i: r.bcall.at[i])
    )
    sx_flow, sb_flow, sp_flow = (
        small_flow(r.sx, r.sxbox, r.sxall), small_flow(r.sb, r.sbbox, r.sball),
        small_flow(r.sp, r.spbox, r.spall),
    )

    step(gain_flow, hid_flow, *wt_flows, *wx_flows)
    owned = [
        (r.hid_in, r.hid.at[q]), (r.gain_in, r.gain.at[d]),
        (tail_source(0, tail_rows), r.wt.at[d, pl.ds(0, tail_rows)]),
        (win_rows(inner, 0, width), r.wx.at[d]), (win_rows(0, 0, width), r.wz.at[d]),
        (r.og_in, r.og.at[q]),
    ]
    copies = [pltpu.make_async_copy(a, b, r.local.at[i]) for i, (a, b) in enumerate(owned)]
    for copy in copies:
        copy.start()

    @pl.when(d == q)
    def _():
        copy = pltpu.make_async_copy(r.wo_in, r.wo, r.local.at[len(owned)])
        copy.start()
        copy.wait()

    for i in range(dps):
        r.wt[i, tail_rows:, :] = jnp.zeros((r.wt.shape[1] - tail_rows, share), BF16)
    r.sx[...] = jnp.zeros_like(r.sx)
    r.sb[...] = jnp.zeros_like(r.sb)
    own_cols = pl.ds(pl.multiple_of(q * width, 128), width)
    r.wxc[...] = r.wx_all[:, own_cols]
    r.bxc[...] = r.bx_all[:, own_cols]
    turned = r.per_head[...]
    for i in range(1, quads):
        turned = jnp.where(q == i, pltpu.roll(r.per_head[...], 128 - i * own_heads, 1), turned)
    r.dtb[...] = turned[0:1]
    r.alog[...] = turned[1:2]
    head_row = lax.broadcasted_iota(jnp.int32, (128, width), 0)
    head_col = lax.broadcasted_iota(jnp.int32, (128, width), 1)
    widen = (head_row == head_col // (width // own_heads)).astype(BF16)
    s0 = turned.astype(BF16)
    rest = turned - s0.astype(F32)
    s1 = rest.astype(BF16)
    s2 = (rest - s1.astype(F32)).astype(BF16)
    r.skip[...] = (mm(s0, widen) + mm(s1, widen) + mm(s2, widen))[2:3]
    for copy in copies:
        copy.wait()
    finish(gain_flow)
    step(hid_flow, *wt_flows, *wx_flows)
    step(*wz_flows, og_flow)
    step(*wo_flows)
    hid_flow.finish()
    step(halo_flow)
    halo_flow.finish()

    gains = r.gain[0]
    for i in range(1, dps):
        gains = gains + r.gain[i]
    pre = gains[:, :model]

    def normed(v):
        v = v.astype(F32)
        unit = v * lax.rsqrt(jnp.mean(v * v, -1, keepdims=True) + EPSILON)
        return (unit * pre).astype(BF16)

    def put_normed(at, rows, v):
        for i in range(dps):
            r.xn[i, pl.ds(at, rows), :] = v[:, i * share : (i + 1) * share]

    put_normed(0, HALO, jnp.where(p > 0, normed(r.halo[...]), jnp.zeros((HALO, model), BF16)))
    few = 32

    @pl.loop(0, tokens // few)
    def _(i):
        at = i * few
        rows = pl.ds(pl.multiple_of(at % piece, few), few)
        put_normed(pl.multiple_of(at + HALO, 16), few, normed(r.hid[at // piece, rows, :]))

    finish(*wt_flows, *wx_flows)

    def project(out_ref, out_at, at, rows, w_ref):
        total = jnp.zeros((rows, w_ref.shape[1]), F32)
        for i in range(dps):
            total = total + mm(r.xn[i, pl.ds(at, rows), :], w_ref[i], NT)
        out_ref[pl.ds(out_at, rows), :] = total.astype(BF16)

    for out_ref, w_ref in ((r.pt, r.wt), (r.px, r.wx)):
        project(out_ref, 0, 0, HALO, w_ref)

        @pl.loop(0, tokens // BLOCK)
        def _(i, out_ref=out_ref, w_ref=w_ref):
            at = pl.multiple_of(i * BLOCK + HALO, 16)
            project(out_ref, at, at, BLOCK, w_ref)

    pick = jnp.logical_and(lane_row == lane_col + q * own_heads, lane_col < own_heads).astype(BF16)
    r.pd[...] = mm(r.pt[:, state2 : state2 + 128], pick).astype(BF16)
    prep_pass(
        width, r.px, r.pt, r.pd, r.wxc, r.bxc, r.wbc, r.bbc, r.dtb, r.alog,
        r.xs, r.bc, r.dt, r.cum, r.fin, {0: lambda: step(*wz_flows, og_flow), 3: wo_flows[0].go},
    )
    step(state_flow)
    inside_pass(
        width, r.xs, r.bc, r.dt, r.cum, r.yl, {1: wo_flows[1].go, 3: wo_flows[2].go},
    )
    finish(*wz_flows)

    @pl.loop(0, tokens // BLOCK)
    def _(i):
        at = pl.multiple_of(i * BLOCK, BLOCK)
        project(r.z, at, pl.multiple_of(at + HALO, 16), BLOCK, r.wz)

    state_flow.finish()
    r.ds[...] = jnp.where(p > 0, r.enter[...], 0.0)
    outside_pass(
        width, r.xs, r.bc, r.dt, r.cum, r.skip, r.y, r.yl, r.states, r.ds, {1: wo_flows[3].go},
    )
    finish(og_flow, *wo_flows)

    @pl.loop(0, quads)
    def _(i):
        r.gm[pl.ds(pl.multiple_of(i * piece, piece), piece), :] = mm(r.og[i], r.wo[...], NT)

    norm_all = gains[:, model:]
    norm_own = norm_all[:, :width]
    for i in range(1, quads):
        norm_own = jnp.where(q == i, norm_all[:, i * width : (i + 1) * width], norm_own)
    chunk = 128

    @pl.loop(0, tokens // chunk)
    def _(i):
        rows = pl.ds(pl.multiple_of(i * chunk, chunk), chunk)
        gate = r.z[rows, :].astype(F32)
        gated = r.y[rows, :].astype(F32) * gate * sigmoid(gate)
        first = jnp.sum(gated * gated, -1, keepdims=True)
        second = jnp.sum(r.gm[rows, :] * norm_own * gated, -1, keepdims=True)
        lane = lax.broadcasted_iota(jnp.int32, (chunk, 128), 1)
        both = jnp.where(lane == 0, first, jnp.where(lane == 1, second, 0.0))
        r.stat[0, :, rows] = both.T[0:8, :]

    finish(stat_flow)

    @pl.loop(0, tokens // chunk)
    def _(i):
        rows = pl.ds(pl.multiple_of(i * chunk, chunk), chunk)
        stats = r.stat[len(up), :, rows]
        stats = jnp.concatenate([stats] * (128 // 8), 0).T
        out_rms = lax.rsqrt(stats[:, 0:1] / inner + EPSILON)
        mean_dot = out_rms * stats[:, 1:2] / inner
        gate = r.z[rows, :].astype(F32)
        y = r.y[rows, :].astype(F32)
        sig = sigmoid(gate)
        unit_gated = y * gate * sig * out_rms
        grad_mixed = r.gm[rows, :]
        r.mixed[rows, :] = (unit_gated * norm_own).astype(BF16)
        r.sx[5:6, :] += jnp.sum(grad_mixed * unit_gated, 0, keepdims=True)
        grad_gated = out_rms * (grad_mixed * norm_own - unit_gated * mean_dot)
        r.y[rows, :] = (grad_gated * gate * sig).astype(BF16)
        r.z[rows, :] = (grad_gated * y * sig * (1.0 + gate * (1.0 - sig))).astype(BF16)

    def weight_grad(grad_ref, out_ref):
        for i in range(dps):
            out_ref[i] = mm(grad_ref[...], r.xn[i, pl.ds(HALO, tokens), :], TN).astype(BF16)

    links.drain()

    @pl.loop(0, quads)
    def _(i):
        rows = pl.ds(pl.multiple_of(i * piece, piece), piece)
        r.hid[i] = mm(r.mixed[rows, :], r.wo[...]).astype(BF16)

    own_copies = [
        pltpu.make_async_copy(a, b, r.local.at[i])
        for i, (a, b) in enumerate(((r.hid_in, r.hown), (r.og_in, r.oown)))
    ]
    for copy in own_copies:
        copy.start()
    step(op_flow)
    weight_grad(r.z, r.grad)
    op_flow.go()
    step(*z_flows)
    leave_pass(width, r.bc, r.cum, r.y, r.fin)
    step(ds_flow)
    size = BLOCK if width % BLOCK == 0 else 128

    @pl.loop(0, width // size)
    def _(i):
        cols = pl.ds(pl.multiple_of(i * size, size), size)
        total = jnp.zeros((size, model), F32)
        for k in range(quads):
            total = total + mm(r.mixed[k * piece : (k + 1) * piece, cols], r.og[k], TN)
        r.wo[cols, :] = total.astype(BF16)

    step(*z_flows, *out_flows)
    blocks = tokens // BLOCK
    back_inside_pass(width, r, {1: lambda: step(*z_flows)})
    ds_flow.finish()
    r.ds[...] = jnp.where(p > 0, 0.0, r.dsin[...])
    back_outside_pass(
        width, r, {1: lambda: step(*out_flows), blocks - 1: lambda: step(*edge_flows, *out_flows)},
    )
    r.sb[5:6, 0:128], r.sb[6:7, 0:128], r.sb[7:8, 0:128] = r.heads[0:1], r.heads[1:2], r.heads[2:3]
    finish(*edge_flows)
    r.xs[pl.ds(tokens, 8), :] = jnp.where(p > 0, 0.0, r.hx[...])
    r.dbc[pl.ds(tokens, 8), :] = jnp.where(p > 0, 0.0, r.hb[...])

    def unconv(source, row, cols, w_ref):
        wide = source[pl.ds(row, chunk + 8), cols]
        total = jnp.zeros((chunk, 128), F32)
        for k in range(4):
            total = total + w_ref[k : k + 1, cols] * wide[3 - k : 3 - k + chunk]
        return total

    @pl.loop(0, tokens // chunk)
    def _(i):
        row = pl.multiple_of(i * chunk, chunk)
        inside = pl.ds(pl.multiple_of(row % piece, chunk), chunk)
        for c in range(2):
            cols = slice(128 * c, 128 * c + 128)
            r.bcs[row // piece, inside, cols] = unconv(r.dbc, row, cols, r.wbc)
        for pair in range(width // 128):
            cols = slice(128 * pair, 128 * pair + 128)
            r.mixed[pl.ds(row, chunk), cols] = unconv(r.xs, row, cols, r.wxc).astype(BF16)

    op_flow.finish()
    op_flow.drain()
    for flow in z_flows:
        flow.drain()
    step(*z_flows)
    step(sx_flow, sb_flow)
    step(bc_flow)
    weight_grad(r.mixed, r.grad)
    for _ in dp_bits:
        step(sx_flow)
    step(*x_flows, bc_flow)
    row = lax.broadcasted_iota(jnp.int32, (state2, 128), 0)
    col = lax.broadcasted_iota(jnp.int32, (state2, 128), 1)
    from_bc = jnp.logical_and(row == col + q * bc_cols, col < bc_cols).astype(BF16)
    from_dt = jnp.logical_and(lane_col == lane_row + bc_cols, lane_row < own_heads).astype(BF16)

    wide_rows = r.wt.shape[1]
    row = lax.broadcasted_iota(jnp.int32, (128, wide_rows), 0)
    col = lax.broadcasted_iota(jnp.int32, (128, wide_rows), 1)

    def dt_rows(i):
        return jnp.logical_and(
            jnp.logical_and(row >= bc_cols, row < bc_cols + own_heads),
            col == state2 + i * own_heads + row - bc_cols,
        )

    def bc_rows(i):
        return jnp.logical_and(row < bc_cols, col == row + i * bc_cols)

    take = dt_rows(q).astype(BF16)
    for i in range(dps):
        r.wtail[i] = mm(take, r.wt[i]).astype(BF16)
    r.tail[...] = mm(r.gdt[...], from_dt).astype(BF16)
    r.sp[...] = jnp.zeros_like(r.sp)

    span = min(BLOCK, piece)

    def grad_rows(k, carry):
        at = pl.multiple_of(k * span, span)
        rows = pl.ds(at, span)
        inside = pl.ds(pl.multiple_of(at % piece, span), span)
        gz, gx, gt = r.z[rows, :], r.mixed[rows, :], r.tail[rows, :]
        for i in range(dps):
            grad = mm(gz, r.wz[i]) + mm(gx, r.wx[i]) + mm(gt, r.wtail[i])
            cols = slice(i * share, (i + 1) * share)
            unit = r.xn[i, pl.ds(pl.multiple_of(at + HALO, 16), span), :].astype(F32)
            r.sp[:, cols] += jnp.sum(grad * unit, 0, keepdims=True)
            r.og[at // piece, inside, cols] = grad.astype(BF16)
        return carry

    lax.fori_loop(0, tokens // span, grad_rows, 0)
    step(gn_flow, *x_flows)
    step(bc_flow, *out_flows, gn_flow)
    step(*x_flows)
    finish(bc_flow)

    @pl.loop(0, quads)
    def _(i):
        rows = pl.ds(pl.multiple_of(i * piece, piece), piece)
        r.tail[rows, :] = (mm(r.bcall[i], from_bc) + mm(r.gdt[rows, :], from_dt)).astype(BF16)

    weight_grad(r.tail, r.gradt)
    step(t_flow, sb_flow, sx_flow)
    own_bc = r.bcall[q]
    for i in range(dps):
        cols = slice(i * share, (i + 1) * share)
        grad = mm(own_bc, r.wt[i, 0:state2, :])
        at = pl.ds(pl.multiple_of(q * piece + HALO, 16), piece)
        r.sp[:, cols] += jnp.sum(grad * r.xn[i, at, :].astype(F32), 0, keepdims=True)
        r.yl[i * piece : (i + 1) * piece, 0:share] = grad
    r.sp[...] = r.sp[...] / pre
    step(sp_flow, t_flow, *out_flows)
    step(sp_flow, t_flow)
    step(*z_flows)
    step(sp_flow, sx_flow, sb_flow, *out_flows)
    gn_flow.finish()
    for copy in own_copies:
        copy.wait()
    for i in range(dps):
        cols = slice(i * share, (i + 1) * share)
        r.gn_own[:, cols] += r.yl[i * piece : (i + 1) * piece, 0:share]

    @pl.loop(0, piece // few)
    def _(i):
        rows = pl.ds(pl.multiple_of(i * few, few), few)
        wide = r.hown[rows, :].astype(F32)
        r.op_own[rows, :] = wide + r.op_own[rows, :]
        inv_rms = lax.rsqrt(jnp.mean(wide * wide, -1, keepdims=True) + EPSILON)
        unit = wide * inv_rms
        grad = r.gn_own[rows, :] * pre
        r.gn_own[rows, :] = r.oown[rows, :].astype(F32) + inv_rms * (
            grad - unit * jnp.mean(grad * unit, -1, keepdims=True)
        )

    finish(*x_flows, t_flow, sp_flow, *out_flows, *z_flows, sx_flow, sb_flow)
    for copy in kept:
        copy.wait()
    for i in range(quads):
        place = jnp.logical_or(bc_rows(i), dt_rows(i)).astype(BF16)
        piece_t = mm(place, r.ttot[i], TN)
        r.tstage[...] = piece_t.astype(BF16) if i == 0 else (r.tstage[...].astype(F32) + piece_t).astype(BF16)
    last = keeper(r.tstage.at[pl.ds(0, tail_rows)], r.in_out.at[pl.ds(2 * inner, tail_rows)], 12)
    last.start()
    for i in range(quads):
        cols = slice(i * width, (i + 1) * width)
        r.cxw[:, cols] = r.sxall[i, 0:4, :]
        r.cxb[:, cols] = r.sxall[i, 4:5, :]
        r.norm[:, cols] = r.sxall[i, 5:6, :]
    total = r.sball[0]
    every = r.spall[0]
    lane = lax.broadcasted_iota(jnp.int32, (8, 128), 1)
    packed = jnp.where(lane < own_heads, r.sball[0, :, 0:128], 0.0)
    for i in range(1, quads):
        total = total + r.sball[i]
        every = every + r.spall[i]
        moved = jnp.where(lane < own_heads, r.sball[i, :, 0:128], 0.0)
        packed = packed + pltpu.roll(moved, i * own_heads, 1)
    r.cbw[...] = total[0:4]
    r.cbb[...] = total[4:5]
    r.head[...] = packed
    r.pre[...] = every
    last.wait()
    links.drain()


def remote_call(kernel, ident, outs, any_inputs, any_outputs, scratch, flops=2 * 10**10):
    vmem, anywhere = pl.BlockSpec(memory_space=pltpu.VMEM), pl.BlockSpec(memory_space=pltpu.HBM)

    def run(*args):
        moved = sum(a.size * a.dtype.itemsize for a in (*args, *outs))
        return pl.pallas_call(
            kernel,
            out_shape=tuple(outs),
            in_specs=[anywhere if i in any_inputs else vmem for i in range(len(args))],
            out_specs=tuple([anywhere if i in any_outputs else vmem for i in range(len(outs))]),
            scratch_shapes=list(scratch),
            compiler_params=pltpu.CompilerParams(
                vmem_limit_bytes=67043328, collective_id=ident, has_side_effects=True
            ),
            cost_estimate=pl.CostEstimate(flops=flops, bytes_accessed=moved, transcendentals=0),
        )(*args)

    return run


def on_device(
    hidden_in, pre_gain, in_weight, conv_x_weight, conv_x_bias, conv_bc_weight, conv_bc_bias,
    dt_bias, a_log, skip, norm_gain, out_weight, output_gradient,
):
    dp, quads, rank = lax.axis_size("dp"), lax.axis_size("quad"), lax.axis_index("dp")
    _, local, model = hidden_in.shape
    inner, state2, heads = conv_x_bias.shape[0], conv_bc_bias.shape[0], dt_bias.shape[0]
    width, own_heads = inner // quads, heads // quads
    tokens, share, columns = local * quads, model // dp, in_weight.shape[1]

    def spaced(v):
        return lax.dynamic_update_slice_in_dim(
            jnp.zeros((v.shape[0] * dp,), F32), v.astype(F32), rank * v.shape[0], 0
        )

    gain_row = jnp.concatenate([spaced(pre_gain), spaced(norm_gain)])[None]
    per_head = jnp.pad(jnp.stack([dt_bias, a_log, skip]), ((0, 5), (0, 128 - heads)))
    tail_rows = columns - 2 * inner
    tail_wide = tail_rows + -tail_rows % 128

    def sds(shape, dtype=F32):
        return jax.ShapeDtypeStruct(shape, dtype)

    def vm(*shape):
        return pltpu.VMEM(shape, F32)

    def vb(*shape):
        return pltpu.VMEM(shape, BF16)

    rows, own_out, steps = HALO + tokens, width // dp, len(bits_of(dp)) + 1
    levels = len(bits_of(quads))
    scratch = dict(
        wz=vb(dp, width, share), wx=vb(dp, width, share), wt=vb(dp, tail_wide, share),
        wo=vb(width, model), xn=vb(dp, rows, share), og=vb(quads, local, model),
        hid=vb(quads, local, model), px=vb(rows, width), pt=vb(rows, tail_wide), pd=vb(rows, 128),
        xs=vm(tokens + 8, width), bc=vm(tokens, state2), dt=vm(tokens, 128), cum=vm(tokens, 128),
        y=vb(tokens, width), yl=vm(tokens, width), states=vm(tokens // BLOCK, 128, width),
        z=vb(tokens, width), gm=vm(tokens, width), mixed=vb(tokens, width),
        dbc=vm(tokens + 8, state2), gdt=vb(tokens, 128), bcs=vm(quads, local, state2),
        bcbox=vm(quads - 1, local, state2), bcall=vb(quads, local, state2), tail=vb(tokens, 128),
        wtail=vb(dp, 128, share), grad=vb(dp, width, share), gradt=vb(dp, 128, share),
        zbox=vb(dp - 1, width, share), zpair=vb(width, share),
        xpair=vb(width, share),
        tbox=vb(dp - 1, 128, share), tpair=vb(128, share),
        obox=vb(2, dp - 1, own_out, model // 2), opair=vb(2, own_out, model // 2),
        opbox=vb(quads - 1, local, model),
        ttot=vb(quads, 128, share), tstage=vb(tail_wide, share),
        gain=vm(dp, *gain_row.shape), halo=vb(HALO, model), fin=vm(128, width), enter=vm(128, width),
        ds=vm(128, width), stat=vm(levels + 1, 8, tokens), statbox=vm(levels, 8, tokens),
        dscore=vm(BLOCK, BLOCK), heads=vm(8, 128), sx=vm(8, width), sb=vm(8, state2), sp=vm(1, model),
        sxbox=vm(steps, 8, width), sbbox=vm(steps, 8, state2), spbox=vm(steps, 1, model),
        sxall=vm(quads, 8, width), sball=vm(quads, 8, state2), spall=vm(quads, 1, model),
        hx=vm(8, width), hb=vm(8, state2), dsin=vm(128, width), hown=vb(local, model), oown=vb(local, model),
        wxc=vm(4, width), bxc=vm(1, width), dtb=vm(1, 128), alog=vm(1, 128), skip=vm(1, width),
        send=pltpu.SemaphoreType.DMA((192,)), recv=pltpu.SemaphoreType.DMA((192,)),
        local=pltpu.SemaphoreType.DMA((16,)),
    )
    (
        in_out, out_out, op_own, gn_own, conv_x_grad, conv_x_bias_grad, norm_grad, conv_bc_grad,
        conv_bc_bias_grad, head_grad, pre_grad,
    ) = remote_call(
        functools.partial(block_kernel, width, own_heads, heads), 0,
        [
            sds((columns, share), BF16), sds((quads, own_out, model), BF16), sds((local, model)),
            sds((local, model)), sds((4, inner)), sds((1, inner)), sds((1, inner)), sds((4, state2)),
            sds((1, state2)), sds((8, 128)), sds((1, model)),
        ],
        range(5), range(2), [scratch[name] for name in SCRATCH],
    )(
        in_weight.T, out_weight, hidden_in[0], output_gradient[0], gain_row, conv_x_weight,
        conv_x_bias[None], conv_bc_weight, conv_bc_bias[None], per_head,
    )
    return (
        op_own[None], gn_own[None],
        lax.dynamic_slice_in_dim(pre_grad[0], rank * share, share, 0), in_out.T.astype(F32),
        conv_x_grad, conv_x_bias_grad[0], conv_bc_grad, conv_bc_bias_grad[0],
        head_grad[5, :heads], head_grad[6, :heads], head_grad[7, :heads],
        lax.dynamic_slice_in_dim(norm_grad[0], rank * (inner // dp), inner // dp, 0),
        out_out.reshape(width, model).astype(F32),
    )


def solution(mesh):
    dp, seq = mesh.shape["dp"], mesh.shape["seq"]
    fine = Mesh(mesh.devices.reshape(dp, 2, seq // 2), ("dp", "pair", "quad"))
    tokens, whole, rows = P("dp", ("pair", "quad"), None), P(), P("dp", None)
    return jax.shard_map(
        on_device,
        mesh=fine,
        in_specs=(
            tokens, P("dp"), rows, whole, whole, whole, whole, whole, whole, whole, P("dp"), rows, tokens,
        ),
        out_specs=(
            tokens, tokens, P("dp"), rows, whole, whole, whole, whole, whole, whole, whole, P("dp"), rows,
        ),
        check_vma=False,
    )
```
